256 devices in a mesh: tm: 32 (over y, z), tensor: 8 (over x, core).
Axes of the slice: x: 4, y: 4, z: 8, core: 2. Of those that a mesh axis runs over, the one named last changes fastest.
Arguments:
- frames_in: bfloat16 [32, 520, 1024], P('tm'), may hold values from -6 to 6
- frame_time: int32 [16], replicated, may hold values from 0 to 15, each once
- cond_count: int32 [16], replicated, may hold values from 0 to 2
- ln1_gain: float32 [2, 1024], replicated, may hold values from 0.5 to 1.5
- ln1_bias: float32 [2, 1024], replicated, may hold values from -1.75 to 1.75
- qkv_weight: bfloat16 [2, 3, 1024, 1024], P(None, None, None, 'tensor'), may hold values from -17 to 17
- qkv_bias: float32 [2, 3, 1024], P(None, None, 'tensor'), may hold values from -1.75 to 1.75
- out_weight: bfloat16 [2, 1024, 1024], P(None, 'tensor'), may hold values from -0.1875 to 0.1875
- out_bias: float32 [2, 1024], replicated, may hold values from -1.75 to 1.75
- ln2_gain: float32 [2, 1024], replicated, may hold values from 0.5 to 1.5
- ln2_bias: float32 [2, 1024], replicated, may hold values from -1.75 to 1.75
- fc1_weight: bfloat16 [2, 1024, 4096], P(None, None, 'tensor'), may hold values from -0.1875 to 0.1875
- fc1_bias: float32 [2, 4096], P(None, 'tensor'), may hold values from -3 to 3
- fc2_weight: bfloat16 [2, 4096, 1024], P(None, 'tensor'), may hold values from -0.09375 to 0.09375
- fc2_bias: float32 [2, 1024], replicated, may hold values from -1.75 to 1.75
Outputs:
- frames_out: bfloat16 [32, 520, 1024], P('tm', 'tensor')
The draws below stay inside these ranges and needn't reach their ends.
Inputs may be any that keep to these rules, and one draw needn't show every extreme that they name: `frame_time`: every time index 0 to 15 appears once. `cond_count`: the valid action and state tokens of a frame are its first ones.
All inputs are finite; a program needn't handle non-finite values.
Results may differ from the reference program's by a relative error of at most 0.04.
Values may be sent and summed in bfloat16 or wider, within the bound.
A program may use at most 128 MiB of HBM per device.

```python
import jax
import jax.numpy as jnp
from jax import lax

D = 1024
HEADS = 16
FF = 4096
PATCH_DEV = 64
COND = 2
SEQS = 8
LAYERS = 2
FRAMES = 16
ROWS = 520
N_TM = 32


def draw_qkv_weight(key, part):
    weights_raw = jnp.clip(jax.random.normal(jax.random.fold_in(key, 101), (LAYERS, 3, D, D), jnp.float32), -5.0, 5.0) * D ** (-0.5)
    return weights_raw.astype(jnp.bfloat16)


def plant(values, stream_key, low, high):
    longest = values.shape.index(max(values.shape))
    spots = []
    for shift in (0, 1):
        where = [jax.random.randint(jax.random.fold_in(stream_key, axis), (), 0, length) for axis, length in enumerate(values.shape)]
        where[longest] = (where[longest] + shift) % values.shape[longest]
        spots.append(tuple(where))
    return values.at[spots[0]].set(low).at[spots[1]].set(high)


def shard_levels(rng, shape, cuts, low, largest):
    gain, own = 1.0, jax.random.fold_in(rng, 6)
    for dim, parts in cuts:
        draws = jnp.exp(jax.random.uniform(jax.random.fold_in(own, dim), (parts,), jnp.float32, low / len(cuts), largest / len(cuts)))
        gain = gain * jnp.repeat(draws, shape[dim] // parts).reshape([-1 if axis == dim else 1 for axis in range(len(shape))])
    return gain


def normal_values(rng, dims, scale, limit, split=(), kind=jnp.bfloat16):
    array = jax.random.normal(rng, dims, jnp.float32) * scale
    if len(split) > 0:
        array = shard_levels(rng, dims, split, -0.22, 0.18) * array
    return jnp.clip(array, min=-limit, max=limit).astype(kind)


def setup_inputs(seed: int = 0) -> dict:
    keys = jax.random.split(jax.random.key(seed), 16)
    return {
        "frames_in": normal_values(keys[0], (N_TM, ROWS, D), 1.0, 6.0, ((0, 32),)),
        "frame_time": jax.random.permutation(keys[1], FRAMES).astype(jnp.int32),
        "cond_count": plant(jax.random.randint(keys[2], (FRAMES,), 0, COND + 1), jax.random.fold_in(keys[2], 1), 0, COND).astype(jnp.int32),
        "ln1_gain": jnp.clip(1.0 + 0.1 * jax.random.normal(keys[3], (LAYERS, D), jnp.float32), 0.5, 1.5),
        "ln1_bias": normal_values(keys[4], (LAYERS, D), 0.3, 1.75, (), jnp.float32),
        "qkv_weight": draw_qkv_weight(jax.random.fold_in(keys[15], 71), 0),
        "qkv_bias": normal_values(keys[6], (LAYERS, 3, D), 0.3, 1.75, ((2, 8),), jnp.float32),
        "out_weight": normal_values(keys[7], (LAYERS, D, D), D ** -0.5, 0.1875, ((1, 8),)),
        "out_bias": normal_values(keys[8], (LAYERS, D), 0.3, 1.75, (), jnp.float32),
        "ln2_gain": jnp.clip(1.0 + 0.1 * jax.random.normal(keys[9], (LAYERS, D), jnp.float32), 0.5, 1.5),
        "ln2_bias": normal_values(keys[10], (LAYERS, D), 0.3, 1.75, (), jnp.float32),
        "fc1_weight": normal_values(keys[11], (LAYERS, D, FF), D ** -0.5, 0.1875, ((2, 8),)),
        "fc1_bias": normal_values(keys[12], (LAYERS, FF), 0.5, 3.0, ((1, 8),), jnp.float32),
        "fc2_weight": normal_values(keys[13], (LAYERS, FF, D), FF ** -0.5, 0.09375, ((1, 8),)),
        "fc2_bias": normal_values(keys[14], (LAYERS, D), 0.3, 1.75, (), jnp.float32),
    }


def layer_norm(inputs, gain_row, bias_row):
    center = lax.optimization_barrier(jnp.mean(inputs, axis=-1, keepdims=True))
    spread = lax.optimization_barrier(jnp.mean(jnp.square(inputs - center), axis=-1, keepdims=True))
    return (inputs - center) * lax.rsqrt(spread + 1e-06) * gain_row + bias_row

def piece_tables(frame_time, cond_count, piece_count, frame_split, piece_rows):
    cond_dev = COND // frame_split
    piece_ids = jnp.arange(piece_count, dtype=jnp.int32)
    frame_ids = jnp.arange(frame_time.shape[0], dtype=jnp.int32)
    matches = (piece_ids // frame_split)[:, None] == frame_ids[None, :]
    piece_time = lax.optimization_barrier(jnp.sum(jnp.where(matches, frame_time[None, :], 0), axis=1)).astype(jnp.int32)
    piece_cond = lax.optimization_barrier(jnp.sum(jnp.where(matches, cond_count[None, :], 0), axis=1)).astype(jnp.int32)
    slot_index = jnp.arange(piece_rows, dtype=jnp.int32)
    cond_slot = (piece_ids % frame_split)[:, None] * cond_dev + slot_index[None, :] - PATCH_DEV
    valid = (slot_index[None, :] < PATCH_DEV) | (cond_slot < piece_cond[:, None])
    return (piece_time, valid)

def reference(frames_in, frame_time, cond_count, ln1_gain, ln1_bias, qkv_weight, qkv_bias, out_weight, out_bias, ln2_gain, ln2_bias, fc1_weight, fc1_bias, fc2_weight, fc2_bias):
    frame_split = N_TM // FRAMES
    cond_dev = COND // frame_split
    piece_rows = PATCH_DEV + cond_dev
    piece_time, valid = piece_tables(frame_time, cond_count, N_TM, frame_split, piece_rows)
    head_dim = D // HEADS
    scale = head_dim ** (-0.5)
    stream = frames_in
    for layer_idx in range(LAYERS):
        flattened = stream.reshape(-1, D).astype(jnp.float32)
        normed = layer_norm(flattened, ln1_gain[layer_idx], ln1_bias[layer_idx]).astype(jnp.bfloat16)
        projected = []
        for part_idx in range(3):
            result = jnp.dot(normed, qkv_weight[layer_idx, part_idx], preferred_element_type=jnp.float32) + qkv_bias[layer_idx, part_idx]
            result = lax.optimization_barrier(result.astype(jnp.bfloat16))
            projected.append(result.astype(jnp.float32).reshape(N_TM, SEQS, piece_rows, HEADS, head_dim))
        queries, keys_all, values_all = projected

        def one_piece(piece_idx):
            query_block = lax.dynamic_index_in_dim(queries, piece_idx, 0, keepdims=False)
            scores = jnp.einsum('sqhd,gskhd->shqgk', query_block, keys_all) * scale
            my_time = lax.dynamic_index_in_dim(piece_time, piece_idx, 0, keepdims=False)
            allowed = (piece_time <= my_time)[:, None] & valid
            scores = jnp.where(allowed, scores, -1e+30)
            highest = lax.optimization_barrier(jnp.max(scores, axis=(3, 4), keepdims=True))
            weights = jnp.where(allowed, jnp.exp(scores - highest), 0.0)
            totals = lax.optimization_barrier(jnp.sum(weights, axis=(3, 4)))
            rounded = lax.optimization_barrier(weights.astype(jnp.bfloat16)).astype(jnp.float32)
            mixed = jnp.einsum('shqgk,gskhd->shqd', rounded, values_all) / totals[..., None]
            return jnp.transpose(mixed, (0, 2, 1, 3)).reshape(SEQS * piece_rows, D).astype(jnp.bfloat16)
        attended = lax.map(one_piece, jnp.arange(N_TM, dtype=jnp.int32))
        projection = jnp.dot(attended.reshape(-1, D), out_weight[layer_idx], preferred_element_type=jnp.float32)
        first = flattened + projection + out_bias[layer_idx]
        normed_two = layer_norm(first, ln2_gain[layer_idx], ln2_bias[layer_idx]).astype(jnp.bfloat16)
        inner = jax.nn.gelu(jnp.dot(normed_two, fc1_weight[layer_idx], preferred_element_type=jnp.float32) + fc1_bias[layer_idx], approximate=False).astype(jnp.bfloat16)
        output = jnp.dot(inner, fc2_weight[layer_idx], preferred_element_type=jnp.float32)
        stream = (first + output + fc2_bias[layer_idx]).astype(jnp.bfloat16).reshape(N_TM, SEQS * piece_rows, D)
    return stream
```

```python
import functools

import jax
import jax.numpy as jnp
from jax import lax
from jax.experimental import pallas as pl
from jax.experimental.pallas import tpu as pltpu
from jax.sharding import PartitionSpec as P

MESH = pl.DeviceIdType.MESH
LAYERS = 2
D = 1024
F32 = jnp.float32
BF16 = jnp.bfloat16
NEG = -1e30
R = 80
VMEM = pltpu.VMEM
DMA = pltpu.SemaphoreType.DMA


def mod(a, n):
    return lax.rem(a, n)


def place(y, z, x, c):
    return {"tm": y * 8 + z, "tensor": x * 2 + c}


def layer_norm(rows, gain, bias):
    center = jnp.mean(rows, axis=-1, keepdims=True)
    moved = rows - center
    spread = jnp.mean(moved * moved, axis=-1, keepdims=True)
    return moved * lax.rsqrt(spread + 1e-06) * gain + bias


def gelu(v):
    return 0.5 * v * (1.0 + lax.erf(v * (0.5**0.5)))


def dot(a, b):
    return lax.dot_general(a, b, (((1,), (0,)), ((), ())), preferred_element_type=F32)


def dot_t(a, b):
    return lax.dot_general(a, b, (((1,), (1,)), ((), ())), preferred_element_type=F32)


def kernel(
    x_ref, bias_ref, ln1g, ln1b, ln2g, ln2b, outb, fc2b, qkvb, fc1b, wq_hbm, wo_hbm, w1_hbm, w2_hbm,
    out_ref,
    wq, qb, wo, w1, b1, w2, xg, msg, rk, fk, ksl, ob, ab, nb, pb, rb, acc, first, bd, bf,
    s_lq, s_lo, s_l1, s_l2,
    s_sq, s_rq, s_sb, s_rb, s_s1, s_r1, s_s2, s_r2,
    s_so, s_ro, s_sfo, s_rfo,
    s_sm, s_rm, s_sf, s_rf, s_sr, s_rr, s_sn, s_rn, s_sp, s_rp, s_sx, s_rx,
):
    p = lax.axis_index("tm")
    t = lax.axis_index("tensor")
    y, z = p // 8, mod(p, 8)
    x, c = t // 2, mod(t, 2)
    sib = place(y, z, x, 1 - c)
    zh, zl = z // 4, mod(z, 4)
    att = mod(y - zl + 4, 4)
    half = 1 - c

    def peer(k):
        return place(y, z, mod(x + k, 4), c)

    def clip_home(i, h):
        return place(mod(i + h, 4), 4 * c + h, x, 1 - zh)

    def part_source(j):
        return place(j // 4, 4 * half + mod(j, 4), x, zh)

    def part_home(j):
        return place(j // 4, 4 * half + mod(j, 4), att, zh)

    def head_source(h):
        return place(mod(x + mod(h, 4), 4), 4 * c + mod(h, 4), h // 4, 1 - zh)

    def remote(src, dst, ssem, rsem, dev):
        return pltpu.make_async_remote_copy(
            src_ref=src, dst_ref=dst, send_sem=ssem, recv_sem=rsem, device_id=dev, device_id_type=MESH
        )

    def arrived(dst, rsem):
        remote(dst, dst, rsem, rsem, sib).wait_recv()

    def sent(src, ssem):
        remote(src, src, ssem, ssem, sib).wait_send()

    barrier = pltpu.get_barrier_semaphore()

    def greet(dev):
        pl.semaphore_signal(barrier, inc=1, device_id=dev, device_id_type=MESH)

    greet(sib)
    for k in range(1, 4):
        greet(peer(k))

    @pl.loop(0, 16)
    def _(j):
        greet(part_source(j))
        greet(head_source(j))

    def lq(l, j):
        cols = pl.ds(pl.multiple_of(c * 384 + j * 128, 128), 128)
        return pltpu.make_async_copy(wq_hbm.at[l, j], wq.at[l, :, cols], s_lq.at[l, j])

    for l in range(LAYERS):
        for j in range(3):
            lq(l, j).start()
    for l in range(LAYERS):
        pltpu.make_async_copy(wo_hbm.at[l], wo.at[l, t], s_lo.at[l]).start()
        pltpu.make_async_copy(w1_hbm.at[l], w1.at[l, c], s_l1.at[l]).start()
        pltpu.make_async_copy(w2_hbm.at[l], w2.at[l, c], s_l2.at[l]).start()

    bd[...] = jnp.broadcast_to(bias_ref[0][:, None, :], (16, 64, 128)).astype(BF16)
    bf[...] = jnp.broadcast_to(bias_ref[1][:, None, :], (16, 64, 128)).astype(BF16)
    qb[c] = qkvb[...]
    b1[c] = fc1b[...]

    pl.semaphore_wait(barrier, 36)

    def rq(l, j):
        cols = pl.ds(pl.multiple_of(c * 384 + j * 128, 128), 128)
        return remote(wq_hbm.at[l, j], wq.at[l, :, cols], s_sq.at[l, j], s_rq.at[l, j], sib)

    def rq_arrived(l, j):
        cols = pl.ds(pl.multiple_of((1 - c) * 384 + j * 128, 128), 128)
        arrived(wq.at[l, :, cols], s_rq.at[l, j])

    cb0 = remote(qkvb, qb.at[c], s_sb.at[0], s_rb.at[0], sib)
    cb1 = remote(fc1b, b1.at[c], s_sb.at[1], s_rb.at[1], sib)
    cb0.start()
    for j in range(3):
        rq(0, j).start()

    def wo_send(l, k):
        return remote(wo_hbm.at[l], wo.at[l, t], s_so.at[l, k - 1], s_ro.at[l, x], peer(k))

    def wo_forward(l, k):
        xx = mod(x + k, 4)
        src = wo_hbm.at[l] if k == 0 else wo.at[l, 2 * xx + c]
        return remote(src, wo.at[l, 2 * xx + c], s_sfo.at[l, k], s_rfo.at[l, xx], sib)

    def later_weights():
        for k in range(1, 4):
            wo_send(0, k).start()
        wo_forward(0, 0).start()
        cb1.start()
        for l in range(LAYERS):
            remote(w1_hbm.at[l], w1.at[l, c], s_s1.at[l], s_r1.at[l], sib).start()
            remote(w2_hbm.at[l], w2.at[l, c], s_s2.at[l], s_r2.at[l], sib).start()
        for j in range(3):
            rq(1, j).start()

    lane_r = lax.broadcasted_iota(jnp.int32, (R, 128), 1)
    low_r = lane_r < 64
    row16 = lax.broadcasted_iota(jnp.int32, (16, 128), 0)
    low16 = lax.broadcasted_iota(jnp.int32, (16, 128), 1) < 64
    low32 = lax.broadcasted_iota(jnp.int32, (32, 128), 1) < 64

    def swap(v, axis=1):
        return pltpu.roll(v, 64, axis)

    def rounded(v):
        return v.astype(BF16).astype(F32)

    def msg_send(l, i, h):
        return remote(
            msg.at[l, i, h], rk.at[l, y * 4 + zl], s_sm.at[l, i, h], s_rm.at[l, y * 4 + zl], clip_home(i, h)
        )

    def project(l, i, rows):
        h = layer_norm(rows.astype(F32), ln1g[l : l + 1], ln1b[l : l + 1]).astype(BF16)
        out = dot(h, wq[l])
        for s in range(2):
            q = rounded(out[:, s * 384 : s * 384 + 128] + qb[s, l, 0:1]) * 0.125
            k = rounded(out[:, s * 384 + 128 : s * 384 + 256] + qb[s, l, 1:2])
            v = rounded(out[:, s * 384 + 256 : s * 384 + 384] + qb[s, l, 2:3])
            kr, vr, qr = swap(k), swap(v), swap(q)
            for hh in range(2):
                kv = jnp.where(low_r, k, vr) if hh == 0 else jnp.where(low_r, kr, v)
                qp = jnp.where(low32, q[0:32], qr[32:64]) if hh == 0 else jnp.where(low32, qr[0:32], q[32:64])
                qs = q[64:65] if hh == 0 else qr[64:65]
                tile = jnp.where(
                    row16 == 0, kv[64:80],
                    jnp.where((row16 == 1) & low16, jnp.broadcast_to(qs, (16, 128)), 0.0),
                )
                msg[l, i, 2 * s + hh, 0:64] = kv[0:64].astype(BF16)
                msg[l, i, 2 * s + hh, 64:80] = tile.astype(BF16)
                msg[l, i, 2 * s + hh, 80:112] = qp.astype(BF16)
        for hh in range(4):
            msg_send(l, i, hh).start()

    def forward(l, j):
        return remote(rk.at[l, j, pl.ds(0, 80)], fk.at[l, j], s_sf.at[l, j], s_rf.at[l, j], sib)

    def result_send(l, j):
        return remote(ob.at[l, j], ab.at[l, 4 * x + zl], s_sr.at[l, j], s_rr.at[l, 4 * x + zl], part_home(j))

    def pick(row, count):
        a = lax.broadcasted_iota(jnp.int32, (count, count * 16), 0)
        b = lax.broadcasted_iota(jnp.int32, (count, count * 16), 1)
        return (b == a * 16 + row).astype(BF16)

    def attend(l):
        @pl.loop(0, 16)
        def _(j):
            arrived(rk.at[l, j], s_rm.at[l, j])
            forward(l, j).start()

        @pl.loop(0, 16)
        def _(j):
            arrived(fk.at[l, j], s_rf.at[l, j])

        tiles = rk[l, :, 64:80, :].reshape(256, 128)
        ksl[0:16, 0:128] = dot(pick(0, 16), tiles).astype(BF16)
        ksl[16:32, 0:128] = dot(pick(0, 16), fk[l, :, 64:80, :].reshape(256, 128)).astype(BF16)
        ksl[0:16, 128:256] = bias_ref[2].astype(BF16)
        ksl[16:32, 128:256] = bias_ref[3].astype(BF16)
        a = lax.broadcasted_iota(jnp.int32, (16, 128), 0)
        b = lax.broadcasted_iota(jnp.int32, (16, 128), 1)
        qslot = jnp.concatenate([dot(pick(1, 16), tiles).astype(BF16), (a == b).astype(BF16)], axis=1)

        @pl.loop(0, 4)
        def _(g):
            q = rk[l, pl.ds(4 * g, 4), 80:112, :].astype(F32).reshape(128, 128)
            low128 = lax.broadcasted_iota(jnp.int32, (128, 128), 1) < 64
            qlo = jnp.where(low128, q, 0.0).astype(BF16).reshape(4, 32, 128)
            qhi = jnp.where(low128, swap(q), 0.0).astype(BF16).reshape(4, 32, 128)
            qq = jnp.concatenate([qlo, qhi], axis=1).reshape(256, 128)
            mine = lax.broadcasted_iota(jnp.int32, (256, 128), 0) // 64 + 4 * g
            hot = (mine == lax.broadcasted_iota(jnp.int32, (256, 128), 1)).astype(BF16)
            qx = jnp.concatenate([jnp.concatenate([qq, hot], axis=1), qslot], axis=0)
            k1 = rk[l, :, 0:64, :].reshape(1024, 128)
            k2 = fk[l, :, 0:64, :].reshape(1024, 128)
            s1 = dot_t(qx, jnp.concatenate([k1, bd[...].reshape(1024, 128)], axis=1))
            s2 = dot_t(qx, jnp.concatenate([k2, bf[...].reshape(1024, 128)], axis=1))
            s3 = dot_t(qx, ksl[...])
            top = jnp.maximum(
                jnp.maximum(jnp.max(s1, axis=1, keepdims=True), jnp.max(s2, axis=1, keepdims=True)),
                jnp.max(s3, axis=1, keepdims=True),
            )
            e1, e2, e3 = jnp.exp(s1 - top), jnp.exp(s2 - top), jnp.exp(s3 - top)
            total = (
                jnp.sum(e1, axis=1, keepdims=True)
                + jnp.sum(e2, axis=1, keepdims=True)
                + jnp.sum(e3, axis=1, keepdims=True)
            )
            o = dot(e1.astype(BF16), k1) + dot(e2.astype(BF16), k2) + dot(e3.astype(BF16), ksl[:, 0:128])
            o = o / total
            patch = o[0:256].reshape(4, 64, 128)
            lo = swap(patch[:, 0:32].reshape(128, 128))
            hi = patch[:, 32:64].reshape(128, 128)
            ob[l, pl.ds(4 * g, 4), 0:32, :] = jnp.where(low128, lo, hi).astype(BF16).reshape(4, 32, 128)
            ra = lax.broadcasted_iota(jnp.int32, (64, 16), 0)
            rc = lax.broadcasted_iota(jnp.int32, (64, 16), 1)
            spread = (ra == (rc - 4 * g) * 16).astype(BF16)
            ob[l, pl.ds(4 * g, 4), 32:48, :] = (
                dot(spread, o[256:272].astype(BF16)).astype(BF16).reshape(4, 16, 128)
            )
            for j in range(4):
                result_send(l, 4 * g + j).start()

    def combine(l, own):
        @pl.loop(0, 16)
        def _(h):
            arrived(ab.at[l, h], s_rr.at[l, h])

        cols = []
        for m in range(8):
            a = ab[l, 2 * m].astype(F32)
            b = ab[l, 2 * m + 1].astype(F32)
            ar, br = swap(a), swap(b)
            cols.append(
                jnp.concatenate(
                    [
                        jnp.where(low32, a[0:32], br[0:32]),
                        jnp.where(low32, ar[0:32], b[0:32]),
                        jnp.where(low16, ar[32:48], b[32:48]),
                    ],
                    axis=0,
                )
            )
        attended = jnp.concatenate(cols, axis=1).astype(BF16)
        proj = dot(attended, wo[l].reshape(D, D))
        f = own.astype(F32) + proj + outb[l : l + 1]
        first[...] = f
        return layer_norm(f, ln2g[l : l + 1], ln2b[l : l + 1]).astype(BF16)

    def norm_send(l, k):
        return remote(nb.at[l, x], nb.at[l, x], s_sn.at[l, k - 1], s_rn.at[l, x], peer(k))

    def part_send(l, k):
        xx = mod(x + k, 4)
        return remote(pb.at[l, xx], rb.at[l, x], s_sp.at[l, k - 1], s_rp.at[l, x], peer(k))

    def mlp(l, rows):
        total = None
        for s in range(2):
            v = dot(rows, w1[l, s]) + b1[s, l : l + 1]
            part = dot(gelu(v).astype(BF16), w2[l, s])
            total = part if total is None else total + part
        return total

    def row_send(k):
        return remote(xg.at[x], xg.at[x], s_sx.at[k - 1], s_rx.at[x], peer(k))

    for l in range(LAYERS):
        if l == 0:
            for j in range(3):
                lq(0, j).wait()
            arrived(qb.at[1 - c], s_rb.at[0])
            for j in range(3):
                rq_arrived(0, j)

            @pl.loop(0, 4)
            def _(k):
                i = mod(x + k, 4)
                project(0, i, x_ref[i])

            later_weights()
        else:
            for k in range(1, 4):
                wo_send(1, k).start()
            wo_forward(1, 0).start()
            for j in range(3):
                lq(1, j).wait()
                rq_arrived(1, j)
            project(1, x, xg[x])
            for k in (1, 3, 2):
                i = mod(x + k, 4)
                arrived(xg.at[i], s_rx.at[i])
                project(1, i, xg[i])

        attend(l)

        pltpu.make_async_copy(wo_hbm.at[l], wo.at[l, t], s_lo.at[l]).wait()
        for k in range(1, 4):
            i = mod(x + k, 4)
            arrived(wo.at[l, 2 * i + c], s_ro.at[l, i])
            wo_forward(l, k).start()
        for k in range(4):
            i = mod(x + k, 4)
            arrived(wo.at[l, 2 * i + 1 - c], s_rfo.at[l, i])

        own = x_ref[x] if l == 0 else xg[x]
        nb[l, x] = combine(l, own)
        for k in (2, 1, 3):
            norm_send(l, k).start()

        pltpu.make_async_copy(w1_hbm.at[l], w1.at[l, c], s_l1.at[l]).wait()
        pltpu.make_async_copy(w2_hbm.at[l], w2.at[l, c], s_l2.at[l]).wait()
        if l == 0:
            arrived(b1.at[1 - c], s_rb.at[1])
        arrived(w1.at[l, 1 - c], s_r1.at[l])
        arrived(w2.at[l, 1 - c], s_r2.at[l])

        acc[...] = mlp(l, nb[l, x])
        for k in (1, 3, 2):
            i = mod(x + k, 4)
            arrived(nb.at[l, i], s_rn.at[l, i])
            pb[l, i] = mlp(l, nb[l, i]).astype(BF16)
            part_send(l, k).start()

        total = acc[...]
        for k in (1, 3, 2):
            i = mod(x + k, 4)
            arrived(rb.at[l, i], s_rp.at[l, i])
            total = total + rb[l, i].astype(F32)
        new = (first[...] + total + fc2b[l : l + 1]).astype(BF16)
        if l == 0:
            xg[x] = new
            for k in (2, 1, 3):
                row_send(k).start()
        else:
            out_ref[0] = new[0:65]

    sent(qb.at[0], s_sb.at[0])
    sent(b1.at[0], s_sb.at[1])
    for k in range(3):
        sent(xg.at[0], s_sx.at[k])
    for l in range(LAYERS):
        for j in range(3):
            rq(l, j).wait_send()
        sent(w1.at[l, 0], s_s1.at[l])
        sent(w2.at[l, 0], s_s2.at[l])
        for k in range(3):
            sent(wo.at[l, 0], s_so.at[l, k])
            sent(nb.at[l, 0], s_sn.at[l, k])
            sent(pb.at[l, 0], s_sp.at[l, k])
        for k in range(4):
            sent(wo.at[l, 0], s_sfo.at[l, k])

        @pl.loop(0, 16)
        def _(j):
            sent(msg.at[l, 0, 0], s_sm.at[l, j // 4, mod(j, 4)])
            sent(fk.at[l, 0], s_sf.at[l, j])
            sent(ob.at[l, 0], s_sr.at[l, j])


def shards(
    frames_in, frame_time, cond_count, ln1_gain, ln1_bias, qkv_weight, qkv_bias, out_weight, out_bias,
    ln2_gain, ln2_bias, fc1_weight, fc1_bias, fc2_weight, fc2_bias,
):
    c = lax.rem(lax.axis_index("tensor"), 2)
    rows = frames_in[0].reshape(4, 2, 65, D)
    rows = lax.dynamic_index_in_dim(rows, c, 1, keepdims=False)
    rows = jnp.pad(rows, ((0, 0), (0, R - 65), (0, 0)))
    j = jnp.arange(16)
    frame_direct = 4 * (j // 4) + 2 * (1 - c) + (j % 4) // 2
    frame_passed = 4 * (j // 4) + 2 * c + (j % 4) // 2
    part = j % 2
    times = jnp.arange(16)

    def look(ids, table):
        return jnp.sum(jnp.where(ids[:, None] == times[None, :], table[None, :], 0), axis=1)

    td, tf = look(frame_direct, frame_time), look(frame_passed, frame_time)
    cd, cf = look(frame_direct, cond_count), look(frame_passed, cond_count)
    seen_d = td[:, None] <= td[None, :]
    seen_f = tf[:, None] <= td[None, :]
    seen = jnp.stack([seen_d, seen_f, seen_d & (part < cd)[:, None], seen_f & (part < cf)[:, None]])
    bias = jnp.pad(jnp.where(seen, 0.0, NEG), ((0, 0), (0, 0), (0, 112)))
    any_ = pl.BlockSpec(memory_space=pl.ANY)
    vm = pl.BlockSpec(memory_space=VMEM)
    L = LAYERS
    return pl.pallas_call(
        kernel,
        name="layers",
        out_shape=jax.ShapeDtypeStruct((1, 65, D), BF16),
        in_specs=[vm] * 10 + [any_] * 4,
        out_specs=vm,
        scratch_shapes=[
            VMEM((L, D, 768), BF16), VMEM((2, L, 3, 128), F32), VMEM((L, 8, 128, D), BF16),
            VMEM((L, 2, D, 512), BF16), VMEM((2, L, 512), F32), VMEM((L, 2, 512, D), BF16),
            VMEM((4, R, D), BF16), VMEM((L, 4, 4, 112, 128), BF16),
            VMEM((L, 16, 112, 128), BF16), VMEM((L, 16, 80, 128), BF16), VMEM((32, 256), BF16),
            VMEM((L, 16, 48, 128), BF16), VMEM((L, 16, 48, 128), BF16),
            VMEM((L, 4, R, D), BF16), VMEM((L, 4, R, D), BF16), VMEM((L, 4, R, D), BF16),
            VMEM((R, D), F32), VMEM((R, D), F32), VMEM((16, 64, 128), BF16), VMEM((16, 64, 128), BF16),
            DMA((L, 3)), DMA((L,)), DMA((L,)), DMA((L,)),
            DMA((L, 3)), DMA((L, 3)), DMA((2,)), DMA((2,)), DMA((L,)), DMA((L,)), DMA((L,)), DMA((L,)),
            DMA((L, 3)), DMA((L, 4)), DMA((L, 4)), DMA((L, 4)),
            DMA((L, 4, 4)), DMA((L, 16)), DMA((L, 16)), DMA((L, 16)), DMA((L, 16)), DMA((L, 16)),
            DMA((L, 3)), DMA((L, 4)), DMA((L, 3)), DMA((L, 4)), DMA((3,)), DMA((4,)),
        ],
        compiler_params=pltpu.CompilerParams(
            collective_id=0, has_side_effects=True, vmem_limit_bytes=60 * 2**20
        ),
    )(
        rows, bias, ln1_gain, ln1_bias, ln2_gain, ln2_bias, out_bias, fc2_bias, qkv_bias, fc1_bias,
        qkv_weight, out_weight, fc1_weight, fc2_weight,
    )


def solution(mesh):
    in_specs = (
        P("tm", None, None), P(), P(), P(), P(),
        P(None, None, None, "tensor"), P(None, None, "tensor"), P(None, "tensor", None), P(), P(), P(),
        P(None, None, "tensor"), P(None, "tensor"), P(None, "tensor", None), P(),
    )
    return jax.shard_map(shards, mesh=mesh, in_specs=in_specs, out_specs=P("tm", "tensor", None), check_vma=False)
```

```python
import jax
import jax.numpy as jnp
from jax import lax
from jax.experimental import pallas as pl
from jax.experimental.pallas import tpu as pltpu
from jax.sharding import PartitionSpec as P

MESH = pl.DeviceIdType.MESH
LAYERS = 2
D = 1024
F32 = jnp.float32
BF16 = jnp.bfloat16
NEG = -1e30
B = 144
VMEM = pltpu.VMEM
DMA = pltpu.SemaphoreType.DMA
scope = jax.named_scope


def mod(a, n):
    return lax.rem(a, n)


def place(y, z, x, c):
    return {"tm": y * 8 + z, "tensor": x * 2 + c}


def iota(shape, dim):
    return lax.broadcasted_iota(jnp.int32, shape, dim)


def layer_norm(rows, gain, bias):
    center = jnp.mean(rows, axis=-1, keepdims=True)
    moved = rows - center
    spread = jnp.mean(moved * moved, axis=-1, keepdims=True)
    return moved * lax.rsqrt(spread + 1e-06) * gain + bias


def gelu(v):
    return 0.5 * v * (1.0 + lax.erf(v * (0.5**0.5)))


def dot(a, b):
    return lax.dot_general(a, b, (((1,), (0,)), ((), ())), preferred_element_type=F32)


def dot_t(a, b):
    return lax.dot_general(a, b, (((1,), (1,)), ((), ())), preferred_element_type=F32)


def rounded(v):
    return v.astype(BF16).astype(F32)


def swap(v):
    return pltpu.roll(v, 64, 1)


def pick(row, count):
    a, b = iota((count, count * 16), 0), iota((count, count * 16), 1)
    return (b == a * 16 + row).astype(BF16)


def kernel(
    time_ref, cond_ref, ln1g, ln1b, ln2g, ln2b, outb, fc2b, qkvb, fc1b, x_hbm, wq_hbm, wo_hbm, w1_hbm, w2_hbm,
    out_ref,
    xin, xs, xl, hb, wq, qb, wo, w1, b1, w2, msg, rk, fk, ksl, ob, ab, ag, fst, pf,
    pb, ps, rb, rs, cb, ct, gb, gt, bd, bf, bsl,
    s_x, s_lq, s_lo, s_l1, s_l2,
    s_sq, s_rq, s_sb, s_rb, s_s1, s_r1, s_s2, s_r2,
    s_so, s_ro, s_sfo, s_rfo,
    s_sm, s_rm, s_sf, s_rf, s_sr, s_rr, s_sg, s_rg,
    s_sp, s_rp, s_sps, s_rps, s_sx, s_rx, s_sxl, s_rxl,
    s_sc, s_rc, s_sct, s_rct,
):
    p = lax.axis_index("tm")
    t = lax.axis_index("tensor")
    y, z = p // 8, mod(p, 8)
    x, c = t // 2, mod(t, 2)
    sib = place(y, z, x, 1 - c)
    zh, zl = z // 4, mod(z, 4)
    att = mod(y - zl + 4, 4)
    half = 1 - c
    slot = y * 4 + zl

    def peer(k):
        return place(y, z, mod(x + k, 4), c)

    def clip_home(i, h):
        return place(mod(i + h, 4), 4 * c + h, x, 1 - zh)

    def part_source(j):
        return place(j // 4, 4 * half + mod(j, 4), x, zh)

    def remote(src, dst, ssem, rsem, dev):
        return pltpu.make_async_remote_copy(
            src_ref=src, dst_ref=dst, send_sem=ssem, recv_sem=rsem, device_id=dev, device_id_type=MESH
        )

    def arrived(dst, rsem):
        remote(dst, dst, rsem, rsem, sib).wait_recv()

    def sent(src, ssem):
        remote(src, src, ssem, ssem, sib).wait_send()

    barrier = pltpu.get_barrier_semaphore()

    def greet(dev):
        pl.semaphore_signal(barrier, inc=1, device_id=dev, device_id_type=MESH)

    @pl.loop(0, 16)
    def _(j):
        greet(part_source(j))

    for k in range(1, 4):
        greet(peer(k))
    greet(sib)

    def lx():
        return pltpu.make_async_copy(x_hbm.at[0], xin, s_x)

    def lq(l, j):
        return pltpu.make_async_copy(wq_hbm.at[l, j], wq.at[l, c, :, pl.ds(128 * j, 128)], s_lq.at[l, j])

    def lo(l):
        return pltpu.make_async_copy(wo_hbm.at[l], wo.at[l, t], s_lo.at[l])

    def l1(l):
        return pltpu.make_async_copy(w1_hbm.at[l], w1.at[l, c], s_l1.at[l])

    def l2(l):
        return pltpu.make_async_copy(w2_hbm.at[l], w2.at[l, c], s_l2.at[l])

    lx().start()
    for l in range(LAYERS):
        for j in range(3):
            lq(l, j).start()
    for l in range(LAYERS):
        lo(l).start()
        l1(l).start()
        l2(l).start()

    qb[c] = qkvb[...]
    b1[c] = fc1b[...]

    low = iota((64, 128), 1) < 64
    low32 = iota((32, 128), 1) < 64
    low16 = iota((16, 128), 1) < 64
    row16 = iota((16, 128), 0)
    lane16 = iota((16, 128), 1)

    def rq(l, j):
        return remote(
            wq_hbm.at[l, j], wq.at[l, c, :, pl.ds(128 * j, 128)], s_sq.at[l, j], s_rq.at[l, j], sib
        )

    def rq_arrived(l, j):
        arrived(wq.at[l, 1 - c, :, pl.ds(128 * j, 128)], s_rq.at[l, j])

    def rb0():
        return remote(qkvb, qb.at[c], s_sb.at[0], s_rb.at[0], sib)

    def rb1():
        return remote(fc1b, b1.at[c], s_sb.at[1], s_rb.at[1], sib)

    def r1(l):
        return remote(w1_hbm.at[l], w1.at[l, c], s_s1.at[l], s_r1.at[l], sib)

    def r2(l):
        return remote(w2_hbm.at[l], w2.at[l, c], s_s2.at[l], s_r2.at[l], sib)

    def wo_send(l, k):
        return remote(wo_hbm.at[l], wo.at[l, t], s_so.at[l, k - 1], s_ro.at[l, x], peer(k))

    def wo_forward(l, k):
        xx = mod(x + k, 4)
        src = wo_hbm.at[l] if k == 0 else wo.at[l, 2 * xx + c]
        return remote(src, wo.at[l, 2 * xx + c], s_sfo.at[l, k], s_rfo.at[l, xx], sib)

    def wo_start(l):
        for k in (2, 1, 3):
            wo_send(l, k).start()
        wo_forward(l, 0).start()

    def msg_send(l, s, a, h):
        return remote(
            msg.at[l, s, a, h], rk.at[l, slot], s_sm.at[l, s, a, h], s_rm.at[l, slot], clip_home(2 * a + s, h)
        )

    def forward(l, j):
        return remote(rk.at[l, j, pl.ds(0, 80)], fk.at[l, j], s_sf.at[l, j], s_rf.at[l, j], sib)

    def result_send(l, j):
        me = (mod(att, 2) * 2 + att // 2) * 4 + zl
        return remote(ob.at[l, j], ab.at[l, me], s_sr.at[l, j], s_rr.at[l, me], part_source(j))

    def gather_send(l, s, k):
        return remote(ag.at[l, s, x], ag.at[l, s, x], s_sg.at[l, s, k - 1], s_rg.at[l, s, x], peer(k))

    def part_send(s, k):
        xx = mod(x + k, 4)
        return remote(pb.at[s, xx], rb.at[s, x], s_sp.at[s, k - 1], s_rp.at[s, x], peer(k))

    def part_slot_send(s, k):
        xx = mod(x + k, 4)
        return remote(ps.at[s, xx], rs.at[s, x], s_sps.at[s, k - 1], s_rps.at[s, x], peer(k))

    rows_x = pl.ds(pl.multiple_of(16 * x, 16), 16)
    cols_x = pl.ds(pl.multiple_of(256 * x, 256), 256)

    def rows_of(xx):
        return pl.ds(pl.multiple_of(16 * xx, 16), 16)

    def cols_of(xx):
        return pl.ds(pl.multiple_of(256 * xx, 256), 256)

    def row_send(s, k):
        return remote(
            xs.at[1, s, :, rows_x], xs.at[1, s, :, rows_x], s_sx.at[s, k - 1], s_rx.at[s, x], peer(k)
        )

    def row_slot_send(s, k):
        return remote(
            xl.at[1, s, :, cols_x], xl.at[1, s, :, cols_x], s_sxl.at[s, k - 1], s_rxl.at[s, x], peer(k)
        )

    def last_send(s, a):
        home = place(y, z, 2 * a + s, c)
        return remote(cb.at[s, a], gb.at[x], s_sc.at[s, a], s_rc.at[x], home)

    def last_slot_send(s, a):
        home = place(y, z, 2 * a + s, c)
        return remote(ct.at[s, a], gt.at[x], s_sct.at[s, a], s_rct.at[x], home)

    def project(l, s, h, sh):
        out = dot(h, wq[l, sh])
        q = rounded(out[:, 0:128] + qb[sh, 0, l : l + 1]) * 0.125
        k = rounded(out[:, 128:256] + qb[sh, 1, l : l + 1])
        v = rounded(out[:, 256:384] + qb[sh, 2, l : l + 1])
        kr, vr, qr = swap(k), swap(v), swap(q)
        for a in range(2):
            o = 64 * a
            for hh in range(2):
                kk, vv = (k, vr) if hh == 0 else (kr, v)
                q0, q1 = (q, qr) if hh == 0 else (qr, q)
                kv = jnp.where(low, kk[o : o + 64], vv[o : o + 64])
                qp = jnp.where(low32, q0[o : o + 32], q1[o + 32 : o + 64])
                ka = jnp.broadcast_to(kk[128 + a : 129 + a], (16, 128))
                va = jnp.broadcast_to(vv[128 + a : 129 + a], (16, 128))
                qa = jnp.broadcast_to(q0[128 + a : 129 + a], (16, 128))
                tile = jnp.where(
                    row16 == 0, jnp.where(low16, ka, va), jnp.where((row16 == 1) & low16, qa, 0.0)
                )
                m = msg.at[l, s, a, 2 * sh + hh]
                m[0:64] = kv.astype(BF16)
                m[64:80] = tile.astype(BF16)
                m[80:112] = qp.astype(BF16)

    def send_shard(l, s, sh):
        for n in range(4):
            q = mod(n + zl, 4)
            msg_send(l, s, q // 2, 2 * sh + mod(q, 2)).start()

    def attend(l):
        with scope("wait_msg"):

            @pl.loop(0, 16)
            def _(j):
                arrived(rk.at[l, j], s_rm.at[l, j])
                forward(l, j).start()

        with scope("wait_pass"):

            @pl.loop(0, 16)
            def _(j):
                arrived(fk.at[l, j], s_rf.at[l, j])

        tiles = rk[l, :, 64:80, :].reshape(256, 128)
        ksl[0:16, 0:128] = dot(pick(0, 16), tiles).astype(BF16)
        ksl[16:32, 0:128] = dot(pick(0, 16), fk[l, :, 64:80, :].reshape(256, 128)).astype(BF16)
        ksl[:, 128:256] = bsl[...]
        qslot = jnp.concatenate([dot(pick(1, 16), tiles).astype(BF16), (row16 == lane16).astype(BF16)], axis=1)

        @pl.loop(0, 4)
        def _(g):
            low128 = iota((128, 128), 1) < 64
            q = rk[l, pl.ds(4 * g, 4), 80:112, :].astype(F32).reshape(128, 128)
            qlo = jnp.where(low128, q, 0.0).astype(BF16).reshape(4, 32, 128)
            qhi = jnp.where(low128, swap(q), 0.0).astype(BF16).reshape(4, 32, 128)
            qq = jnp.concatenate([qlo, qhi], axis=1).reshape(256, 128)
            mine = iota((256, 128), 0) // 64 + 4 * g
            hot = (mine == iota((256, 128), 1)).astype(BF16)
            qx = jnp.concatenate([jnp.concatenate([qq, hot], axis=1), qslot], axis=0)
            k1 = rk[l, :, 0:64, :].reshape(1024, 128)
            k2 = fk[l, :, 0:64, :].reshape(1024, 128)
            s1 = dot_t(qx, jnp.concatenate([k1, bd[...].reshape(1024, 128)], axis=1))
            s2 = dot_t(qx, jnp.concatenate([k2, bf[...].reshape(1024, 128)], axis=1))
            s3 = dot_t(qx, ksl[...])
            top = jnp.maximum(
                jnp.maximum(jnp.max(s1, axis=1, keepdims=True), jnp.max(s2, axis=1, keepdims=True)),
                jnp.max(s3, axis=1, keepdims=True),
            )
            e1, e2, e3 = jnp.exp(s1 - top), jnp.exp(s2 - top), jnp.exp(s3 - top)
            total = (
                jnp.sum(e1, axis=1, keepdims=True)
                + jnp.sum(e2, axis=1, keepdims=True)
                + jnp.sum(e3, axis=1, keepdims=True)
            )
            o = dot(e1.astype(BF16), k1) + dot(e2.astype(BF16), k2) + dot(e3.astype(BF16), ksl[:, 0:128])
            o = o / total
            patch = o[0:256].reshape(4, 64, 128)
            lo_ = swap(patch[:, 0:32].reshape(128, 128))
            hi_ = patch[:, 32:64].reshape(128, 128)
            ob[l, pl.ds(4 * g, 4), 0:32, :] = jnp.where(low128, lo_, hi_).astype(BF16).reshape(4, 32, 128)
            spread = (iota((64, 16), 0) == (iota((64, 16), 1) - 4 * g) * 16).astype(BF16)
            ob[l, pl.ds(4 * g, 4), 32:48, :] = (
                dot(spread, o[256:272].astype(BF16)).astype(BF16).reshape(4, 16, 128)
            )
            for j in range(4):
                result_send(l, 4 * g + j).start()

    def assemble(l, s):
        with scope("wait_result"):

            @pl.loop(0, 8)
            def _(n):
                arrived(ab.at[l, 8 * s + n], s_rr.at[l, 8 * s + n])

        for m in range(2):
            slots = []
            for a in range(2):
                u = ab[l, 8 * s + 4 * a + 2 * m].astype(F32)
                v = ab[l, 8 * s + 4 * a + 2 * m + 1].astype(F32)
                ur, vr = swap(u), swap(v)
                out = ag.at[l, s, x]
                out[64 * a : 64 * a + 32, 128 * m : 128 * m + 128] = jnp.where(low32, u[0:32], vr[0:32]).astype(BF16)
                out[64 * a + 32 : 64 * a + 64, 128 * m : 128 * m + 128] = jnp.where(
                    low32, ur[0:32], v[0:32]
                ).astype(BF16)
                slots.append(jnp.broadcast_to(jnp.where(low16[0:1], ur[32:33], v[32:33]), (16, 128)))
            ag[l, s, x, 128:144, 128 * m : 128 * m + 128] = jnp.where(
                row16 == 0, slots[0], jnp.where(row16 == 1, slots[1], 0.0)
            ).astype(BF16)
        for k in (2, 1, 3):
            gather_send(l, s, k).start()

    def stream_rows(l, s):
        return jnp.concatenate([xs[l, s].reshape(128, D), xl[l, s]], axis=0).astype(F32)

    def mix(l, s):
        with scope("wait_gather"):
            for k in (1, 3, 2):
                i = mod(x + k, 4)
                arrived(ag.at[l, s, i], s_rg.at[l, s, i])
        with scope("out_proj"):
            attended = jnp.concatenate([ag[l, s, i] for i in range(4)], axis=1)
            first = stream_rows(l, s) + dot(attended, wo[l].reshape(D, D)) + outb[l : l + 1]
            fst[s] = first
            normed = layer_norm(first, ln2g[l : l + 1], ln2b[l : l + 1]).astype(BF16)
        with scope("mlp"):
            total = None
            for sh in range(2):
                v = dot(normed, w1[l, sh]) + b1[sh, l : l + 1]
                part = dot(gelu(v).astype(BF16), w2[l, sh])
                total = part if total is None else total + part
            pf[s] = total
            if l == 0:
                for i in range(4):
                    for a in range(2):
                        o = 64 * a + 16 * i
                        pb[s, i, a] = total[o : o + 16].astype(BF16)
                    ps[s, i] = total[128:144, 256 * i : 256 * i + 256].astype(BF16)
            else:
                row8 = iota((8, 128), 0)
                for a in range(2):
                    cb[s, a] = total[64 * a : 64 * a + 64].astype(BF16)
                    tile = jnp.zeros((8, 128), F32)
                    for m in range(8):
                        piece = total[128 + a : 129 + a, 128 * m : 128 * m + 128]
                        tile = jnp.where(row8 == m, jnp.broadcast_to(piece, (8, 128)), tile)
                    ct[s, a] = tile
        if l == 0:
            for k in (2, 1, 3):
                part_send(s, k).start()
                part_slot_send(s, k).start()
        else:
            for a in range(2):

                @pl.when(x != 2 * a + s)
                def _():
                    last_send(s, a).start()
                    last_slot_send(s, a).start()

    def next_rows(s):
        with scope("wait_part"):
            for k in (1, 3, 2):
                i = mod(x + k, 4)
                arrived(rb.at[s, i], s_rp.at[s, i])
                arrived(rs.at[s, i], s_rps.at[s, i])
        bias = fc2b[0:1]
        for a in range(2):
            own = pl.ds(pl.multiple_of(64 * a + 16 * x, 16), 16)
            total = pf[s, own] + fst[s, own] + bias
            for k in (1, 2, 3):
                total = total + rb[s, mod(x + k, 4), a].astype(F32)
            xs[1, s, a, rows_x] = total.astype(BF16)
        total = pf[s, 128:144, cols_x] + fst[s, 128:144, cols_x] + fc2b[0:1, cols_x]
        for k in (1, 2, 3):
            total = total + rs[s, mod(x + k, 4)].astype(F32)
        xl[1, s, :, cols_x] = total.astype(BF16)
        for k in (2, 1, 3):
            row_send(s, k).start()
            row_slot_send(s, k).start()

    tq = jnp.zeros((16, 128), jnp.int32)
    td, tf, nd, nf = tq, tq, tq, tq
    for j in range(16):
        fd = 4 * (j // 4) + 2 * (1 - c) + (j % 4) // 2
        fp = 4 * (j // 4) + 2 * c + (j % 4) // 2
        tq = jnp.where(lane16 == j, time_ref[fd], tq)
        td = jnp.where(row16 == j, time_ref[fd], td)
        tf = jnp.where(row16 == j, time_ref[fp], tf)
        nd = jnp.where(row16 == j, cond_ref[fd], nd)
        nf = jnp.where(row16 == j, cond_ref[fp], nf)
    part = mod(row16, 2)
    bias_d = jnp.where(td <= tq, 0.0, NEG)
    bias_f = jnp.where(tf <= tq, 0.0, NEG)
    bsl[0:16] = jnp.where(part < nd, bias_d, NEG).astype(BF16)
    bsl[16:32] = jnp.where(part < nf, bias_f, NEG).astype(BF16)
    for j in range(16):
        bd[j] = jnp.broadcast_to(bias_d[j : j + 1], (64, 128)).astype(BF16)
        bf[j] = jnp.broadcast_to(bias_f[j : j + 1], (64, 128)).astype(BF16)

    with scope("first_rows"):
        lx().wait()
        for s in range(2):
            r = iota((B, 520), 0)
            is_slot = r >= 128
            a = jnp.where(is_slot, r - 128, r // 64)
            want = 65 * (2 * (2 * a + s) + c) + jnp.where(is_slot, 64, mod(r, 64))
            want = jnp.where(r < 130, want, -1)
            rows = dot((want == iota((B, 520), 1)).astype(BF16), xin[...])
            xs[0, s] = rows[0:128].astype(BF16).reshape(2, 64, D)
            xl[0, s] = rows[128:144].astype(BF16)
            hb[s] = layer_norm(rows, ln1g[0:1], ln1b[0:1]).astype(BF16)
        for j in range(3):
            lq(0, j).wait()
        for s in range(2):
            project(0, s, hb[s], c)

    with scope("barrier"):
        pl.semaphore_wait(barrier, 20)

    rb0().start()
    for j in range(3):
        rq(0, j).start()
    for s in range(2):
        send_shard(0, s, c)
    with scope("wait_wq"):
        arrived(qb.at[1 - c], s_rb.at[0])
        for j in range(3):
            rq_arrived(0, j)
    with scope("project0"):
        for s in range(2):
            project(0, s, hb[s], 1 - c)
            send_shard(0, s, 1 - c)
    wo_start(0)
    rb1().start()
    for l in range(LAYERS):
        r1(l).start()
        r2(l).start()
    for j in range(3):
        rq(1, j).start()

    for l in range(LAYERS):
        if l == 1:
            for j in range(3):
                lq(1, j).wait()
                rq_arrived(1, j)
            for s in range(2):
                with scope("wait_row"):
                    for k in (1, 3, 2):
                        i = mod(x + k, 4)
                        arrived(xs.at[1, s, :, rows_of(i)], s_rx.at[s, i])
                        arrived(xl.at[1, s, :, cols_of(i)], s_rxl.at[s, i])
                with scope("project1"):
                    h = layer_norm(stream_rows(1, s), ln1g[1:2], ln1b[1:2]).astype(BF16)
                    for sh in range(2):
                        project(1, s, h, sh)
                        send_shard(1, s, sh)
            wo_start(1)

        with scope("attend"):
            attend(l)

        with scope("assemble"):
            assemble(l, 0)

        with scope("wait_wo"):
            lo(l).wait()
            for k in range(1, 4):
                i = mod(x + k, 4)
                arrived(wo.at[l, 2 * i + c], s_ro.at[l, i])
                wo_forward(l, k).start()
        with scope("assemble"):
            assemble(l, 1)
        with scope("wait_w"):
            for k in range(4):
                i = mod(x + k, 4)
                arrived(wo.at[l, 2 * i + 1 - c], s_rfo.at[l, i])
            l1(l).wait()
            l2(l).wait()
            if l == 0:
                arrived(b1.at[1 - c], s_rb.at[1])
            arrived(w1.at[l, 1 - c], s_r1.at[l])
            arrived(w2.at[l, 1 - c], s_r2.at[l])
        for s in range(2):
            mix(l, s)
        if l == 0:
            for s in range(2):
                next_rows(s)

    sx, ax = mod(x, 2), x // 2
    own = pl.ds(pl.multiple_of(64 * ax, 64), 64)
    last = pf[sx, own] + fst[sx, own] + fc2b[1:2]
    tiles = pf[sx, 128:144] + fst[sx, 128:144] + fc2b[1:2]
    slot_row = jnp.where(ax == 0, tiles[0:1], tiles[1:2])
    for k in (1, 3, 2):
        i = mod(x + k, 4)
        with scope("wait_last"):
            arrived(gb.at[i], s_rc.at[i])
            arrived(gt.at[i], s_rct.at[i])
        last = last + gb[i].astype(F32)
        slot_row = slot_row + jnp.concatenate([gt[i, m : m + 1] for m in range(8)], axis=1)
    out_ref[0, 0:64] = last.astype(BF16)
    out_ref[0, 64:65] = slot_row.astype(BF16)

    with scope("drain"):
        rb0().wait_send()
        rb1().wait_send()
        for s in range(2):
            for k in range(1, 4):
                part_send(s, k).wait_send()
                part_slot_send(s, k).wait_send()
                row_send(s, k).wait_send()
                row_slot_send(s, k).wait_send()
            for a in range(2):

                @pl.when(x != 2 * a + s)
                def _():
                    last_send(s, a).wait_send()
                    last_slot_send(s, a).wait_send()

        for l in range(LAYERS):
            for j in range(3):
                rq(l, j).wait_send()
            r1(l).wait_send()
            r2(l).wait_send()
            for k in range(1, 4):
                wo_send(l, k).wait_send()
                for s in range(2):
                    gather_send(l, s, k).wait_send()
            for k in range(4):
                wo_forward(l, k).wait_send()

            @pl.loop(0, 16)
            def _(j):
                sent(msg.at[l, 0, 0, 0], s_sm.at[l, j // 8, mod(j // 4, 2), mod(j, 4)])
                sent(fk.at[l, 0], s_sf.at[l, j])
                sent(ob.at[l, 0], s_sr.at[l, j])


def shards(
    frames_in, frame_time, cond_count, ln1_gain, ln1_bias, qkv_weight, qkv_bias, out_weight, out_bias,
    ln2_gain, ln2_bias, fc1_weight, fc1_bias, fc2_weight, fc2_bias,
):
    any_ = pl.BlockSpec(memory_space=pl.ANY)
    vm = pl.BlockSpec(memory_space=VMEM)
    sm = pl.BlockSpec(memory_space=pltpu.SMEM)
    L = LAYERS
    return pl.pallas_call(
        kernel,
        name="layers",
        out_shape=jax.ShapeDtypeStruct((1, 65, D), BF16),
        in_specs=[sm] * 2 + [vm] * 8 + [any_] * 5,
        out_specs=vm,
        scratch_shapes=[
            VMEM((520, D), BF16), VMEM((L, 2, 2, 64, D), BF16), VMEM((L, 2, 16, D), BF16), VMEM((2, B, D), BF16),
            VMEM((L, 2, D, 384), BF16), VMEM((2, 3, L, 128), F32), VMEM((L, 8, 128, D), BF16),
            VMEM((L, 2, D, 512), BF16), VMEM((2, L, 512), F32), VMEM((L, 2, 512, D), BF16),
            VMEM((L, 2, 2, 4, 112, 128), BF16),
            VMEM((L, 16, 112, 128), BF16), VMEM((L, 16, 80, 128), BF16), VMEM((32, 256), BF16),
            VMEM((L, 16, 48, 128), BF16), VMEM((L, 16, 48, 128), BF16),
            VMEM((L, 2, 4, B, 256), BF16), VMEM((2, B, D), F32), VMEM((2, B, D), F32),
            VMEM((2, 4, 2, 16, D), BF16), VMEM((2, 4, 16, 256), BF16),
            VMEM((2, 4, 2, 16, D), BF16), VMEM((2, 4, 16, 256), BF16),
            VMEM((2, 2, 64, D), BF16), VMEM((2, 2, 8, 128), F32), VMEM((4, 64, D), BF16), VMEM((4, 8, 128), F32),
            VMEM((16, 64, 128), BF16), VMEM((16, 64, 128), BF16), VMEM((32, 128), BF16),
            DMA, DMA((L, 3)), DMA((L,)), DMA((L,)), DMA((L,)),
            DMA((L, 3)), DMA((L, 3)), DMA((2,)), DMA((2,)), DMA((L,)), DMA((L,)), DMA((L,)), DMA((L,)),
            DMA((L, 3)), DMA((L, 4)), DMA((L, 4)), DMA((L, 4)),
            DMA((L, 2, 2, 4)), DMA((L, 16)), DMA((L, 16)), DMA((L, 16)), DMA((L, 16)), DMA((L, 16)),
            DMA((L, 2, 3)), DMA((L, 2, 4)),
            DMA((2, 3)), DMA((2, 4)), DMA((2, 3)), DMA((2, 4)), DMA((2, 3)), DMA((2, 4)), DMA((2, 3)), DMA((2, 4)),
            DMA((2, 2)), DMA((4,)), DMA((2, 2)), DMA((4,)),
        ],
        compiler_params=pltpu.CompilerParams(
            collective_id=0, has_side_effects=True, vmem_limit_bytes=60 * 2**20
        ),
    )(
        frame_time, cond_count, ln1_gain, ln1_bias, ln2_gain, ln2_bias, out_bias, fc2_bias,
        jnp.transpose(qkv_bias, (1, 0, 2)), fc1_bias, frames_in, qkv_weight, out_weight, fc1_weight, fc2_weight,
    )


def solution(mesh):
    in_specs = (
        P("tm", None, None), P(), P(), P(), P(),
        P(None, None, None, "tensor"), P(None, None, "tensor"), P(None, "tensor", None), P(), P(), P(),
        P(None, None, "tensor"), P(None, "tensor"), P(None, "tensor", None), P(),
    )
    return jax.shard_map(shards, mesh=mesh, in_specs=in_specs, out_specs=P("tm", "tensor", None), check_vma=False)
```

```python
import jax
import jax.numpy as jnp
from jax import lax
from jax.experimental import pallas as pl
from jax.experimental.pallas import tpu as pltpu
from jax.sharding import PartitionSpec as P

MESH = pl.DeviceIdType.MESH
LAYERS = 2
D = 1024
F32 = jnp.float32
BF16 = jnp.bfloat16
NEG = -1e30
ORDER = (0, 2, 1, 3)
VMEM = pltpu.VMEM
DMA = pltpu.SemaphoreType.DMA
scope = jax.named_scope


def mod(a, n):
    return lax.rem(a, n)


def place(y, z, x, c):
    return {"tm": y * 8 + z, "tensor": x * 2 + c}


def iota(shape, dim):
    return lax.broadcasted_iota(jnp.int32, shape, dim)


def layer_norm(rows, gain, bias):
    center = jnp.mean(rows, axis=-1, keepdims=True)
    moved = rows - center
    spread = jnp.mean(moved * moved, axis=-1, keepdims=True)
    return moved * lax.rsqrt(spread + 1e-06) * gain + bias


def gelu(v):
    return 0.5 * v * (1.0 + lax.erf(v * (0.5**0.5)))


def dot(a, b):
    return lax.dot_general(a, b, (((1,), (0,)), ((), ())), preferred_element_type=F32)


def dot_t(a, b):
    return lax.dot_general(a, b, (((1,), (1,)), ((), ())), preferred_element_type=F32)


def rounded(v):
    return v.astype(BF16).astype(F32)


def swap(v):
    return pltpu.roll(v, 64, 1)


def kernel(
    time_ref, cond_ref, ln1g, ln1b, ln2g, ln2b, outb, fc2b, qkvb, fc1b, x_hbm, wq_hbm, wo_hbm, w1_hbm, w2_hbm,
    out_ref,
    xin, xs, xl, hb, wq, qb, wo, w1, b1, w2, msg, msl, rk, rkl, fk, fkl, ksl, ob, obl, ab, abl, ag, agl, fst, pf,
    pb, ps, rb, rs, cb, ct, gb, gt, bd, bf, bsl,
    s_x, s_lq, s_lo, s_l1, s_l2,
    s_sq, s_rq, s_sb, s_rb, s_s1, s_r1, s_s2, s_r2,
    s_so, s_ro, s_sfo, s_rfo,
    s_sm, s_rm, s_sf, s_rf, s_sr, s_rr, s_sg, s_rg,
    s_sp, s_rp, s_sx, s_rx, s_sc, s_rc,
):
    p = lax.axis_index("tm")
    t = lax.axis_index("tensor")
    y, z = p // 8, mod(p, 8)
    x, c = t // 2, mod(t, 2)
    sib = place(y, z, x, 1 - c)
    zh, zl = z // 4, mod(z, 4)
    att = mod(y - zl + 4, 4)
    half = 1 - c
    slot = y * 4 + zl

    def peer(k):
        return place(y, z, mod(x + k, 4), c)

    def clip_home(i, h):
        return place(mod(i + h, 4), 4 * c + h, x, 1 - zh)

    def part_source(j):
        return place(j // 4, 4 * half + mod(j, 4), x, zh)

    def near(n):
        a = n // 4
        return mod(y + a + a // 2 * (5 - 2 * a), 4) * 4 + mod(zl + n, 4)

    def remote(src, dst, ssem, rsem, dev):
        return pltpu.make_async_remote_copy(
            src_ref=src, dst_ref=dst, send_sem=ssem, recv_sem=rsem, device_id=dev, device_id_type=MESH
        )

    def arrived(dst, rsem):
        remote(dst, dst, rsem, rsem, sib).wait_recv()

    def sent(src, ssem):
        remote(src, src, ssem, ssem, sib).wait_send()

    barrier = pltpu.get_barrier_semaphore()

    def greet(dev):
        pl.semaphore_signal(barrier, inc=1, device_id=dev, device_id_type=MESH)

    @pl.loop(0, 16)
    def _(j):
        greet(part_source(j))

    for k in range(1, 4):
        greet(peer(k))
    greet(sib)

    def lx():
        return pltpu.make_async_copy(x_hbm.at[0], xin, s_x)

    def lq(l, j):
        return pltpu.make_async_copy(wq_hbm.at[l, j], wq.at[l, c, :, pl.ds(128 * j, 128)], s_lq.at[l, j])

    def lo(l):
        return pltpu.make_async_copy(wo_hbm.at[l], wo.at[l, t], s_lo.at[l])

    def l1(l):
        return pltpu.make_async_copy(w1_hbm.at[l], w1.at[l, c], s_l1.at[l])

    def l2(l):
        return pltpu.make_async_copy(w2_hbm.at[l], w2.at[l, c], s_l2.at[l])

    lx().start()
    for l in range(LAYERS):
        for j in range(3):
            lq(l, j).start()
    for l in range(LAYERS):
        lo(l).start()
        l1(l).start()
        l2(l).start()

    qb[c] = qkvb[...]
    b1[c] = fc1b[...]

    low = iota((64, 128), 1) < 64
    low1 = iota((1, 128), 1) < 64
    low32 = iota((32, 128), 1) < 64
    row16 = iota((16, 128), 0)
    lane16 = iota((16, 128), 1)

    def rq(l, j):
        return remote(
            wq_hbm.at[l, j], wq.at[l, c, :, pl.ds(128 * j, 128)], s_sq.at[l, j], s_rq.at[l, j], sib
        )

    def rq_arrived(l, j):
        arrived(wq.at[l, 1 - c, :, pl.ds(128 * j, 128)], s_rq.at[l, j])

    def rb0():
        return remote(qkvb, qb.at[c], s_sb.at[0], s_rb.at[0], sib)

    def rb1():
        return remote(fc1b, b1.at[c], s_sb.at[1], s_rb.at[1], sib)

    def r1(l):
        return remote(w1_hbm.at[l], w1.at[l, c], s_s1.at[l], s_r1.at[l], sib)

    def r2(l):
        return remote(w2_hbm.at[l], w2.at[l, c], s_s2.at[l], s_r2.at[l], sib)

    def wo_send(l, k):
        return remote(wo_hbm.at[l], wo.at[l, t], s_so.at[l, k - 1], s_ro.at[l, x], peer(k))

    def wo_forward(l, k):
        xx = mod(x + k, 4)
        src = wo_hbm.at[l] if k == 0 else wo.at[l, 2 * xx + c]
        return remote(src, wo.at[l, 2 * xx + c], s_sfo.at[l, k], s_rfo.at[l, xx], sib)

    def wo_start(l):
        for k in (2, 1, 3):
            wo_send(l, k).start()
        wo_forward(l, 0).start()

    def pair(rows, slot_row, rows_to, slot_to, ssem, rsem, dev):
        return (
            remote(rows, rows_to, ssem.at[0], rsem.at[0], dev),
            remote(slot_row, slot_to, ssem.at[1], rsem.at[1], dev),
        )

    def start(copies):
        for copy in copies:
            copy.start()

    def leave(copies):
        for copy in copies:
            copy.wait_send()

    def both_arrived(rows, slot_row, rsem):
        arrived(rows, rsem.at[0])
        arrived(slot_row, rsem.at[1])

    def msg_send(l, i, h):
        return pair(
            msg.at[l, i, h], msl.at[l, i, h], rk.at[l, slot], rkl.at[l, slot], s_sm.at[l, 4 * i + h],
            s_rm.at[l, slot], clip_home(i, h),
        )

    def forward(l, j):
        return pair(
            rk.at[l, j, pl.ds(0, 64)], rkl.at[l, j, :, pl.ds(0, 128)], fk.at[l, j], fkl.at[l, j], s_sf.at[l, j],
            s_rf.at[l, j], sib,
        )

    def result_send(l, j):
        me = 4 * att + zl
        return pair(
            ob.at[l, j], obl.at[l, j], ab.at[l, me], abl.at[l, me], s_sr.at[l, j], s_rr.at[l, me], part_source(j)
        )

    def gather_send(l, i, k):
        rows, row = ag.at[l, i, x], agl.at[l, i, x]
        return pair(rows, row, rows, row, s_sg.at[l, i, k - 1], s_rg.at[l, i, x], peer(k))

    def rows_of(xx):
        return pl.ds(pl.multiple_of(16 * xx, 16), 16)

    def cols_of(xx):
        return pl.ds(pl.multiple_of(256 * xx, 256), 256)

    def part_send(i, k):
        xx = mod(x + k, 4)
        return pair(
            pb.at[i, xx], ps.at[i, xx], rb.at[i, x], rs.at[i, x], s_sp.at[i, k - 1], s_rp.at[i, x], peer(k)
        )

    def row_send(i, k):
        rows, row = xs.at[1, i, rows_of(x)], xl.at[1, i, :, cols_of(x)]
        return pair(rows, row, rows, row, s_sx.at[i, k - 1], s_rx.at[i, x], peer(k))

    def last_send(i):
        return pair(cb.at[i], ct.at[i], gb.at[x], gt.at[x], s_sc.at[i], s_rc.at[x], place(y, z, i, c))

    def project(l, i, h, sh):
        out = dot(h, wq[l, sh])
        q = rounded(out[:, 0:128] + qb[sh, 0, l : l + 1]) * 0.125
        k = rounded(out[:, 128:256] + qb[sh, 1, l : l + 1])
        v = rounded(out[:, 256:384] + qb[sh, 2, l : l + 1])
        kr, vr, qr = swap(k), swap(v), swap(q)
        for hh in range(2):
            kk, vv = (k, vr) if hh == 0 else (kr, v)
            q0, q1 = (q, qr) if hh == 0 else (qr, q)
            m = msg.at[l, i, 2 * sh + hh]
            m[0:64] = jnp.where(low, kk[0:64], vv[0:64]).astype(BF16)
            m[64:96] = jnp.where(low32, q0[0:32], q1[32:64]).astype(BF16)
            msl[l, i, 2 * sh + hh] = jnp.concatenate(
                [jnp.where(low1, kk[64:65], vv[64:65]), jnp.where(low1, q0[64:65], 0.0)], axis=1
            )

    def send_shard(l, i, sh):
        for n in range(2):
            start(msg_send(l, i, 2 * sh + mod(n + zl, 2)))

    def attend(l):
        with scope("wait_msg"):

            @pl.loop(0, 16)
            def _(n):
                j = near(n)
                both_arrived(rk.at[l, j], rkl.at[l, j], s_rm.at[l, j])
                start(forward(l, j))

        low512 = iota((512, 128), 1) < 64
        low1024 = iota((1024, 128), 1) < 64

        def values(kv, n):
            return jnp.where(low1024[0:n], jnp.ones((n, 128), BF16), kv)

        with scope("attend_own"):
            q = rk[l, :, 64:96, :].astype(F32).reshape(512, 128)
            qq = jnp.concatenate([jnp.where(low512, q, 0.0), jnp.where(low512, swap(q), 0.0)], axis=0).astype(BF16)
            hot = (mod(iota((1024, 128), 0), 512) // 32 == iota((1024, 128), 1)).astype(BF16)
            slots = rkl[l].reshape(16, 256).astype(BF16)
            slots_q = jnp.concatenate([slots[:, 128:256], (row16 == lane16).astype(BF16)], axis=1)
            qx = jnp.concatenate([jnp.concatenate([qq, hot], axis=1), slots_q], axis=0)
            k1 = rk[l, :, 0:64, :].reshape(1024, 128)
            s1 = dot_t(qx, jnp.concatenate([k1, bd[...].reshape(1024, 128)], axis=1))
            top1 = jnp.max(s1, axis=1, keepdims=True)
            o1 = dot(jnp.exp((s1 - top1).astype(BF16)), values(k1, 1024))

        with scope("wait_pass"):

            @pl.loop(0, 16)
            def _(n):
                j = near(n)
                both_arrived(fk.at[l, j], fkl.at[l, j], s_rf.at[l, j])

        with scope("attend_passed"):
            ksl[0:16, 0:128] = slots[:, 0:128]
            ksl[16:32, 0:128] = fkl[l].reshape(16, 128).astype(BF16)
            ksl[:, 128:256] = bsl[...]
            k2 = fk[l].reshape(1024, 128)
            s2 = dot_t(qx, jnp.concatenate([k2, bf[...].reshape(1024, 128)], axis=1))
            s3 = dot_t(qx, ksl[...])
            top2 = jnp.maximum(jnp.max(s2, axis=1, keepdims=True), jnp.max(s3, axis=1, keepdims=True))
            o2 = dot(jnp.exp((s2 - top2).astype(BF16)), values(k2, 1024))
            o2 = o2 + dot(jnp.exp((s3 - top2).astype(BF16)), values(ksl[:, 0:128], 32))
            top = jnp.maximum(top1, top2)
            o = jnp.exp(top1 - top) * o1 + jnp.exp(top2 - top) * o2
            o = jnp.where(iota((1040, 128), 1) >= 64, o / swap(o), 0.0)
            ob[l] = jnp.where(low512, swap(o[0:512]), o[512:1024]).astype(BF16).reshape(16, 32, 128)
            obl[l] = rounded(o[1024:1040]).reshape(16, 1, 128)

        @pl.loop(0, 16)
        def _(n):
            start(result_send(l, near(15 - n)))

    def assemble(l, i):
        with scope("wait_result"):
            for h in range(4):
                both_arrived(ab.at[l, 4 * i + h], abl.at[l, 4 * i + h], s_rr.at[l, 4 * i + h])

        for m in range(2):
            u = ab[l, 4 * i + 2 * m].astype(F32)
            v = ab[l, 4 * i + 2 * m + 1].astype(F32)
            cols = slice(128 * m, 128 * m + 128)
            ag[l, i, x, 0:32, cols] = jnp.where(low32, u, swap(v)).astype(BF16)
            ag[l, i, x, 32:64, cols] = jnp.where(low32, swap(u), v).astype(BF16)
            agl[l, i, x, :, cols] = jnp.where(low1, swap(abl[l, 4 * i + 2 * m]), abl[l, 4 * i + 2 * m + 1])
        for k in (2, 1, 3):
            start(gather_send(l, i, k))

    def padded(rows, row):
        n = row.shape[1]
        tile = jnp.where(iota((16, n), 0) == 0, jnp.broadcast_to(row, (16, n)), 0.0)
        return jnp.concatenate([rows, tile.astype(rows.dtype)], axis=0)

    def mix(l, i):
        def arrive(k):
            xx = mod(x + k, 4)
            with scope("wait_gather"):
                both_arrived(ag.at[l, i, xx], agl.at[l, i, xx], s_rg.at[l, i, xx])

        def piece(k):
            xx = mod(x + k, 4)
            return dot(padded(ag[l, i, xx], agl[l, i, xx]), wo[l, pl.ds(2 * xx, 2)].reshape(256, D))

        with scope("out_proj"):
            first = padded(xs[l, i].astype(F32), xl[l, i]) + outb[l : l + 1] + piece(0)
        arrive(1)
        arrive(3)
        with scope("out_proj"):
            first = first + (piece(1) + piece(3))
        arrive(2)
        with scope("out_proj"):
            first = first + piece(2)
            fst[i] = first
            normed = layer_norm(first, ln2g[l : l + 1], ln2b[l : l + 1]).astype(BF16)
        with scope("mlp"):
            total = None
            for sh in range(2):
                v = dot(normed, w1[l, sh]) + b1[sh, l : l + 1]
                part = dot(gelu(v).astype(BF16), w2[l, sh])
                total = part if total is None else total + part
            pf[i] = total
            row = rounded(total[64:65])
            if l == 0:
                for xx in range(4):
                    pb[i, xx] = total[16 * xx : 16 * xx + 16].astype(BF16)
                    ps[i, xx] = row[:, 256 * xx : 256 * xx + 256]
            else:
                cb[i] = total[0:64].astype(BF16)
                ct[i] = row
        if l == 0:
            for k in (2, 1, 3):
                start(part_send(i, k))
        else:

            @pl.when(x != i)
            def _():
                start(last_send(i))

    def next_rows(i):
        with scope("wait_part"):
            for k in (1, 3, 2):
                xx = mod(x + k, 4)
                both_arrived(rb.at[i, xx], rs.at[i, xx], s_rp.at[i, xx])
        total = pf[i, rows_of(x)] + fst[i, rows_of(x)] + fc2b[0:1]
        row = pf[i, 64:65, cols_of(x)] + fst[i, 64:65, cols_of(x)] + fc2b[0:1, cols_of(x)]
        for k in (1, 2, 3):
            xx = mod(x + k, 4)
            total = total + rb[i, xx].astype(F32)
            row = row + rs[i, xx]
        xs[1, i, rows_of(x)] = total.astype(BF16)
        xl[1, i, :, cols_of(x)] = rounded(row)
        for k in (2, 1, 3):
            start(row_send(i, k))

    tq = jnp.zeros((16, 128), jnp.int32)
    td, tf, nd, nf = tq, tq, tq, tq
    for j in range(16):
        fd = 4 * (j // 4) + 2 * (1 - c) + (j % 4) // 2
        fp = 4 * (j // 4) + 2 * c + (j % 4) // 2
        tq = jnp.where(lane16 == j, time_ref[fd], tq)
        td = jnp.where(row16 == j, time_ref[fd], td)
        tf = jnp.where(row16 == j, time_ref[fp], tf)
        nd = jnp.where(row16 == j, cond_ref[fd], nd)
        nf = jnp.where(row16 == j, cond_ref[fp], nf)
    part = mod(row16, 2)
    bias_d = jnp.where(td <= tq, 0.0, NEG)
    bias_f = jnp.where(tf <= tq, 0.0, NEG)
    bsl[0:16] = jnp.where(part < nd, bias_d, NEG).astype(BF16)
    bsl[16:32] = jnp.where(part < nf, bias_f, NEG).astype(BF16)
    for j in range(16):
        bd[j] = jnp.broadcast_to(bias_d[j : j + 1], (64, 128)).astype(BF16)
        bf[j] = jnp.broadcast_to(bias_f[j : j + 1], (64, 128)).astype(BF16)

    with scope("first_rows"):
        lx().wait()
        r = iota((320, 520), 0)
        i, r = r // 80, mod(r, 80)
        want = jnp.where(r < 65, 65 * (2 * i + c) + r, -1)
        rows = dot((want == iota((320, 520), 1)).astype(BF16), xin[...])
        normed = layer_norm(rows, ln1g[0:1], ln1b[0:1]).astype(BF16)
        for i in ORDER:
            o = 80 * i
            xs[0, i] = rows[o : o + 64].astype(BF16)
            xl[0, i] = rows[o + 64 : o + 65]
            hb[i] = normed[o : o + 80]
        for j in range(3):
            lq(0, j).wait()
        for i in ORDER:
            project(0, i, hb[i], c)

    with scope("barrier"):
        pl.semaphore_wait(barrier, 20)

    rb0().start()
    for j in range(3):
        rq(0, j).start()
    for i in ORDER[:2]:
        send_shard(0, i, c)
    with scope("wait_wq"):
        arrived(qb.at[1 - c], s_rb.at[0])
        for j in range(3):
            rq_arrived(0, j)
    with scope("project0"):
        for i in ORDER:
            if i == ORDER[2]:
                for m in ORDER[2:]:
                    send_shard(0, m, c)
            project(0, i, hb[i], 1 - c)
            send_shard(0, i, 1 - c)
    wo_start(0)
    rb1().start()
    for l in range(LAYERS):
        r1(l).start()
        r2(l).start()
    for j in range(3):
        rq(1, j).start()

    for l in range(LAYERS):
        if l == 1:
            for j in range(3):
                lq(1, j).wait()
                rq_arrived(1, j)
            for i in ORDER:
                with scope("wait_row"):
                    for k in (1, 3, 2):
                        xx = mod(x + k, 4)
                        both_arrived(xs.at[1, i, rows_of(xx)], xl.at[1, i, :, cols_of(xx)], s_rx.at[i, xx])
                with scope("project1"):
                    h = padded(xs[1, i].astype(F32), xl[1, i])
                    h = layer_norm(h, ln1g[1:2], ln1b[1:2]).astype(BF16)
                    for sh in range(2):
                        project(1, i, h, sh)
                        send_shard(1, i, sh)
            wo_start(1)

        attend(l)

        with scope("assemble"):
            for i in ORDER[:2]:
                assemble(l, i)
        with scope("wait_wo"):
            lo(l).wait()
            for k in range(1, 4):
                i = mod(x + k, 4)
                arrived(wo.at[l, 2 * i + c], s_ro.at[l, i])
                wo_forward(l, k).start()
        with scope("assemble"):
            for i in ORDER[2:]:
                assemble(l, i)
        with scope("wait_w"):
            for k in range(4):
                i = mod(x + k, 4)
                arrived(wo.at[l, 2 * i + 1 - c], s_rfo.at[l, i])
            l1(l).wait()
            l2(l).wait()
            if l == 0:
                arrived(b1.at[1 - c], s_rb.at[1])
            arrived(w1.at[l, 1 - c], s_r1.at[l])
            arrived(w2.at[l, 1 - c], s_r2.at[l])
        if l == 0:
            for i in ORDER[:3]:
                mix(0, i)
            next_rows(ORDER[0])
            mix(0, ORDER[3])
            for i in ORDER[1:]:
                next_rows(i)
        else:
            for i in ORDER:
                mix(1, i)

    with scope("drain"):
        rb0().wait_send()
        rb1().wait_send()
        for i in range(4):
            for k in range(1, 4):
                leave(part_send(i, k))
                leave(row_send(i, k))
        for l in range(LAYERS):
            for j in range(3):
                rq(l, j).wait_send()
            r1(l).wait_send()
            r2(l).wait_send()
            for k in range(1, 4):
                wo_send(l, k).wait_send()
                for i in range(4):
                    leave(gather_send(l, i, k))
            for k in range(4):
                wo_forward(l, k).wait_send()

            @pl.loop(0, 16)
            def _(j):
                leave(msg_send(l, j // 4, mod(j, 4)))
                leave(forward(l, j))
                leave(result_send(l, j))

    last = pf[x, 0:64] + fst[x, 0:64] + fc2b[1:2]
    row = pf[x, 64:65] + fst[x, 64:65] + fc2b[1:2]
    for k in (1, 3, 2):
        xx = mod(x + k, 4)
        with scope("wait_last"):
            both_arrived(gb.at[xx], gt.at[xx], s_rc.at[xx])
        last = last + gb[xx].astype(F32)
        row = row + gt[xx]
    out_ref[0, 0:64] = last
    out_ref[0, 64:65] = row
    for i in range(4):

        @pl.when(x != i)
        def _():
            leave(last_send(i))


def shards(
    frames_in, frame_time, cond_count, ln1_gain, ln1_bias, qkv_weight, qkv_bias, out_weight, out_bias,
    ln2_gain, ln2_bias, fc1_weight, fc1_bias, fc2_weight, fc2_bias,
):
    any_ = pl.BlockSpec(memory_space=pl.ANY)
    vm = pl.BlockSpec(memory_space=VMEM)
    sm = pl.BlockSpec(memory_space=pltpu.SMEM)
    L = LAYERS
    rows = pl.pallas_call(
        kernel,
        name="layers",
        out_shape=jax.ShapeDtypeStruct((1, 65, D), F32),
        in_specs=[sm] * 2 + [vm] * 8 + [any_] * 5,
        out_specs=vm,
        scratch_shapes=[
            VMEM((520, D), BF16), VMEM((L, 4, 64, D), BF16), VMEM((L, 4, 1, D), F32), VMEM((4, 80, D), BF16),
            VMEM((L, 2, D, 384), BF16), VMEM((2, 3, L, 128), F32), VMEM((L, 8, 128, D), BF16),
            VMEM((L, 2, D, 512), BF16), VMEM((2, L, 512), F32), VMEM((L, 2, 512, D), BF16),
            VMEM((L, 4, 4, 96, 128), BF16), VMEM((L, 4, 4, 1, 256), F32),
            VMEM((L, 16, 96, 128), BF16), VMEM((L, 16, 1, 256), F32),
            VMEM((L, 16, 64, 128), BF16), VMEM((L, 16, 1, 128), F32), VMEM((32, 256), BF16),
            VMEM((L, 16, 32, 128), BF16), VMEM((L, 16, 1, 128), F32),
            VMEM((L, 16, 32, 128), BF16), VMEM((L, 16, 1, 128), F32),
            VMEM((L, 4, 4, 64, 256), BF16), VMEM((L, 4, 4, 1, 256), F32), VMEM((4, 80, D), F32), VMEM((4, 80, D), F32),
            VMEM((4, 4, 16, D), BF16), VMEM((4, 4, 1, 256), F32), VMEM((4, 4, 16, D), BF16), VMEM((4, 4, 1, 256), F32),
            VMEM((4, 64, D), BF16), VMEM((4, 1, D), F32), VMEM((4, 64, D), BF16), VMEM((4, 1, D), F32),
            VMEM((16, 64, 128), BF16), VMEM((16, 64, 128), BF16), VMEM((32, 128), BF16),
            DMA, DMA((L, 3)), DMA((L,)), DMA((L,)), DMA((L,)),
            DMA((L, 3)), DMA((L, 3)), DMA((2,)), DMA((2,)), DMA((L,)), DMA((L,)), DMA((L,)), DMA((L,)),
            DMA((L, 3)), DMA((L, 4)), DMA((L, 4)), DMA((L, 4)),
            DMA((L, 16, 2)), DMA((L, 16, 2)), DMA((L, 16, 2)), DMA((L, 16, 2)), DMA((L, 16, 2)), DMA((L, 16, 2)),
            DMA((L, 4, 3, 2)), DMA((L, 4, 4, 2)),
            DMA((4, 3, 2)), DMA((4, 4, 2)), DMA((4, 3, 2)), DMA((4, 4, 2)), DMA((4, 2)), DMA((4, 2)),
        ],
        compiler_params=pltpu.CompilerParams(
            collective_id=0, has_side_effects=True, vmem_limit_bytes=60 * 2**20
        ),
    )(
        frame_time, cond_count, ln1_gain, ln1_bias, ln2_gain, ln2_bias, out_bias, fc2_bias,
        jnp.transpose(qkv_bias, (1, 0, 2)), fc1_bias, frames_in, qkv_weight, out_weight, fc1_weight, fc2_weight,
    )
    return rows.astype(BF16)


def solution(mesh):
    in_specs = (
        P("tm", None, None), P(), P(), P(), P(),
        P(None, None, None, "tensor"), P(None, None, "tensor"), P(None, "tensor", None), P(), P(), P(),
        P(None, None, "tensor"), P(None, "tensor"), P(None, "tensor", None), P(),
    )
    return jax.shard_map(shards, mesh=mesh, in_specs=in_specs, out_specs=P("tm", "tensor", None), check_vma=False)
```

```python
import jax
import jax.numpy as jnp
from jax import lax
from jax.experimental import pallas as pl
from jax.experimental.pallas import tpu as pltpu
from jax.sharding import PartitionSpec as P

MESH = pl.DeviceIdType.MESH
LAYERS = 2
D = 1024
F32 = jnp.float32
BF16 = jnp.bfloat16
NEG = -1e30
VMEM = pltpu.VMEM
DMA = pltpu.SemaphoreType.DMA
scope = jax.named_scope


def mod(a, n):
    return lax.rem(a, n)


def place(y, z, x, c):
    return {"tm": y * 8 + z, "tensor": x * 2 + c}


def iota(shape, dim):
    return lax.broadcasted_iota(jnp.int32, shape, dim)


def layer_norm(rows, gain, bias):
    center = jnp.mean(rows, axis=-1, keepdims=True)
    moved = rows - center
    spread = jnp.mean(moved * moved, axis=-1, keepdims=True)
    return moved * lax.rsqrt(spread + 1e-06) * gain + bias


def gelu(v):
    return 0.5 * v * (1.0 + lax.erf(v * (0.5**0.5)))


def dot(a, b):
    return lax.dot_general(a, b, (((1,), (0,)), ((), ())), preferred_element_type=F32)


def dot_t(a, b):
    return lax.dot_general(a, b, (((1,), (1,)), ((), ())), preferred_element_type=F32)


def rounded(v):
    return v.astype(BF16).astype(F32)


def swap(v):
    return pltpu.roll(v, 64, 1)


def kernel(
    time_ref, cond_ref, ln1g, ln1b, ln2g, ln2b, outb, fc2b, qkvb, fc1b, x_hbm, wq_hbm, wo_hbm, w1_hbm, w2_hbm,
    out_ref,
    xin, xs, xl, hb, wq, qb, wo, w1, b1, w2, msg, msl, rk, rkl, fk, fkl, ksl, ob, obl, ab, abl, ag, agl, fst, pf,
    pb, ps, rb, rs, cb, ct, gb, gt, bd, bf, bsl,
    s_x, s_lq, s_lo, s_l1, s_l2,
    s_sq, s_rq, s_sb, s_rb, s_s1, s_r1, s_s2, s_r2,
    s_so, s_ro, s_sfo, s_rfo,
    s_sm, s_rm, s_sf, s_rf, s_sr, s_rr, s_sg, s_rg,
    s_sp, s_rp, s_sx, s_rx, s_sc, s_rc,
):
    p = lax.axis_index("tm")
    t = lax.axis_index("tensor")
    y, z = p // 8, mod(p, 8)
    x, c = t // 2, mod(t, 2)
    sib = place(y, z, x, 1 - c)
    zh, zl = z // 4, mod(z, 4)
    att = mod(y - zl + 4, 4)
    half = 1 - c
    slot = y * 4 + zl

    def peer(k):
        return place(y, z, mod(x + k, 4), c)

    def clip_home(i, h):
        return place(mod(i + h, 4), 4 * c + h, x, 1 - zh)

    def part_source(j):
        return place(j // 4, 4 * half + mod(j, 4), x, zh)

    def near(n):
        a = n // 4
        return mod(y + a + a // 2 * (5 - 2 * a), 4) * 4 + mod(zl + n, 4)

    def remote(src, dst, ssem, rsem, dev):
        return pltpu.make_async_remote_copy(
            src_ref=src, dst_ref=dst, send_sem=ssem, recv_sem=rsem, device_id=dev, device_id_type=MESH
        )

    def arrived(dst, rsem):
        remote(dst, dst, rsem, rsem, sib).wait_recv()

    def sent(src, ssem):
        remote(src, src, ssem, ssem, sib).wait_send()

    barrier = pltpu.get_barrier_semaphore()

    def greet(dev):
        pl.semaphore_signal(barrier, inc=1, device_id=dev, device_id_type=MESH)

    @pl.loop(0, 16)
    def _(j):
        greet(part_source(j))

    for k in range(1, 4):
        greet(peer(k))
    greet(sib)

    def lx():
        return pltpu.make_async_copy(x_hbm.at[0], xin, s_x)

    def lq(l, j):
        return pltpu.make_async_copy(wq_hbm.at[l, j], wq.at[l, c, :, pl.ds(128 * j, 128)], s_lq.at[l])

    def lq_wait(l):
        pltpu.make_async_copy(wq.at[l, c], wq.at[l, c], s_lq.at[l]).wait()

    def lo(l):
        return pltpu.make_async_copy(wo_hbm.at[l], wo.at[l, t], s_lo.at[l])

    def l1(l):
        return pltpu.make_async_copy(w1_hbm.at[l], w1.at[l, c], s_l1.at[l])

    def l2(l):
        return pltpu.make_async_copy(w2_hbm.at[l], w2.at[l, c], s_l2.at[l])

    lx().start()
    for l in range(LAYERS):
        for j in range(3):
            lq(l, j).start()
    for l in range(LAYERS):
        lo(l).start()
        l1(l).start()
        l2(l).start()

    qb[c] = qkvb[...]
    b1[c] = fc1b[...]

    low = iota((64, 128), 1) < 64
    low1 = iota((1, 128), 1) < 64
    low32 = iota((32, 128), 1) < 64
    row16 = iota((16, 128), 0)
    lane16 = iota((16, 128), 1)

    def rq(l, j):
        return remote(wq_hbm.at[l, j], wq.at[l, c, :, pl.ds(128 * j, 128)], s_sq.at[l], s_rq.at[l], sib)

    def rb0():
        return remote(qkvb, qb.at[c], s_sb.at[0], s_rb.at[0], sib)

    def rb1():
        return remote(fc1b, b1.at[c], s_sb.at[1], s_rb.at[1], sib)

    def r1(l):
        return remote(w1_hbm.at[l], w1.at[l, c], s_s1.at[l], s_r1.at[l], sib)

    def r2(l):
        return remote(w2_hbm.at[l], w2.at[l, c], s_s2.at[l], s_r2.at[l], sib)

    def wo_send(l, k):
        return remote(wo_hbm.at[l], wo.at[l, t], s_so.at[l], s_ro.at[l], peer(k))

    def wo_forward(l, k):
        xx = mod(x + k, 4)
        src = wo_hbm.at[l] if k == 0 else wo.at[l, 2 * xx + c]
        return remote(src, wo.at[l, 2 * xx + c], s_sfo.at[l], s_rfo.at[l], sib)

    def wo_start(l):
        for k in (2, 1, 3):
            wo_send(l, k).start()
        wo_forward(l, 0).start()

    def with_row(rows, slot_row, rows_to, slot_to, ssem, rsem, dev):
        return (
            remote(rows, rows_to, ssem.at[0], rsem.at[0], dev),
            remote(slot_row, slot_to, ssem.at[1], rsem.at[1], dev),
        )

    def start(copies):
        for copy in copies:
            copy.start()

    def both_arrived(rows, slot_row, rsem):
        arrived(rows, rsem.at[0])
        arrived(slot_row, rsem.at[1])

    def both_left(rows, slot_row, ssem):
        sent(rows, ssem.at[0])
        sent(slot_row, ssem.at[1])

    def msg_send(l, g, a, h):
        return with_row(
            msg.at[l, g, a, h], msl.at[l, g, a, h], rk.at[l, slot], rkl.at[l, slot], s_sm.at[l], s_rm.at[l, y],
            clip_home(2 * a + g, h),
        )

    def four(n):
        return pl.ds(pl.multiple_of(4 * n, 4), 4)

    def forward(l, n):
        return with_row(
            rk.at[l, four(n), pl.ds(0, 64)], rkl.at[l, four(n), :, pl.ds(0, 128)], fk.at[l, four(n)],
            fkl.at[l, four(n)], s_sf.at[l], s_rf.at[l], sib,
        )

    def result_send(l, j):
        me = 2 * mod(att, 2) + att // 2
        return with_row(
            ob.at[l, j], obl.at[l, j], ab.at[l, 4 * me + zl], abl.at[l, 4 * me + zl], s_sr.at[l], s_rr.at[l, me],
            part_source(j),
        )

    def gather_send(l, g, k):
        rows, row = ag.at[l, g, x], agl.at[l, g, x]
        return with_row(rows, row, rows, row, s_sg.at[l, g], s_rg.at[l, g, x], peer(k))

    def rows_of(xx):
        return pl.ds(pl.multiple_of(16 * xx, 16), 16)

    def cols_of(xx):
        return pl.ds(pl.multiple_of(256 * xx, 256), 256)

    def part_send(g, k):
        xx = mod(x + k, 4)
        return with_row(
            pb.at[g, xx], ps.at[g, xx], rb.at[g, 3 - k], rs.at[g, 3 - k], s_sp.at[g], s_rp.at[g], peer(k)
        )

    def row_send(g, k):
        rows, row = xs.at[1, g, :, rows_of(x)], xl.at[1, g, :, :, cols_of(x)]
        return with_row(rows, row, rows, row, s_sx.at[g], s_rx.at[g], peer(k))

    def last_send(g, a):
        i = 2 * a + g
        k = mod(x - i + 4, 4) - 1
        return with_row(cb.at[i], ct.at[i], gb.at[k], gt.at[k], s_sc, s_rc, place(y, z, i, c))

    def project(l, g, h, sh):
        out = dot(h, wq[l, sh])
        q = rounded(out[:, 0:128] + qb[sh, 0, l : l + 1]) * 0.125
        k = rounded(out[:, 128:256] + qb[sh, 1, l : l + 1])
        v = rounded(out[:, 256:384] + qb[sh, 2, l : l + 1])
        kr, vr, qr = swap(k), swap(v), swap(q)
        for a in range(2):
            o, r = 64 * a, 128 + a
            for hh in range(2):
                kk, vv = (k, vr) if hh == 0 else (kr, v)
                q0, q1 = (q, qr) if hh == 0 else (qr, q)
                m = msg.at[l, g, a, 2 * sh + hh]
                m[0:64] = jnp.where(low, kk[o : o + 64], vv[o : o + 64]).astype(BF16)
                m[64:96] = jnp.where(low32, q0[o : o + 32], q1[o + 32 : o + 64]).astype(BF16)
                msl[l, g, a, 2 * sh + hh] = jnp.concatenate(
                    [jnp.where(low1, kk[r : r + 1], vv[r : r + 1]), jnp.where(low1, q0[r : r + 1], 0.0)], axis=1
                )

    def send_shard(l, g, sh):
        for n in range(2):
            for a in range(2):
                start(msg_send(l, g, a, 2 * sh + mod(n + zl, 2)))

    def attend(l):
        with scope("wait_msg"):

            @pl.loop(0, 4)
            def _(a):
                n = mod(y + a + a // 2 * (5 - 2 * a), 4)
                both_arrived(rk.at[l, four(n)], rkl.at[l, four(n)], s_rm.at[l, n])
                start(forward(l, n))

        low512 = iota((512, 128), 1) < 64
        low1024 = iota((1024, 128), 1) < 64

        def values(kv, n):
            return jnp.where(low1024[0:n], jnp.ones((n, 128), BF16), kv)

        with scope("attend_own"):
            q = rk[l, :, 64:96, :].astype(F32).reshape(512, 128)
            qq = jnp.concatenate([jnp.where(low512, q, 0.0), jnp.where(low512, swap(q), 0.0)], axis=0).astype(BF16)
            hot = (mod(iota((1024, 128), 0), 512) // 32 == iota((1024, 128), 1)).astype(BF16)
            slots = rkl[l].reshape(16, 256).astype(BF16)
            slots_q = jnp.concatenate([slots[:, 128:256], (row16 == lane16).astype(BF16)], axis=1)
            qx = jnp.concatenate([jnp.concatenate([qq, hot], axis=1), slots_q], axis=0)
            k1 = rk[l, :, 0:64, :].reshape(1024, 128)
            s1 = dot_t(qx, jnp.concatenate([k1, bd[...].reshape(1024, 128)], axis=1))
            top1 = jnp.max(s1, axis=1, keepdims=True)
            o1 = dot(jnp.exp((s1 - top1).astype(BF16)), values(k1, 1024))

        with scope("wait_pass"):
            both_arrived(fk.at[l], fkl.at[l], s_rf.at[l])

        with scope("attend_passed"):
            ksl[0:16, 0:128] = slots[:, 0:128]
            ksl[16:32, 0:128] = fkl[l].reshape(16, 128).astype(BF16)
            ksl[:, 128:256] = bsl[...]
            k2 = fk[l].reshape(1024, 128)
            s2 = dot_t(qx, jnp.concatenate([k2, bf[...].reshape(1024, 128)], axis=1))
            s3 = dot_t(qx, ksl[...])
            top2 = jnp.maximum(jnp.max(s2, axis=1, keepdims=True), jnp.max(s3, axis=1, keepdims=True))
            top = jnp.maximum(top1, top2)
            o = jnp.exp(top1 - top) * o1 + dot(jnp.exp((s2 - top).astype(BF16)), values(k2, 1024))
            o = o + dot(jnp.exp((s3 - top).astype(BF16)), values(ksl[:, 0:128], 32))
            lo_, hi_, sl = o[0:512], o[512:1024], o[1024:1040]
            mixed = jnp.where(low512, swap(lo_), hi_) / jnp.where(low512, lo_, swap(hi_))
            ob[l] = mixed.astype(BF16).reshape(16, 32, 128)
            obl[l] = jnp.where(lane16 >= 64, rounded(sl / swap(sl)), 0.0).reshape(16, 1, 128)

        @pl.loop(0, 16)
        def _(n):
            start(result_send(l, near(15 - n)))

    def assemble(l, g):
        for a in range(2):
            q = 4 * (2 * g + a)
            with scope("wait_result"):
                both_arrived(ab.at[l, pl.ds(q, 4)], abl.at[l, pl.ds(q, 4)], s_rr.at[l, 2 * g + a])

            for m in range(2):
                u = ab[l, q + 2 * m].astype(F32)
                v = ab[l, q + 2 * m + 1].astype(F32)
                cols = slice(128 * m, 128 * m + 128)
                ag[l, g, x, a, 0:32, cols] = jnp.where(low32, u, swap(v)).astype(BF16)
                ag[l, g, x, a, 32:64, cols] = jnp.where(low32, swap(u), v).astype(BF16)
                agl[l, g, x, a, :, cols] = jnp.where(low1, swap(abl[l, q + 2 * m]), abl[l, q + 2 * m + 1])
        for k in (2, 1, 3):
            start(gather_send(l, g, k))

    def stacked(blocks, rows):
        n = rows[0].shape[1]
        which = iota((16, n), 0)
        tile = jnp.where(which == 0, jnp.broadcast_to(rows[0], (16, n)), 0.0)
        tile = jnp.where(which == 1, jnp.broadcast_to(rows[1], (16, n)), tile)
        return jnp.concatenate([*blocks, tile.astype(blocks[0].dtype)], axis=0)

    def stream(l, g):
        return stacked([xs[l, g, a].astype(F32) for a in range(2)], [xl[l, g, a] for a in range(2)])

    def mix(l, g):
        def arrive(k):
            xx = mod(x + k, 4)
            with scope("wait_gather"):
                both_arrived(ag.at[l, g, xx], agl.at[l, g, xx], s_rg.at[l, g, xx])

        def piece(k):
            xx = mod(x + k, 4)
            attended = stacked([ag[l, g, xx, a] for a in range(2)], [agl[l, g, xx, a] for a in range(2)])
            return dot(attended, wo[l, pl.ds(2 * xx, 2)].reshape(256, D))

        with scope("out_proj"):
            first = stream(l, g) + outb[l : l + 1] + piece(0)
        arrive(1)
        arrive(3)
        with scope("out_proj"):
            first = first + (piece(1) + piece(3))
        arrive(2)
        with scope("out_proj"):
            first = first + piece(2)
            fst[g] = first
            normed = layer_norm(first, ln2g[l : l + 1], ln2b[l : l + 1]).astype(BF16)
        with scope("mlp"):
            total = None
            for sh in range(2):
                v = dot(normed, w1[l, sh]) + b1[sh, l : l + 1]
                part = dot(gelu(v).astype(BF16), w2[l, sh])
                total = part if total is None else total + part
            pf[g] = total
            for a in range(2):
                mine = total[64 * a : 64 * a + 64].astype(BF16)
                row = rounded(total[128 + a : 129 + a])
                if l == 0:
                    for xx in range(4):
                        pb[g, xx, a] = mine[16 * xx : 16 * xx + 16]
                        ps[g, xx, a] = row[:, 256 * xx : 256 * xx + 256]
                else:
                    cb[2 * a + g] = mine
                    ct[2 * a + g] = row
        if l == 0:
            for k in (2, 1, 3):
                start(part_send(g, k))
        else:
            for a in range(2):

                @pl.when(x != 2 * a + g)
                def _():
                    start(last_send(g, a))

    def next_rows(g):
        with scope("wait_part"):
            both_arrived(rb.at[g], rs.at[g], s_rp.at[g])
        for a in range(2):
            own = pl.ds(pl.multiple_of(64 * a + 16 * x, 16), 16)
            row = pl.ds(128 + a, 1)
            total = pf[g, own] + fst[g, own] + fc2b[0:1]
            slot_row = pf[g, row, cols_of(x)] + fst[g, row, cols_of(x)] + fc2b[0:1, cols_of(x)]
            for k in range(3):
                total = total + rb[g, k, a].astype(F32)
                slot_row = slot_row + rs[g, k, a]
            xs[1, g, a, rows_of(x)] = total.astype(BF16)
            xl[1, g, a, :, cols_of(x)] = rounded(slot_row)
        for k in (2, 1, 3):
            start(row_send(g, k))

    tq = jnp.zeros((16, 128), jnp.int32)
    td, tf, nd, nf = tq, tq, tq, tq
    for j in range(16):
        fd = 4 * (j // 4) + 2 * (1 - c) + (j % 4) // 2
        fp = 4 * (j // 4) + 2 * c + (j % 4) // 2
        tq = jnp.where(lane16 == j, time_ref[fd], tq)
        td = jnp.where(row16 == j, time_ref[fd], td)
        tf = jnp.where(row16 == j, time_ref[fp], tf)
        nd = jnp.where(row16 == j, cond_ref[fd], nd)
        nf = jnp.where(row16 == j, cond_ref[fp], nf)
    part = mod(row16, 2)
    bias_d = jnp.where(td <= tq, 0.0, NEG)
    bias_f = jnp.where(tf <= tq, 0.0, NEG)
    bsl[0:16] = jnp.where(part < nd, bias_d, NEG).astype(BF16)
    bsl[16:32] = jnp.where(part < nf, bias_f, NEG).astype(BF16)
    for j in range(16):
        bd[j] = jnp.broadcast_to(bias_d[j : j + 1], (64, 128)).astype(BF16)
        bf[j] = jnp.broadcast_to(bias_f[j : j + 1], (64, 128)).astype(BF16)

    with scope("first_rows"):
        lx().wait()
        r = iota((288, 520), 0)
        g, r = r // 144, mod(r, 144)
        i = jnp.where(r < 128, r // 64, r - 128) * 2 + g
        want = jnp.where(r < 130, 65 * (2 * i + c) + jnp.where(r < 128, mod(r, 64), 64), -1)
        rows = dot((want == iota((288, 520), 1)).astype(BF16), xin[...])
        normed = layer_norm(rows, ln1g[0:1], ln1b[0:1]).astype(BF16)
        for g in range(2):
            o = 144 * g
            for a in range(2):
                xs[0, g, a] = rows[o + 64 * a : o + 64 * a + 64].astype(BF16)
                xl[0, g, a] = rows[o + 128 + a : o + 129 + a]
            hb[g] = normed[o : o + 144]
        lq_wait(0)
        for g in range(2):
            project(0, g, hb[g], c)

    with scope("barrier"):
        pl.semaphore_wait(barrier, 20)

    rb0().start()
    for j in range(3):
        rq(0, j).start()
    send_shard(0, 0, c)
    with scope("wait_wq"):
        arrived(qb.at[1 - c], s_rb.at[0])
        arrived(wq.at[0, 1 - c], s_rq.at[0])
    with scope("project0"):
        for g in range(2):
            if g == 1:
                send_shard(0, 1, c)
            project(0, g, hb[g], 1 - c)
            send_shard(0, g, 1 - c)
    wo_start(0)
    rb1().start()
    for l in range(LAYERS):
        r1(l).start()
        r2(l).start()
    for j in range(3):
        rq(1, j).start()

    for l in range(LAYERS):
        if l == 1:
            lq_wait(1)
            arrived(wq.at[1, 1 - c], s_rq.at[1])
            for g in range(2):
                with scope("wait_row"):
                    both_arrived(xs.at[1, g, :, pl.ds(0, 48)], xl.at[1, g, :, :, pl.ds(0, 768)], s_rx.at[g])
                with scope("project1"):
                    h = layer_norm(stream(1, g), ln1g[1:2], ln1b[1:2]).astype(BF16)
                    for sh in range(2):
                        project(1, g, h, sh)
                        send_shard(1, g, sh)
            wo_start(1)

        attend(l)

        with scope("assemble"):
            assemble(l, 0)
        with scope("wait_wo"):
            lo(l).wait()
            arrived(wo.at[l, pl.ds(0, 3)], s_ro.at[l])
            for k in range(1, 4):
                wo_forward(l, k).start()
        with scope("assemble"):
            assemble(l, 1)
        with scope("wait_w"):
            arrived(wo.at[l, pl.ds(0, 4)], s_rfo.at[l])
            l1(l).wait()
            l2(l).wait()
            if l == 0:
                arrived(b1.at[1 - c], s_rb.at[1])
            arrived(w1.at[l, 1 - c], s_r1.at[l])
            arrived(w2.at[l, 1 - c], s_r2.at[l])
        for g in range(2):
            mix(l, g)
        if l == 0:
            for g in range(2):
                next_rows(g)

    with scope("drain"):
        rb0().wait_send()
        rb1().wait_send()
        for g in range(2):
            both_left(pb.at[g, pl.ds(0, 3)], ps.at[g, pl.ds(0, 3)], s_sp.at[g])
            both_left(xs.at[1, g, :, pl.ds(0, 48)], xl.at[1, g, :, :, pl.ds(0, 768)], s_sx.at[g])
        for l in range(LAYERS):
            sent(wq.at[l, 0], s_sq.at[l])
            r1(l).wait_send()
            r2(l).wait_send()
            sent(wo.at[l, pl.ds(0, 3)], s_so.at[l])
            sent(wo.at[l, pl.ds(0, 4)], s_sfo.at[l])
            for g in range(2):
                both_left(ag.at[l, g, pl.ds(0, 3)], agl.at[l, g, pl.ds(0, 3)], s_sg.at[l, g])
            both_left(msg.at[l], msl.at[l], s_sm.at[l])
            both_left(fk.at[l], fkl.at[l], s_sf.at[l])
            both_left(ob.at[l], obl.at[l], s_sr.at[l])

    gx, ax = mod(x, 2), x // 2
    own, own_row = pl.ds(pl.multiple_of(64 * ax, 64), 64), pl.ds(128 + ax, 1)
    last = pf[gx, own] + fst[gx, own] + fc2b[1:2]
    row = pf[gx, own_row] + fst[gx, own_row] + fc2b[1:2]
    with scope("wait_last"):
        both_arrived(gb, gt, s_rc)
    for k in range(3):
        last = last + gb[k].astype(F32)
        row = row + gt[k]
    out_ref[0, 0:64] = last
    out_ref[0, 64:65] = row
    with scope("leave"):
        both_left(cb.at[pl.ds(0, 3)], ct.at[pl.ds(0, 3)], s_sc)


def shards(
    frames_in, frame_time, cond_count, ln1_gain, ln1_bias, qkv_weight, qkv_bias, out_weight, out_bias,
    ln2_gain, ln2_bias, fc1_weight, fc1_bias, fc2_weight, fc2_bias,
):
    any_ = pl.BlockSpec(memory_space=pl.ANY)
    vm = pl.BlockSpec(memory_space=VMEM)
    sm = pl.BlockSpec(memory_space=pltpu.SMEM)
    L = LAYERS
    rows = pl.pallas_call(
        kernel,
        name="layers",
        out_shape=VMEM((1, 65, D), F32),
        in_specs=[sm] * 2 + [vm] * 8 + [any_] * 5,
        out_specs=vm,
        scratch_shapes=[
            VMEM((520, D), BF16), VMEM((L, 2, 2, 64, D), BF16), VMEM((L, 2, 2, 1, D), F32), VMEM((2, 144, D), BF16),
            VMEM((L, 2, D, 384), BF16), VMEM((2, 3, L, 128), F32), VMEM((L, 8, 128, D), BF16),
            VMEM((L, 2, D, 512), BF16), VMEM((2, L, 512), F32), VMEM((L, 2, 512, D), BF16),
            VMEM((L, 2, 2, 4, 96, 128), BF16), VMEM((L, 2, 2, 4, 1, 256), F32),
            VMEM((L, 16, 96, 128), BF16), VMEM((L, 16, 1, 256), F32),
            VMEM((L, 16, 64, 128), BF16), VMEM((L, 16, 1, 128), F32), VMEM((32, 256), BF16),
            VMEM((L, 16, 32, 128), BF16), VMEM((L, 16, 1, 128), F32),
            VMEM((L, 16, 32, 128), BF16), VMEM((L, 16, 1, 128), F32),
            VMEM((L, 2, 4, 2, 64, 256), BF16), VMEM((L, 2, 4, 2, 1, 256), F32),
            VMEM((2, 144, D), F32), VMEM((2, 144, D), F32),
            VMEM((2, 4, 2, 16, D), BF16), VMEM((2, 4, 2, 1, 256), F32),
            VMEM((2, 3, 2, 16, D), BF16), VMEM((2, 3, 2, 1, 256), F32),
            VMEM((4, 64, D), BF16), VMEM((4, 1, D), F32), VMEM((3, 64, D), BF16), VMEM((3, 1, D), F32),
            VMEM((16, 64, 128), BF16), VMEM((16, 64, 128), BF16), VMEM((32, 128), BF16),
            DMA, DMA((L,)), DMA((L,)), DMA((L,)), DMA((L,)),
            DMA((L,)), DMA((L,)), DMA((2,)), DMA((2,)), DMA((L,)), DMA((L,)), DMA((L,)), DMA((L,)),
            DMA((L,)), DMA((L,)), DMA((L,)), DMA((L,)),
            DMA((L, 2)), DMA((L, 4, 2)), DMA((L, 2)), DMA((L, 2)), DMA((L, 2)), DMA((L, 4, 2)),
            DMA((L, 2, 2)), DMA((L, 2, 4, 2)),
            DMA((2, 2)), DMA((2, 2)), DMA((2, 2)), DMA((2, 2)), DMA((2,)), DMA((2,)),
        ],
        compiler_params=pltpu.CompilerParams(
            collective_id=0, has_side_effects=True, vmem_limit_bytes=60 * 2**20
        ),
    )(
        frame_time, cond_count, ln1_gain, ln1_bias, ln2_gain, ln2_bias, out_bias, fc2_bias,
        jnp.transpose(qkv_bias, (1, 0, 2)), fc1_bias, frames_in, qkv_weight, out_weight, fc1_weight, fc2_weight,
    )
    return rows.astype(BF16)


def solution(mesh):
    in_specs = (
        P("tm", None, None), P(), P(), P(), P(),
        P(None, None, None, "tensor"), P(None, None, "tensor"), P(None, "tensor", None), P(), P(), P(),
        P(None, None, "tensor"), P(None, "tensor"), P(None, "tensor", None), P(),
    )
    return jax.shard_map(shards, mesh=mesh, in_specs=in_specs, out_specs=P("tm", "tensor", None), check_vma=False)
```

```python
import jax
import jax.numpy as jnp
from jax import lax
from jax.experimental import pallas as pl
from jax.experimental.pallas import tpu as pltpu
from jax.sharding import PartitionSpec as P

MESH = pl.DeviceIdType.MESH
LAYERS = 2
D = 1024
F32 = jnp.float32
BF16 = jnp.bfloat16
NEG = -1e30
VMEM = pltpu.VMEM
DMA = pltpu.SemaphoreType.DMA
scope = jax.named_scope


def mod(a, n):
    return lax.rem(a, n)


def place(y, z, x, c):
    return {"tm": y * 8 + z, "tensor": x * 2 + c}


def iota(shape, dim):
    return lax.broadcasted_iota(jnp.int32, shape, dim)


def layer_norm(rows, gain, bias):
    center = jnp.mean(rows, axis=-1, keepdims=True)
    moved = rows - center
    spread = jnp.mean(moved * moved, axis=-1, keepdims=True)
    return moved * lax.rsqrt(spread + 1e-06) * gain + bias


def gelu(v):
    return 0.5 * v * (1.0 + lax.erf(v * (0.5**0.5)))


def dot(a, b):
    return lax.dot_general(a, b, (((1,), (0,)), ((), ())), preferred_element_type=F32)


def dot_t(a, b):
    return lax.dot_general(a, b, (((1,), (1,)), ((), ())), preferred_element_type=F32)


def rounded(v):
    return v.astype(BF16).astype(F32)


def swap(v):
    return pltpu.roll(v, 64, 1)


def kernel(
    time_hbm, cond_hbm, ln1g_hbm, ln1b_hbm, ln2g_hbm, ln2b_hbm, outb_hbm, fc2b_hbm, qkvb_hbm, fc1b_hbm,
    x_hbm, wq_hbm, wo_hbm, w1_hbm, w2_hbm,
    out_ref,
    time_ref, cond_ref, ln1g, ln1b, ln2g, ln2b, outb, fc2b,
    xin, xs, xl, hb, wq, qb, wo, w1, b1, w2, msg, msl, rk, rkl, fk, fkl, ksl, ob, obl, ab, abl, ag, agl, fst, pf,
    pb, ps, rb, rs, cb, ct, gb, gt, bd, bf, bsl, qx, ruler,
    s_t, s_p, s_x, s_lq, s_lo, s_l1, s_l2,
    s_sq, s_rq, s_sb, s_rb, s_s1, s_r1, s_s2, s_r2,
    s_so, s_ro, s_sfo, s_rfo,
    s_sm, s_rm, s_sf, s_rf, s_sr, s_rr, s_sg, s_rg,
    s_sp, s_rp, s_sx, s_rx, s_sc, s_rc,
):
    p = lax.axis_index("tm")
    t = lax.axis_index("tensor")
    y, z = p // 8, mod(p, 8)
    x, c = t // 2, mod(t, 2)
    sib = place(y, z, x, 1 - c)
    zh, zl = z // 4, mod(z, 4)
    att = mod(y - zl + 4, 4)
    half = 1 - c
    slot = y * 4 + zl

    def peer(k):
        return place(y, z, mod(x + k, 4), c)

    def clip_home(i, h):
        return place(mod(i + h, 4), 4 * c + h, x, 1 - zh)

    def part_source(j):
        return place(j // 4, 4 * half + mod(j, 4), x, zh)

    def near(n):
        a = n // 4
        return mod(y + a + a // 2 * (5 - 2 * a), 4) * 4 + mod(zl + n, 4)

    def remote(src, dst, ssem, rsem, dev):
        return pltpu.make_async_remote_copy(
            src_ref=src, dst_ref=dst, send_sem=ssem, recv_sem=rsem, device_id=dev, device_id_type=MESH
        )

    def arrived(dst, rsem):
        remote(dst, dst, rsem, rsem, sib).wait_recv()

    def sent(src, ssem):
        remote(src, src, ssem, ssem, sib).wait_send()

    barrier = pltpu.get_barrier_semaphore()

    def greet(dev):
        pl.semaphore_signal(barrier, inc=1, device_id=dev, device_id_type=MESH)

    @pl.loop(0, 16)
    def _(j):
        greet(part_source(j))

    for k in range(1, 4):
        greet(peer(k))
    greet(sib)

    def lx():
        return pltpu.make_async_copy(x_hbm.at[0], xin, s_x)

    def lq(l, j):
        return pltpu.make_async_copy(wq_hbm.at[l, j], wq.at[l, c, :, pl.ds(128 * j, 128)], s_lq.at[l])

    def lq_wait(l):
        pltpu.make_async_copy(wq.at[l, c], wq.at[l, c], s_lq.at[l]).wait()

    def lo(l):
        return pltpu.make_async_copy(wo_hbm.at[l], wo.at[l, t], s_lo.at[l])

    def l1(l):
        return pltpu.make_async_copy(w1_hbm.at[l], w1.at[l, c], s_l1.at[l])

    def l2(l):
        return pltpu.make_async_copy(w2_hbm.at[l], w2.at[l, c], s_l2.at[l])

    lx().start()
    params = (
        (ln1g_hbm, ln1g), (ln1b_hbm, ln1b), (ln2g_hbm, ln2g), (ln2b_hbm, ln2b), (outb_hbm, outb), (fc2b_hbm, fc2b),
        (qkvb_hbm, qb.at[c]), (fc1b_hbm, b1.at[c]),
    )
    for src, dst in params:
        pltpu.make_async_copy(src, dst, s_p).start()
    copy_t = pltpu.make_async_copy(time_hbm, time_ref, s_t.at[0])
    copy_c = pltpu.make_async_copy(cond_hbm, cond_ref, s_t.at[1])
    copy_t.start()
    copy_c.start()
    for j in range(3):
        lq(0, j).start()

    low = iota((64, 128), 1) < 64
    low1 = iota((1, 128), 1) < 64
    low32 = iota((32, 128), 1) < 64
    row16 = iota((16, 128), 0)
    lane16 = iota((16, 128), 1)

    def rq(l, j):
        return remote(wq_hbm.at[l, j], wq.at[l, c, :, pl.ds(128 * j, 128)], s_sq.at[l], s_rq.at[l], sib)

    def rb0():
        return remote(qkvb_hbm, qb.at[c], s_sb.at[0], s_rb.at[0], sib)

    def rb1():
        return remote(fc1b_hbm, b1.at[c], s_sb.at[1], s_rb.at[1], sib)

    def r1(l):
        return remote(w1_hbm.at[l], w1.at[l, c], s_s1.at[l], s_r1.at[l], sib)

    def r2(l):
        return remote(w2_hbm.at[l], w2.at[l, c], s_s2.at[l], s_r2.at[l], sib)

    def wo_send(l, k):
        return remote(wo_hbm.at[l], wo.at[l, t], s_so.at[l], s_ro.at[l], peer(k))

    def wo_forward(l, k):
        xx = mod(x + k, 4)
        src = wo_hbm.at[l] if k == 0 else wo.at[l, 2 * xx + c]
        return remote(src, wo.at[l, 2 * xx + c], s_sfo.at[l], s_rfo.at[l], sib)

    def wo_start(l):
        for k in (2, 1, 3):
            wo_send(l, k).start()
        wo_forward(l, 0).start()

    def with_row(rows, slot_row, rows_to, slot_to, ssem, rsem, dev):
        return remote(rows, rows_to, ssem, rsem, dev), remote(slot_row, slot_to, ssem, rsem, dev)

    def start(copies):
        for copy in copies:
            copy.start()

    def came(kib, rsem):
        arrived(ruler.at[pl.ds(0, kib)], rsem)

    def left(kib, ssem):
        sent(ruler.at[pl.ds(0, kib)], ssem)

    def msg_send(l, g, a, h):
        return with_row(
            msg.at[l, g, a, h], msl.at[l, g, a, h], rk.at[l, slot], rkl.at[l, slot], s_sm.at[l], s_rm.at[l, y],
            clip_home(2 * a + g, h),
        )

    def four(n):
        return pl.ds(pl.multiple_of(4 * n, 4), 4)

    def forward(l, n):
        return with_row(
            rk.at[l, four(n), pl.ds(0, 64)], rkl.at[l, four(n), :, pl.ds(0, 128)], fk.at[l, four(n)],
            fkl.at[l, four(n)], s_sf.at[l], s_rf.at[l], sib,
        )

    def result_send(l, j):
        me = 2 * mod(att, 2) + att // 2
        return with_row(
            ob.at[l, j], obl.at[l, j], ab.at[l, 4 * me + zl], abl.at[l, 4 * me + zl], s_sr.at[l], s_rr.at[l, me],
            part_source(j),
        )

    def gather_send(l, g, k):
        rows, row = ag.at[l, g, x], agl.at[l, g, x]
        return with_row(rows, row, rows, row, s_sg.at[l, g], s_rg.at[l, g, x], peer(k))

    def rows_of(xx):
        return pl.ds(pl.multiple_of(16 * xx, 16), 16)

    def cols_of(xx):
        return pl.ds(pl.multiple_of(256 * xx, 256), 256)

    def part_send(g, k):
        xx = mod(x + k, 4)
        return with_row(
            pb.at[g, xx], ps.at[g, xx], rb.at[g, 3 - k], rs.at[g, 3 - k], s_sp.at[g], s_rp.at[g], peer(k)
        )

    def row_send(g, k):
        rows, row = xs.at[1, g, :, rows_of(x)], xl.at[1, g, :, :, cols_of(x)]
        return with_row(rows, row, rows, row, s_sx.at[g], s_rx.at[g], peer(k))

    def last_send(g, a):
        i = 2 * a + g
        k = mod(x - i + 4, 4) - 1
        return with_row(cb.at[i], ct.at[i], gb.at[k], gt.at[k], s_sc, s_rc, place(y, z, i, c))

    def project(l, g, h, sh):
        out = dot(h, wq[l, sh])
        q = rounded(out[:, 0:128] + qb[sh, 0, l : l + 1]) * 0.125
        k = rounded(out[:, 128:256] + qb[sh, 1, l : l + 1])
        v = rounded(out[:, 256:384] + qb[sh, 2, l : l + 1])
        kr, vr, qr = swap(k), swap(v), swap(q)
        for a in range(2):
            o, r = 64 * a, 128 + a
            for hh in range(2):
                kk, vv = (k, vr) if hh == 0 else (kr, v)
                q0, q1 = (q, qr) if hh == 0 else (qr, q)
                m = msg.at[l, g, a, 2 * sh + hh]
                m[0:64] = jnp.where(low, kk[o : o + 64], vv[o : o + 64]).astype(BF16)
                m[64:96] = jnp.where(low32, q0[o : o + 32], q1[o + 32 : o + 64]).astype(BF16)
                msl[l, g, a, 2 * sh + hh] = jnp.concatenate(
                    [jnp.where(low1, kk[r : r + 1], vv[r : r + 1]), jnp.where(low1, q0[r : r + 1], 0.0)], axis=1
                )

    def send_shard(l, g, sh):
        for n in range(2):
            for a in range(2):
                start(msg_send(l, g, a, 2 * sh + mod(n + zl, 2)))

    def attend(l):
        with scope("wait_msg"):

            @pl.loop(0, 4)
            def _(a):
                n = mod(y + a + a // 2 * (5 - 2 * a), 4)
                came(4 * 25, s_rm.at[l, n])
                start(forward(l, n))

        low512 = iota((512, 128), 1) < 64
        low1024 = iota((1024, 128), 1) < 64

        def values(kv, n):
            return jnp.where(low1024[0:n], jnp.ones((n, 128), BF16), kv)

        def queries():
            q = rk[l, :, 64:96, :].astype(F32).reshape(512, 128)
            qq = jnp.concatenate([jnp.where(low512, q, 0.0), jnp.where(low512, swap(q), 0.0)], axis=0).astype(BF16)
            hot = (mod(iota((1024, 128), 0), 512) // 32 == iota((1024, 128), 1)).astype(BF16)
            slots = rkl[l].reshape(16, 256).astype(BF16)
            ksl[0:16, 0:128] = slots[:, 0:128]
            slots_q = jnp.concatenate([slots[:, 128:256], (row16 == lane16).astype(BF16)], axis=1)
            qx[...] = jnp.concatenate([jnp.concatenate([qq, hot], axis=1), slots_q], axis=0)

        def scored(k, bias):
            return dot_t(qx[...], jnp.concatenate([k, bias[...].reshape(1024, 128)], axis=1))

        def top_of(s):
            return jnp.max(s, axis=1, keepdims=True)

        def weighted(s, top, kv, n):
            return dot(jnp.exp((s - top).astype(BF16)), values(kv, n))

        def own_keys():
            return rk[l, :, 0:64, :].reshape(1024, 128)

        def passed_keys():
            return fk[l].reshape(1024, 128)

        def slot_keys():
            ksl[16:32, 0:128] = fkl[l].reshape(16, 128).astype(BF16)
            ksl[:, 128:256] = bsl[...]
            return dot_t(qx[...], ksl[...])

        def finish(o):
            lo_, hi_, sl = o[0:512], o[512:1024], o[1024:1040]
            mixed = jnp.where(low512, swap(lo_), hi_) / jnp.where(low512, lo_, swap(hi_))
            ob[l] = mixed.astype(BF16).reshape(16, 32, 128)
            obl[l] = jnp.where(lane16 >= 64, rounded(sl / swap(sl)), 0.0).reshape(16, 1, 128)

        with scope("queries"):
            queries()

        @pl.when(half == zh)
        def _():
            k1 = own_keys()
            s1 = scored(k1, bd)
            top1 = top_of(s1)
            o1 = weighted(s1, top1, k1, 1024)
            came(264, s_rf.at[l])
            k2 = passed_keys()
            s2, s3 = scored(k2, bf), slot_keys()
            top = jnp.maximum(jnp.maximum(top_of(s2), top_of(s3)), top1)
            o = jnp.exp(top1 - top) * o1 + weighted(s2, top, k2, 1024)
            finish(o + weighted(s3, top, ksl[:, 0:128], 32))

        @pl.when(half != zh)
        def _():
            came(264, s_rf.at[l])
            k1, k2 = own_keys(), passed_keys()
            s1, s3 = scored(k1, bd), slot_keys()
            top1 = jnp.maximum(top_of(s1), top_of(s3))
            o1 = weighted(s1, top1, k1, 1024) + weighted(s3, top1, ksl[:, 0:128], 32)
            s2 = scored(k2, bf)
            top2 = top_of(s2)
            o2 = weighted(s2, top2, k2, 1024)
            top = jnp.maximum(top1, top2)
            finish(jnp.exp(top1 - top) * o1 + jnp.exp(top2 - top) * o2)

        @pl.loop(0, 16)
        def _(n):
            start(result_send(l, near(15 - n)))

    def assemble(l, g):
        for a in range(2):
            q = 4 * (2 * g + a)
            with scope("wait_result"):
                came(34, s_rr.at[l, 2 * g + a])

            for m in range(2):
                u = ab[l, q + 2 * m].astype(F32)
                v = ab[l, q + 2 * m + 1].astype(F32)
                cols = slice(128 * m, 128 * m + 128)
                ag[l, g, x, a, 0:32, cols] = jnp.where(low32, u, swap(v)).astype(BF16)
                ag[l, g, x, a, 32:64, cols] = jnp.where(low32, swap(u), v).astype(BF16)
                agl[l, g, x, a, :, cols] = jnp.where(low1, swap(abl[l, q + 2 * m]), abl[l, q + 2 * m + 1])
        for k in (2, 1, 3):
            start(gather_send(l, g, k))

    def stacked(blocks, rows):
        n = rows[0].shape[1]
        which = iota((16, n), 0)
        tile = jnp.where(which == 0, jnp.broadcast_to(rows[0], (16, n)), 0.0)
        tile = jnp.where(which == 1, jnp.broadcast_to(rows[1], (16, n)), tile)
        return jnp.concatenate([*blocks, tile.astype(blocks[0].dtype)], axis=0)

    def stream(l, g):
        return stacked([xs[l, g, a].astype(F32) for a in range(2)], [xl[l, g, a] for a in range(2)])

    def mix(l, g):
        def arrive(k):
            xx = mod(x + k, 4)
            with scope("wait_gather"):
                came(66, s_rg.at[l, g, xx])

        def piece(k):
            xx = mod(x + k, 4)
            attended = stacked([ag[l, g, xx, a] for a in range(2)], [agl[l, g, xx, a] for a in range(2)])
            return dot(attended, wo[l, pl.ds(2 * xx, 2)].reshape(256, D))

        with scope("out_proj"):
            first = stream(l, g) + outb[l : l + 1] + piece(0)
        arrive(1)
        arrive(3)
        with scope("out_proj"):
            first = first + (piece(1) + piece(3))
        arrive(2)
        with scope("out_proj"):
            first = first + piece(2)
            fst[g] = first
            normed = layer_norm(first, ln2g[l : l + 1], ln2b[l : l + 1]).astype(BF16)
        with scope("mlp"):
            total = None
            for sh in range(2):
                v = dot(normed, w1[l, sh]) + b1[sh, l : l + 1]
                part = dot(gelu(v).astype(BF16), w2[l, sh])
                total = part if total is None else total + part
            pf[g] = total
            for a in range(2):
                mine = total[64 * a : 64 * a + 64].astype(BF16)
                row = rounded(total[128 + a : 129 + a])
                if l == 0:
                    for xx in range(4):
                        pb[g, xx, a] = mine[16 * xx : 16 * xx + 16]
                        ps[g, xx, a] = row[:, 256 * xx : 256 * xx + 256]
                else:
                    cb[2 * a + g] = mine
                    ct[2 * a + g] = row
        if l == 0:
            for k in (2, 1, 3):
                start(part_send(g, k))
        else:
            for a in range(2):

                @pl.when(x != 2 * a + g)
                def _():
                    start(last_send(g, a))

    def next_rows(g):
        with scope("wait_part"):
            came(3 * 66, s_rp.at[g])
        for a in range(2):
            own = pl.ds(pl.multiple_of(64 * a + 16 * x, 16), 16)
            row = pl.ds(128 + a, 1)
            total = pf[g, own] + fst[g, own] + fc2b[0:1]
            slot_row = pf[g, row, cols_of(x)] + fst[g, row, cols_of(x)] + fc2b[0:1, cols_of(x)]
            for k in range(3):
                total = total + rb[g, k, a].astype(F32)
                slot_row = slot_row + rs[g, k, a]
            xs[1, g, a, rows_of(x)] = total.astype(BF16)
            xl[1, g, a, :, cols_of(x)] = rounded(slot_row)
        for k in (2, 1, 3):
            start(row_send(g, k))

    def first_rows(g):
        r = iota((144, 520), 0)
        i = jnp.where(r < 128, r // 64, r - 128) * 2 + g
        want = jnp.where(r < 130, 65 * (2 * i + c) + jnp.where(r < 128, mod(r, 64), 64), -1)
        rows = dot((want == iota((144, 520), 1)).astype(BF16), xin[...])
        for a in range(2):
            xs[0, g, a] = rows[64 * a : 64 * a + 64].astype(BF16)
            xl[0, g, a] = rows[128 + a : 129 + a]
        hb[g] = layer_norm(rows, ln1g[0:1], ln1b[0:1]).astype(BF16)

    with scope("first_rows"):
        lx().wait()
        pltpu.make_async_copy(ruler.at[pl.ds(0, 55)], ruler.at[pl.ds(0, 55)], s_p).wait()
        first_rows(0)
        lq_wait(0)
        project(0, 0, hb[0], c)

    with scope("barrier"):
        pl.semaphore_wait(barrier, 20)

    rb0().start()
    for j in range(3):
        rq(0, j).start()
    send_shard(0, 0, c)
    with scope("second_rows"):
        first_rows(1)
        project(0, 1, hb[1], c)
    with scope("wait_wq"):
        arrived(qb.at[1 - c], s_rb.at[0])
        arrived(wq.at[0, 1 - c], s_rq.at[0])
    with scope("project0"):
        for g in range(2):
            if g == 1:
                send_shard(0, 1, c)
            project(0, g, hb[g], 1 - c)
            send_shard(0, g, 1 - c)
    wo_start(0)
    rb1().start()
    for l in range(LAYERS):
        r1(l).start()
        r2(l).start()
    for j in range(3):
        rq(1, j).start()
        lq(1, j).start()
    for l in range(LAYERS):
        lo(l).start()
        l1(l).start()
        l2(l).start()

    copy_t.wait()
    copy_c.wait()
    tq = jnp.zeros((16, 128), jnp.int32)
    td, tf, nd, nf = tq, tq, tq, tq
    for j in range(16):
        fd = 4 * (j // 4) + 2 * (1 - c) + (j % 4) // 2
        fp = 4 * (j // 4) + 2 * c + (j % 4) // 2
        tq = jnp.where(lane16 == j, time_ref[fd], tq)
        td = jnp.where(row16 == j, time_ref[fd], td)
        tf = jnp.where(row16 == j, time_ref[fp], tf)
        nd = jnp.where(row16 == j, cond_ref[fd], nd)
        nf = jnp.where(row16 == j, cond_ref[fp], nf)
    part = mod(row16, 2)
    bias_d = jnp.where(td <= tq, 0.0, NEG)
    bias_f = jnp.where(tf <= tq, 0.0, NEG)
    bsl[0:16] = jnp.where(part < nd, bias_d, NEG).astype(BF16)
    bsl[16:32] = jnp.where(part < nf, bias_f, NEG).astype(BF16)
    for j in range(16):
        bd[j] = jnp.broadcast_to(bias_d[j : j + 1], (64, 128)).astype(BF16)
        bf[j] = jnp.broadcast_to(bias_f[j : j + 1], (64, 128)).astype(BF16)


    for l in range(LAYERS):
        if l == 1:
            lq_wait(1)
            arrived(wq.at[1, 1 - c], s_rq.at[1])
            for g in range(2):
                with scope("wait_row"):
                    came(3 * 66, s_rx.at[g])
                with scope("project1"):
                    h = layer_norm(stream(1, g), ln1g[1:2], ln1b[1:2]).astype(BF16)
                    for sh in range(2):
                        project(1, g, h, sh)
                        send_shard(1, g, sh)
            wo_start(1)

        attend(l)

        with scope("assemble"):
            assemble(l, 0)
        with scope("wait_wo"):
            lo(l).wait()
            arrived(wo.at[l, pl.ds(0, 3)], s_ro.at[l])
            for k in range(1, 4):
                wo_forward(l, k).start()
        with scope("assemble"):
            assemble(l, 1)
        with scope("wait_w"):
            arrived(wo.at[l, pl.ds(0, 4)], s_rfo.at[l])
            l1(l).wait()
            l2(l).wait()
            if l == 0:
                arrived(b1.at[1 - c], s_rb.at[1])
            arrived(w1.at[l, 1 - c], s_r1.at[l])
            arrived(w2.at[l, 1 - c], s_r2.at[l])
        for g in range(2):
            mix(l, g)
        if l == 0:
            for g in range(2):
                next_rows(g)

    with scope("drain"):
        rb0().wait_send()
        rb1().wait_send()
        for g in range(2):
            left(3 * 66, s_sp.at[g])
            left(3 * 66, s_sx.at[g])
        for l in range(LAYERS):
            sent(wq.at[l, 0], s_sq.at[l])
            r1(l).wait_send()
            r2(l).wait_send()
            sent(wo.at[l, pl.ds(0, 3)], s_so.at[l])
            sent(wo.at[l, pl.ds(0, 4)], s_sfo.at[l])
            for g in range(2):
                left(3 * 66, s_sg.at[l, g])
            left(16 * 25, s_sm.at[l])
            left(264, s_sf.at[l])
            left(136, s_sr.at[l])

    gx, ax = mod(x, 2), x // 2
    own, own_row = pl.ds(pl.multiple_of(64 * ax, 64), 64), pl.ds(128 + ax, 1)
    last = pf[gx, own] + fst[gx, own] + fc2b[1:2]
    row = pf[gx, own_row] + fst[gx, own_row] + fc2b[1:2]
    with scope("wait_last"):
        came(3 * 132, s_rc)
    for k in range(3):
        last = last + gb[k].astype(F32)
        row = row + gt[k]
    out_ref[0, 0:64] = last
    out_ref[0, 64:65] = row
    with scope("leave"):
        left(3 * 132, s_sc)


def shards(
    frames_in, frame_time, cond_count, ln1_gain, ln1_bias, qkv_weight, qkv_bias, out_weight, out_bias,
    ln2_gain, ln2_bias, fc1_weight, fc1_bias, fc2_weight, fc2_bias,
):
    any_ = pl.BlockSpec(memory_space=pl.ANY)
    vm = pl.BlockSpec(memory_space=VMEM)
    L = LAYERS
    rows = pl.pallas_call(
        kernel,
        name="layers",
        out_shape=VMEM((1, 65, D), F32),
        in_specs=[any_] * 15,
        out_specs=vm,
        scratch_shapes=[
            pltpu.SMEM((16,), jnp.int32), pltpu.SMEM((16,), jnp.int32), *[VMEM((L, D), F32)] * 6,
            VMEM((520, D), BF16), VMEM((L, 2, 2, 64, D), BF16), VMEM((L, 2, 2, 1, D), F32), VMEM((2, 144, D), BF16),
            VMEM((L, 2, D, 384), BF16), VMEM((2, 3, L, 128), F32), VMEM((L, 8, 128, D), BF16),
            VMEM((L, 2, D, 512), BF16), VMEM((2, L, 512), F32), VMEM((L, 2, 512, D), BF16),
            VMEM((L, 2, 2, 4, 96, 128), BF16), VMEM((L, 2, 2, 4, 1, 256), F32),
            VMEM((L, 16, 96, 128), BF16), VMEM((L, 16, 1, 256), F32),
            VMEM((L, 16, 64, 128), BF16), VMEM((L, 16, 1, 128), F32), VMEM((32, 256), BF16),
            VMEM((L, 16, 32, 128), BF16), VMEM((L, 16, 1, 128), F32),
            VMEM((L, 16, 32, 128), BF16), VMEM((L, 16, 1, 128), F32),
            VMEM((L, 2, 4, 2, 64, 256), BF16), VMEM((L, 2, 4, 2, 1, 256), F32),
            VMEM((2, 144, D), F32), VMEM((2, 144, D), F32),
            VMEM((2, 4, 2, 16, D), BF16), VMEM((2, 4, 2, 1, 256), F32),
            VMEM((2, 3, 2, 16, D), BF16), VMEM((2, 3, 2, 1, 256), F32),
            VMEM((4, 64, D), BF16), VMEM((4, 1, D), F32), VMEM((3, 64, D), BF16), VMEM((3, 1, D), F32),
            VMEM((16, 64, 128), BF16), VMEM((16, 64, 128), BF16), VMEM((32, 128), BF16),
            VMEM((1040, 256), BF16), VMEM((400, 1, 256), F32),
            DMA((2,)), DMA, DMA, DMA((L,)), DMA((L,)), DMA((L,)), DMA((L,)),
            DMA((L,)), DMA((L,)), DMA((2,)), DMA((2,)), DMA((L,)), DMA((L,)), DMA((L,)), DMA((L,)),
            DMA((L,)), DMA((L,)), DMA((L,)), DMA((L,)),
            DMA((L,)), DMA((L, 4)), DMA((L,)), DMA((L,)), DMA((L,)), DMA((L, 4)), DMA((L, 2)), DMA((L, 2, 4)),
            DMA((2,)), DMA((2,)), DMA((2,)), DMA((2,)), DMA, DMA,
        ],
        compiler_params=pltpu.CompilerParams(
            collective_id=0, has_side_effects=True, vmem_limit_bytes=60 * 2**20
        ),
    )(
        frame_time, cond_count, ln1_gain, ln1_bias, ln2_gain, ln2_bias, out_bias, fc2_bias,
        jnp.transpose(qkv_bias, (1, 0, 2)), fc1_bias, frames_in, qkv_weight, out_weight, fc1_weight, fc2_weight,
    )
    return rows.astype(BF16)


def solution(mesh):
    in_specs = (
        P("tm", None, None), P(), P(), P(), P(),
        P(None, None, None, "tensor"), P(None, None, "tensor"), P(None, "tensor", None), P(), P(), P(),
        P(None, None, "tensor"), P(None, "tensor"), P(None, "tensor", None), P(),
    )
    return jax.shard_map(shards, mesh=mesh, in_specs=in_specs, out_specs=P("tm", "tensor", None), check_vma=False)
```

```python
import jax
import jax.numpy as jnp
from jax import lax
from jax.experimental import pallas as pl
from jax.experimental.pallas import tpu as pltpu
from jax.sharding import PartitionSpec as P

MESH = pl.DeviceIdType.MESH
LAYERS = 2
D = 1024
F32 = jnp.float32
BF16 = jnp.bfloat16
NEG = -1e30
VMEM = pltpu.VMEM
DMA = pltpu.SemaphoreType.DMA
scope = jax.named_scope


def mod(a, n):
    return lax.rem(a, n)


def place(y, z, x, c):
    return {"tm": y * 8 + z, "tensor": x * 2 + c}


def iota(shape, dim):
    return lax.broadcasted_iota(jnp.int32, shape, dim)


def layer_norm(rows, gain, bias):
    center = jnp.mean(rows, axis=-1, keepdims=True)
    moved = rows - center
    spread = jnp.mean(moved * moved, axis=-1, keepdims=True)
    return moved * lax.rsqrt(spread + 1e-06) * gain + bias


def gelu(v):
    return 0.5 * v * (1.0 + lax.erf(v * (0.5**0.5)))


def dot(a, b):
    return lax.dot_general(a, b, (((1,), (0,)), ((), ())), preferred_element_type=F32)


def dot_t(a, b):
    return lax.dot_general(a, b, (((1,), (1,)), ((), ())), preferred_element_type=F32)


def rounded(v):
    return v.astype(BF16).astype(F32)


def swap(v):
    return pltpu.roll(v, 64, 1)


def kernel(
    time_hbm, cond_hbm, ln1g_hbm, ln1b_hbm, ln2g_hbm, ln2b_hbm, outb_hbm, fc2b_hbm, qkvb_hbm, fc1b_hbm,
    x_hbm, wq_hbm, wo_hbm, w1_hbm, w2_hbm,
    out_ref,
    time_ref, cond_ref, ln1g, ln1b, ln2g, ln2b, outb, fc2b,
    xin, xs, xl, om, oml, wq, qb, wo, w1, b1, w2, msg, msl, rk, rkl, fk, fkl, ksl, ob, obl, ab, abl, ag, agl, fst, pf,
    pb, ps, rb, rs, cb, ct, gb, gt, bd, bf, bsl, qx, ruler,
    s_t, s_p, s_x, s_lq, s_lw, s_out, s_rq, s_rw, s_ro, s_rfo, s_rm, s_rf, s_rr, s_rg, s_rp, s_rx, s_rc, s_take,
):
    p = lax.axis_index("tm")
    t = lax.axis_index("tensor")
    y, z = p // 8, mod(p, 8)
    x, c = t // 2, mod(t, 2)
    sib = place(y, z, x, 1 - c)
    zh, zl = z // 4, mod(z, 4)
    att = mod(y - zl + 4, 4)
    half = 1 - c
    slot = y * 4 + zl

    def peer(k):
        return place(y, z, mod(x + k, 4), c)

    def clip(g, a, parity):
        return 2 * a + mod(g + parity, 2)

    def clip_home(i, h):
        return place(mod(i + h, 4), 4 * c + h, x, 1 - zh)

    def part_source(j):
        return place(j // 4, 4 * half + mod(j, 4), x, zh)

    def near(n):
        a = n // 4
        return mod(y + a + a // 2 * (5 - 2 * a), 4) * 4 + mod(zl + n, 4)

    def remote(src, dst, ssem, rsem, dev):
        return pltpu.make_async_remote_copy(
            src_ref=src, dst_ref=dst, send_sem=ssem, recv_sem=rsem, device_id=dev, device_id_type=MESH
        )

    def arrived(dst, rsem):
        remote(dst, dst, rsem, rsem, sib).wait_recv()

    def sent(src, ssem):
        remote(src, src, ssem, ssem, sib).wait_send()

    barrier = pltpu.get_barrier_semaphore()

    def greet(dev):
        pl.semaphore_signal(barrier, inc=1, device_id=dev, device_id_type=MESH)

    @pl.loop(0, 16)
    def _(j):
        greet(part_source(j))

    for k in range(1, 4):
        greet(peer(k))
    greet(sib)

    def lx():
        return pltpu.make_async_copy(x_hbm.at[0], xin, s_x)

    def lq(l, j):
        return pltpu.make_async_copy(wq_hbm.at[l, j], wq.at[l, c, :, pl.ds(128 * j, 128)], s_lq.at[l])

    def lq_wait(l):
        pltpu.make_async_copy(wq.at[l, c], wq.at[l, c], s_lq.at[l]).wait()

    def lo(l):
        return pltpu.make_async_copy(wo_hbm.at[l], wo.at[l, t], s_lw.at[l])

    def l1(l):
        return pltpu.make_async_copy(w1_hbm.at[l], w1.at[l, c], s_lw.at[l])

    def l2(l):
        return pltpu.make_async_copy(w2_hbm.at[l], w2.at[l, c], s_lw.at[l])

    lx().start()
    params = (
        (ln1g_hbm, ln1g), (ln1b_hbm, ln1b), (ln2g_hbm, ln2g), (ln2b_hbm, ln2b), (outb_hbm, outb), (fc2b_hbm, fc2b),
        (qkvb_hbm, qb.at[c]), (fc1b_hbm, b1.at[c]),
    )
    for src, dst in params:
        pltpu.make_async_copy(src, dst, s_p).start()
    copy_t = pltpu.make_async_copy(time_hbm, time_ref, s_t.at[0])
    copy_c = pltpu.make_async_copy(cond_hbm, cond_ref, s_t.at[1])
    copy_t.start()
    copy_c.start()
    for j in range(3):
        lq(0, j).start()

    low = iota((64, 128), 1) < 64
    low1 = iota((1, 128), 1) < 64
    low32 = iota((32, 128), 1) < 64
    row16 = iota((16, 128), 0)
    lane16 = iota((16, 128), 1)

    def rq(l, j):
        return remote(wq_hbm.at[l, j], wq.at[l, c, :, pl.ds(128 * j, 128)], s_out, s_rq, sib)

    def rb0():
        return remote(qkvb_hbm, qb.at[c], s_out, s_rq, sib)

    def rb1():
        return remote(fc1b_hbm, b1.at[c], s_out, s_rw.at[0], sib)

    def r1(l):
        return remote(w1_hbm.at[l], w1.at[l, c], s_out, s_rw.at[l], sib)

    def r2(l):
        return remote(w2_hbm.at[l], w2.at[l, c], s_out, s_rw.at[l], sib)

    def wo_send(l, k):
        return remote(wo_hbm.at[l], wo.at[l, t], s_out, s_ro.at[l], peer(k))

    def wo_forward(l, k):
        xx = mod(x + k, 4)
        src = wo_hbm.at[l] if k == 0 else wo.at[l, 2 * xx + c]
        return remote(src, wo.at[l, 2 * xx + c], s_out, s_rfo.at[l], sib)

    def wo_start(l):
        for k in (2, 1, 3):
            wo_send(l, k).start()
        wo_forward(l, 0).start()

    def with_row(rows, slot_row, rows_to, slot_to, ssem, rsem, dev):
        return remote(rows, rows_to, ssem, rsem, dev), remote(slot_row, slot_to, ssem, rsem, dev)

    def start(copies):
        for copy in copies:
            copy.start()

    def came(kib, rsem):
        arrived(ruler.at[pl.ds(0, kib)], rsem)

    def left(kib, ssem):
        sent(ruler.at[pl.ds(0, kib)], ssem)

    def msg_send(l, g, a, h):
        return with_row(
            msg.at[l, g, a, h], msl.at[l, g, a, h], rk.at[l, slot], rkl.at[l, slot], s_out, s_rm.at[l, y],
            clip_home(clip(g, a, c), h),
        )

    def four(n):
        return pl.ds(pl.multiple_of(4 * n, 4), 4)

    def forward(l, n):
        return with_row(
            rk.at[l, four(n), pl.ds(0, 64)], rkl.at[l, four(n), :, pl.ds(0, 128)], fk.at[l, four(n)],
            fkl.at[l, four(n)], s_out, s_rf.at[l], sib,
        )

    def result_send(l, j):
        me = 2 * mod(att + zh, 2) + att // 2
        return with_row(
            ob.at[l, j], obl.at[l, j], ab.at[l, 4 * me + zl], abl.at[l, 4 * me + zl], s_out, s_rr.at[l, me],
            part_source(j),
        )

    def gather_send(l, g, k):
        rows, row = ag.at[l, g, x], agl.at[l, g, x]
        return with_row(rows, row, rows, row, s_out, s_rg.at[l, g, k % 2], peer(k))

    def rows_of(xx):
        return pl.ds(pl.multiple_of(16 * xx, 16), 16)

    def cols_of(xx):
        return pl.ds(pl.multiple_of(256 * xx, 256), 256)

    def part_send(g, k):
        xx = mod(x + k, 4)
        return with_row(
            pb.at[g, xx], ps.at[g, xx], rb.at[g, 3 - k], rs.at[g, 3 - k], s_out, s_rp.at[g], peer(k)
        )

    def row_send(g, k):
        rows, row = xs.at[1, g, :, rows_of(x)], xl.at[1, g, :, :, cols_of(x)]
        return with_row(rows, row, rows, row, s_out, s_rx.at[g], peer(k))

    def last_send(g, a):
        i = clip(g, a, c)
        k = mod(x - i + 4, 4) - 1
        n = 2 * g + a
        return with_row(cb.at[n], ct.at[n], gb.at[k], gt.at[k], s_out, s_rc, place(y, z, i, c))

    def project(l, h, sh, blocks, rows, first):
        out = dot(h, wq[l, sh])
        q = rounded(out[:, 0:128] + qb[sh, 0, l : l + 1]) * 0.125
        k = rounded(out[:, 128:256] + qb[sh, 1, l : l + 1])
        v = rounded(out[:, 256:384] + qb[sh, 2, l : l + 1])
        kr, vr, qr = swap(k), swap(v), swap(q)
        for a in range(2):
            o, r = 64 * a, 128 + a
            for hh in range(2):
                kk, vv = (k, vr) if hh == 0 else (kr, v)
                q0, q1 = (q, qr) if hh == 0 else (qr, q)
                m = blocks.at[a, first + hh]
                m[0:64] = jnp.where(low, kk[o : o + 64], vv[o : o + 64]).astype(BF16)
                m[64:96] = jnp.where(low32, q0[o : o + 32], q1[o + 32 : o + 64]).astype(BF16)
                rows[a, first + hh] = jnp.concatenate(
                    [jnp.where(low1, kk[r : r + 1], vv[r : r + 1]), jnp.where(low1, q0[r : r + 1], 0.0)], axis=1
                )

    def send_shard(l, g, sh):
        for n in range(2):
            for a in range(2):
                start(msg_send(l, g, a, 2 * sh + mod(n + zl, 2)))

    def attend(l):
        with scope("wait_msg"):

            @pl.loop(0, 4)
            def _(a):
                n = mod(y + a + a // 2 * (5 - 2 * a), 4)
                came(4 * 25, s_rm.at[l, n])
                start(forward(l, n))

        low512 = iota((512, 128), 1) < 64
        low1024 = iota((1024, 128), 1) < 64

        def values(kv, n):
            return jnp.where(low1024[0:n], jnp.ones((n, 128), BF16), kv)

        def queries():
            q = rk[l, :, 64:96, :].astype(F32).reshape(512, 128)
            qq = jnp.concatenate([jnp.where(low512, q, 0.0), jnp.where(low512, swap(q), 0.0)], axis=0).astype(BF16)
            hot = (mod(iota((1024, 128), 0), 512) // 32 == iota((1024, 128), 1)).astype(BF16)
            slots = rkl[l].reshape(16, 256).astype(BF16)
            ksl[0:16, 0:128] = slots[:, 0:128]
            slots_q = jnp.concatenate([slots[:, 128:256], (row16 == lane16).astype(BF16)], axis=1)
            qx[...] = jnp.concatenate([jnp.concatenate([qq, hot], axis=1), slots_q], axis=0)

        def scored(k, bias):
            return dot_t(qx[...], jnp.concatenate([k, bias[...].reshape(1024, 128)], axis=1))

        def top_of(s):
            return jnp.max(s, axis=1, keepdims=True)

        def weighted(s, top, kv, n):
            return dot(jnp.exp((s - top).astype(BF16)), values(kv, n))

        def own_keys():
            return rk[l, :, 0:64, :].reshape(1024, 128)

        def passed_keys():
            return fk[l].reshape(1024, 128)

        def slot_keys():
            ksl[16:32, 0:128] = fkl[l].reshape(16, 128).astype(BF16)
            ksl[:, 128:256] = bsl[...]
            return dot_t(qx[...], ksl[...])

        def finish(o):
            lo_, hi_, sl = o[0:512], o[512:1024], o[1024:1040]
            mixed = jnp.where(low512, swap(lo_), hi_) / jnp.where(low512, lo_, swap(hi_))
            ob[l] = mixed.astype(BF16).reshape(16, 32, 128)
            obl[l] = jnp.where(lane16 >= 64, rounded(sl / swap(sl)), 0.0).reshape(16, 1, 128)

        with scope("queries"):
            queries()

        @pl.when(half == zh)
        def _():
            k1 = own_keys()
            s1 = scored(k1, bd)
            top1 = top_of(s1)
            o1 = weighted(s1, top1, k1, 1024)
            came(264, s_rf.at[l])
            k2 = passed_keys()
            s2, s3 = scored(k2, bf), slot_keys()
            top = jnp.maximum(jnp.maximum(top_of(s2), top_of(s3)), top1)
            o = jnp.exp(top1 - top) * o1 + weighted(s2, top, k2, 1024)
            finish(o + weighted(s3, top, ksl[:, 0:128], 32))

        @pl.when(half != zh)
        def _():
            came(264, s_rf.at[l])
            k1, k2 = own_keys(), passed_keys()
            s1, s3 = scored(k1, bd), slot_keys()
            top1 = jnp.maximum(top_of(s1), top_of(s3))
            o1 = weighted(s1, top1, k1, 1024) + weighted(s3, top1, ksl[:, 0:128], 32)
            s2 = scored(k2, bf)
            top2 = top_of(s2)
            o2 = weighted(s2, top2, k2, 1024)
            top = jnp.maximum(top1, top2)
            finish(jnp.exp(top1 - top) * o1 + jnp.exp(top2 - top) * o2)

        @pl.loop(0, 16)
        def _(n):
            start(result_send(l, near(15 - n)))

    def assemble(l, g):
        for a in range(2):
            q = 4 * (2 * g + a)
            with scope("wait_result"):
                came(34, s_rr.at[l, 2 * g + a])

            for m in range(2):
                u = ab[l, q + 2 * m].astype(F32)
                v = ab[l, q + 2 * m + 1].astype(F32)
                cols = slice(128 * m, 128 * m + 128)
                ag[l, g, x, a, 0:32, cols] = jnp.where(low32, u, swap(v)).astype(BF16)
                ag[l, g, x, a, 32:64, cols] = jnp.where(low32, swap(u), v).astype(BF16)
                agl[l, g, x, a, :, cols] = jnp.where(low1, swap(abl[l, q + 2 * m]), abl[l, q + 2 * m + 1])
        for k in (2, 1, 3):
            start(gather_send(l, g, k))

    def stacked(blocks, rows):
        n = rows[0].shape[1]
        which = iota((16, n), 0)
        tile = jnp.where(which == 0, jnp.broadcast_to(rows[0], (16, n)), 0.0)
        tile = jnp.where(which == 1, jnp.broadcast_to(rows[1], (16, n)), tile)
        return jnp.concatenate([*blocks, tile.astype(blocks[0].dtype)], axis=0)

    def stream(l, g):
        return stacked([xs[l, g, a].astype(F32) for a in range(2)], [xl[l, g, a] for a in range(2)])

    def mix(l, g):
        def arrive(odd):
            with scope("wait_gather"):
                came(66 * (1 + odd), s_rg.at[l, g, odd])

        def piece(k):
            xx = mod(x + k, 4)
            attended = stacked([ag[l, g, xx, a] for a in range(2)], [agl[l, g, xx, a] for a in range(2)])
            return dot(attended, wo[l, pl.ds(2 * xx, 2)].reshape(256, D))

        with scope("out_proj"):
            first = stream(l, g) + outb[l : l + 1] + piece(0)
        arrive(1)
        with scope("out_proj"):
            first = first + (piece(1) + piece(3))
        arrive(0)
        with scope("out_proj"):
            first = first + piece(2)
            fst[g] = first
            normed = layer_norm(first, ln2g[l : l + 1], ln2b[l : l + 1]).astype(BF16)
        with scope("mlp"):
            inner = [gelu(dot(normed, w1[l, sh]) + b1[sh, l : l + 1]).astype(BF16) for sh in range(2)]
            total = dot(jnp.concatenate(inner, axis=1), w2[l].reshape(D, D))
            pf[g] = total
            for a in range(2):
                mine = total[64 * a : 64 * a + 64].astype(BF16)
                row = rounded(total[128 + a : 129 + a])
                if l == 0:
                    for xx in range(4):
                        pb[g, xx, a] = mine[16 * xx : 16 * xx + 16]
                        ps[g, xx, a] = row[:, 256 * xx : 256 * xx + 256]
                else:
                    cb[2 * g + a] = mine
                    ct[2 * g + a] = row
        if l == 0:
            for k in (2, 1, 3):
                start(part_send(g, k))
        else:
            for a in range(2):

                @pl.when(x != clip(g, a, c))
                def _():
                    start(last_send(g, a))

    def next_rows(g):
        with scope("wait_part"):
            came(3 * 66, s_rp.at[g])
        for a in range(2):
            own = pl.ds(pl.multiple_of(64 * a + 16 * x, 16), 16)
            row = pl.ds(128 + a, 1)
            total = pf[g, own] + fst[g, own] + fc2b[0:1]
            slot_row = pf[g, row, cols_of(x)] + fst[g, row, cols_of(x)] + fc2b[0:1, cols_of(x)]
            for k in range(3):
                total = total + rb[g, k, a].astype(F32)
                slot_row = slot_row + rs[g, k, a]
            xs[1, g, a, rows_of(x)] = total.astype(BF16)
            xl[1, g, a, :, cols_of(x)] = rounded(slot_row)
        for k in (2, 1, 3):
            start(row_send(g, k))

    def first_rows(g, parity):
        r = iota((144, 520), 0)
        i = clip(g, jnp.where(r < 128, r // 64, r - 128), parity)
        want = jnp.where(r < 130, 65 * (2 * i + parity) + jnp.where(r < 128, mod(r, 64), 64), -1)
        rows = dot((want == iota((144, 520), 1)).astype(BF16), xin[...])
        return rows, layer_norm(rows, ln1g[0:1], ln1b[0:1]).astype(BF16)

    def for_sibling(g):
        project(0, first_rows(g, 1 - c)[1], c, om.at[g], oml.at[g], 0)

    def give(g):
        heads = pl.ds(pl.multiple_of(2 * c, 2), 2)
        return with_row(
            om.at[g], oml.at[g], msg.at[0, g, :, heads], msl.at[0, g, :, heads], s_out, s_take.at[g], sib
        )

    def own_rows(g):
        rows, h = first_rows(g, c)
        for a in range(2):
            xs[0, g, a] = rows[64 * a : 64 * a + 64].astype(BF16)
            xl[0, g, a] = rows[128 + a : 129 + a]
        project(0, h, c, msg.at[0, g], msl.at[0, g], 2 * c)

    with scope("first_rows"):
        lx().wait()
        pltpu.make_async_copy(ruler.at[pl.ds(0, 55)], ruler.at[pl.ds(0, 55)], s_p).wait()
        lq_wait(0)
        for_sibling(0)
        own_rows(0)

    with scope("barrier"):
        pl.semaphore_wait(barrier, 20)

    start(give(0))
    send_shard(0, 0, c)
    with scope("second_rows"):
        for_sibling(1)
    start(give(1))
    with scope("wait_take"):
        came(100, s_take.at[0])
    send_shard(0, 0, 1 - c)
    with scope("second_rows"):
        own_rows(1)
    send_shard(0, 1, c)
    with scope("wait_take"):
        came(100, s_take.at[1])
    send_shard(0, 1, 1 - c)
    wo_start(0)
    rb0().start()
    rb1().start()
    for l in range(LAYERS):
        r1(l).start()
        r2(l).start()
    for j in range(3):
        rq(1, j).start()
        lq(1, j).start()
    for l in range(LAYERS):
        lo(l).start()
        l1(l).start()
        l2(l).start()

    copy_t.wait()
    copy_c.wait()
    tq = jnp.zeros((16, 128), jnp.int32)
    td, tf, nd, nf = tq, tq, tq, tq
    for j in range(16):
        fd = 4 * (j // 4) + 2 * (1 - c) + (j % 4) // 2
        fp = 4 * (j // 4) + 2 * c + (j % 4) // 2
        tq = jnp.where(lane16 == j, time_ref[fd], tq)
        td = jnp.where(row16 == j, time_ref[fd], td)
        tf = jnp.where(row16 == j, time_ref[fp], tf)
        nd = jnp.where(row16 == j, cond_ref[fd], nd)
        nf = jnp.where(row16 == j, cond_ref[fp], nf)
    part = mod(row16, 2)
    bias_d = jnp.where(td <= tq, 0.0, NEG)
    bias_f = jnp.where(tf <= tq, 0.0, NEG)
    bsl[0:16] = jnp.where(part < nd, bias_d, NEG).astype(BF16)
    bsl[16:32] = jnp.where(part < nf, bias_f, NEG).astype(BF16)
    for j in range(16):
        bd[j] = jnp.broadcast_to(bias_d[j : j + 1], (64, 128)).astype(BF16)
        bf[j] = jnp.broadcast_to(bias_f[j : j + 1], (64, 128)).astype(BF16)


    for l in range(LAYERS):
        if l == 1:
            lq_wait(1)
            came(3 * 256 + 3, s_rq)
            for g in range(2):
                with scope("wait_row"):
                    came(3 * 66, s_rx.at[g])
                with scope("project1"):
                    h = layer_norm(stream(1, g), ln1g[1:2], ln1b[1:2]).astype(BF16)
                    for sh in range(2):
                        project(1, h, sh, msg.at[1, g], msl.at[1, g], 2 * sh)
                        send_shard(1, g, sh)
            wo_start(1)

        attend(l)

        with scope("assemble"):
            assemble(l, 0)
        with scope("wait_wo"):
            loaded = ruler.at[pl.ds(0, 256 + 2 * 1024)]
            pltpu.make_async_copy(loaded, loaded, s_lw.at[l]).wait()
            arrived(wo.at[l, pl.ds(0, 3)], s_ro.at[l])
            for k in range(1, 4):
                wo_forward(l, k).start()
        with scope("assemble"):
            assemble(l, 1)
        with scope("wait_w"):
            arrived(wo.at[l, pl.ds(0, 4)], s_rfo.at[l])
            came(2 * 1024 + (4 if l == 0 else 0), s_rw.at[l])
        for g in range(2):
            mix(l, g)
        if l == 0:
            for g in range(2):
                next_rows(g)

    gx, ax = mod(x + c, 2), x // 2
    own, own_row = pl.ds(pl.multiple_of(64 * ax, 64), 64), pl.ds(128 + ax, 1)
    last = pf[gx, own] + fst[gx, own] + fc2b[1:2]
    row = pf[gx, own_row] + fst[gx, own_row] + fc2b[1:2]
    with scope("wait_last"):
        came(3 * 132, s_rc)
    for k in range(3):
        last = last + gb[k].astype(F32)
        row = row + gt[k]
    out_ref[0, 0:64] = last
    out_ref[0, 64:65] = row
    with scope("leave"):
        layer = 7 * 256 + 16 * 25 + 264 + 136 + 6 * 66
        total = 2 * layer + 4 * 1024 + 3 * 256 + 3 + 4 + 200 + 12 * 66 + 3 * 132
        for n in range(0, total, 2304):
            left(min(2304, total - n), s_out)


def shards(
    frames_in, frame_time, cond_count, ln1_gain, ln1_bias, qkv_weight, qkv_bias, out_weight, out_bias,
    ln2_gain, ln2_bias, fc1_weight, fc1_bias, fc2_weight, fc2_bias,
):
    any_ = pl.BlockSpec(memory_space=pl.ANY)
    vm = pl.BlockSpec(memory_space=VMEM)
    L = LAYERS
    rows = pl.pallas_call(
        kernel,
        name="layers",
        out_shape=VMEM((1, 65, D), F32),
        in_specs=[any_] * 15,
        out_specs=vm,
        scratch_shapes=[
            pltpu.SMEM((16,), jnp.int32), pltpu.SMEM((16,), jnp.int32), *[VMEM((L, D), F32)] * 6,
            VMEM((520, D), BF16), VMEM((L, 2, 2, 64, D), BF16), VMEM((L, 2, 2, 1, D), F32),
            VMEM((2, 2, 2, 96, 128), BF16), VMEM((2, 2, 2, 1, 256), F32),
            VMEM((L, 2, D, 384), BF16), VMEM((2, 3, L, 128), F32), VMEM((L, 8, 128, D), BF16),
            VMEM((L, 2, D, 512), BF16), VMEM((2, L, 512), F32), VMEM((L, 2, 512, D), BF16),
            VMEM((L, 2, 2, 4, 96, 128), BF16), VMEM((L, 2, 2, 4, 1, 256), F32),
            VMEM((L, 16, 96, 128), BF16), VMEM((L, 16, 1, 256), F32),
            VMEM((L, 16, 64, 128), BF16), VMEM((L, 16, 1, 128), F32), VMEM((32, 256), BF16),
            VMEM((L, 16, 32, 128), BF16), VMEM((L, 16, 1, 128), F32),
            VMEM((L, 16, 32, 128), BF16), VMEM((L, 16, 1, 128), F32),
            VMEM((L, 2, 4, 2, 64, 256), BF16), VMEM((L, 2, 4, 2, 1, 256), F32),
            VMEM((2, 144, D), F32), VMEM((2, 144, D), F32),
            VMEM((2, 4, 2, 16, D), BF16), VMEM((2, 4, 2, 1, 256), F32),
            VMEM((2, 3, 2, 16, D), BF16), VMEM((2, 3, 2, 1, 256), F32),
            VMEM((4, 64, D), BF16), VMEM((4, 1, D), F32), VMEM((3, 64, D), BF16), VMEM((3, 1, D), F32),
            VMEM((16, 64, 128), BF16), VMEM((16, 64, 128), BF16), VMEM((32, 128), BF16),
            VMEM((1040, 256), BF16), VMEM((2304, 1, 256), F32),
            DMA((2,)), DMA, DMA, DMA((L,)), DMA((L,)), DMA, DMA, DMA((L,)), DMA((L,)), DMA((L,)),
            DMA((L, 4)), DMA((L,)), DMA((L, 4)), DMA((L, 2, 2)), DMA((2,)), DMA((2,)), DMA, DMA((2,)),
        ],
        compiler_params=pltpu.CompilerParams(
            collective_id=0, has_side_effects=True, vmem_limit_bytes=60 * 2**20
        ),
    )(
        frame_time, cond_count, ln1_gain, ln1_bias, ln2_gain, ln2_bias, out_bias, fc2_bias,
        jnp.transpose(qkv_bias, (1, 0, 2)), fc1_bias, frames_in, qkv_weight, out_weight, fc1_weight, fc2_weight,
    )
    return rows.astype(BF16)


def solution(mesh):
    in_specs = (
        P("tm", None, None), P(), P(), P(), P(),
        P(None, None, None, "tensor"), P(None, None, "tensor"), P(None, "tensor", None), P(), P(), P(),
        P(None, None, "tensor"), P(None, "tensor"), P(None, "tensor", None), P(),
    )
    return jax.shard_map(shards, mesh=mesh, in_specs=in_specs, out_specs=P("tm", "tensor", None), check_vma=False)
```

```python
import jax
import jax.numpy as jnp
from jax import lax
from jax.experimental import pallas as pl
from jax.experimental.pallas import tpu as pltpu
from jax.sharding import PartitionSpec as P

MESH = pl.DeviceIdType.MESH
LAYERS = 2
D = 1024
F32 = jnp.float32
BF16 = jnp.bfloat16
NEG = -1e30
VMEM = pltpu.VMEM
DMA = pltpu.SemaphoreType.DMA
scope = jax.named_scope


def mod(a, n):
    return lax.rem(a, n)


def place(y, z, x, c):
    return {"tm": y * 8 + z, "tensor": x * 2 + c}


def iota(shape, dim):
    return lax.broadcasted_iota(jnp.int32, shape, dim)


def layer_norm(rows, gain, bias):
    center = jnp.mean(rows, axis=-1, keepdims=True)
    moved = rows - center
    spread = jnp.mean(moved * moved, axis=-1, keepdims=True)
    return moved * lax.rsqrt(spread + 1e-06) * gain + bias


def gelu(v):
    return 0.5 * v * (1.0 + lax.erf(v * (0.5**0.5)))


def dot(a, b):
    return lax.dot_general(a, b, (((1,), (0,)), ((), ())), preferred_element_type=F32)


def dot_t(a, b):
    return lax.dot_general(a, b, (((1,), (1,)), ((), ())), preferred_element_type=F32)


def rounded(v):
    return v.astype(BF16).astype(F32)


def swap(v):
    return pltpu.roll(v, 64, 1)


def kernel(
    time_hbm, cond_hbm, ln1g_hbm, ln1b_hbm, ln2g_hbm, ln2b_hbm, outb_hbm, fc2b_hbm, qkvb_hbm, fc1b_hbm,
    x_hbm, wq_hbm, wo_hbm, w1_hbm, w2_hbm,
    out_ref,
    time_ref, cond_ref, ln1g, ln1b, ln2g, ln2b, outb, fc2b,
    xin, xs, xl, om, oml, wq, qb, wo, w1, b1, w2, msg, msl, rk, rkl, fk, fkl, ksl, ob, obl, ab, abl, ag, agl, fst, pf,
    pb, ps, rb, rs, cb, ct, gb, gt, bd, bf, bsl, qx, ruler,
    s_t, s_p, s_x, s_lq, s_lw, s_out, s_rq, s_rw, s_ro, s_rfo, s_rm, s_rf, s_rr, s_rg, s_rp, s_rx, s_rc, s_take,
):
    p = lax.axis_index("tm")
    t = lax.axis_index("tensor")
    y, z = p // 8, mod(p, 8)
    x, c = t // 2, mod(t, 2)
    sib = place(y, z, x, 1 - c)
    zh, zl = z // 4, mod(z, 4)
    att = mod(y - zl + 4, 4)
    half = 1 - c
    slot = y * 4 + zl

    def peer(k):
        return place(y, z, mod(x + k, 4), c)

    def clip(g, a, parity):
        return 2 * a + mod(g + parity, 2)

    def clip_home(i, h):
        return place(mod(i + h, 4), 4 * c + h, x, 1 - zh)

    def part_source(j):
        return place(j // 4, 4 * half + mod(j, 4), x, zh)

    def far_first(n):
        a, r = 3 - n // 4, mod(n, 4)
        down = 1 - mod(z - 4 * half + 10, 8) // 4
        return mod(y + a + a // 2 * (5 - 2 * a), 4) * 4 + r + down * (3 - 2 * r)

    def remote(src, dst, ssem, rsem, dev):
        return pltpu.make_async_remote_copy(
            src_ref=src, dst_ref=dst, send_sem=ssem, recv_sem=rsem, device_id=dev, device_id_type=MESH
        )

    def arrived(dst, rsem):
        remote(dst, dst, rsem, rsem, sib).wait_recv()

    def sent(src, ssem):
        remote(src, src, ssem, ssem, sib).wait_send()

    barrier = pltpu.get_barrier_semaphore()

    def greet(dev):
        pl.semaphore_signal(barrier, inc=1, device_id=dev, device_id_type=MESH)

    @pl.loop(0, 16)
    def _(j):
        greet(part_source(j))

    for k in range(1, 4):
        greet(peer(k))
    greet(sib)

    def lx():
        return pltpu.make_async_copy(x_hbm.at[0], xin, s_x)

    def lq(l, j):
        return pltpu.make_async_copy(wq_hbm.at[l, j], wq.at[l, c, :, pl.ds(128 * j, 128)], s_lq.at[l])

    def lq_wait(l):
        pltpu.make_async_copy(wq.at[l, c], wq.at[l, c], s_lq.at[l]).wait()

    def lo(l):
        return pltpu.make_async_copy(wo_hbm.at[l], wo.at[l, t], s_lw.at[l])

    def l1(l):
        return pltpu.make_async_copy(w1_hbm.at[l], w1.at[l, c], s_lw.at[l])

    def l2(l):
        return pltpu.make_async_copy(w2_hbm.at[l], w2.at[l, c], s_lw.at[l])

    lx().start()
    params = (
        (ln1g_hbm, ln1g), (ln1b_hbm, ln1b), (ln2g_hbm, ln2g), (ln2b_hbm, ln2b), (outb_hbm, outb), (fc2b_hbm, fc2b),
        (qkvb_hbm, qb.at[c]), (fc1b_hbm, b1.at[c]),
    )
    for src, dst in params:
        pltpu.make_async_copy(src, dst, s_p).start()
    copy_t = pltpu.make_async_copy(time_hbm, time_ref, s_t.at[0])
    copy_c = pltpu.make_async_copy(cond_hbm, cond_ref, s_t.at[1])
    copy_t.start()
    copy_c.start()
    for j in range(3):
        lq(0, j).start()

    low = iota((64, 128), 1) < 64
    low1 = iota((1, 128), 1) < 64
    low32 = iota((32, 128), 1) < 64
    row16 = iota((16, 128), 0)
    lane16 = iota((16, 128), 1)

    def rq(l, j):
        return remote(wq_hbm.at[l, j], wq.at[l, c, :, pl.ds(128 * j, 128)], s_out, s_rq, sib)

    def rb0():
        return remote(qkvb_hbm, qb.at[c], s_out, s_rq, sib)

    def rb1():
        return remote(fc1b_hbm, b1.at[c], s_out, s_rw.at[0], sib)

    def r1(l):
        return remote(w1_hbm.at[l], w1.at[l, c], s_out, s_rw.at[l], sib)

    def r2(l):
        return remote(w2_hbm.at[l], w2.at[l, c], s_out, s_rw.at[l], sib)

    def wo_send(l, k):
        return remote(wo_hbm.at[l], wo.at[l, t], s_out, s_ro.at[l], peer(k))

    def wo_forward(l, k):
        xx = mod(x + k, 4)
        src = wo_hbm.at[l] if k == 0 else wo.at[l, 2 * xx + c]
        return remote(src, wo.at[l, 2 * xx + c], s_out, s_rfo.at[l], sib)

    def wo_start(l):
        for k in (2, 1, 3):
            wo_send(l, k).start()
        wo_forward(l, 0).start()

    def with_row(rows, slot_row, rows_to, slot_to, ssem, rsem, dev):
        return remote(rows, rows_to, ssem, rsem, dev), remote(slot_row, slot_to, ssem, rsem, dev)

    def start(copies):
        for copy in copies:
            copy.start()

    def came(kib, rsem):
        arrived(ruler.at[pl.ds(0, kib)], rsem)

    def left(kib, ssem):
        sent(ruler.at[pl.ds(0, kib)], ssem)

    def msg_send(l, g, a, h):
        return with_row(
            msg.at[l, g, a, h], msl.at[l, g, a, h], rk.at[l, slot], rkl.at[l, slot], s_out, s_rm.at[l, y],
            clip_home(clip(g, a, c), h),
        )

    def four(n):
        return pl.ds(pl.multiple_of(4 * n, 4), 4)

    def forward(l, n):
        return with_row(
            rk.at[l, four(n), pl.ds(0, 64)], rkl.at[l, four(n), :, pl.ds(0, 128)], fk.at[l, four(n)],
            fkl.at[l, four(n)], s_out, s_rf.at[l], sib,
        )

    def result_send(l, j):
        me = 2 * mod(att + zh, 2) + att // 2
        return with_row(
            ob.at[l, j], obl.at[l, j], ab.at[l, 4 * me + zl], abl.at[l, 4 * me + zl], s_out, s_rr.at[l, me],
            part_source(j),
        )

    def gather_send(l, g, k):
        rows, row = ag.at[l, g, x], agl.at[l, g, x]
        return with_row(rows, row, rows, row, s_out, s_rg.at[l, g, k % 2], peer(k))

    def rows_of(xx):
        return pl.ds(pl.multiple_of(16 * xx, 16), 16)

    def cols_of(xx):
        return pl.ds(pl.multiple_of(256 * xx, 256), 256)

    def part_send(g, k):
        xx = mod(x + k, 4)
        return with_row(
            pb.at[g, xx], ps.at[g, xx], rb.at[g, 3 - k], rs.at[g, 3 - k], s_out, s_rp.at[g], peer(k)
        )

    def row_send(g, k):
        rows, row = xs.at[1, g, :, rows_of(x)], xl.at[1, g, :, :, cols_of(x)]
        return with_row(rows, row, rows, row, s_out, s_rx.at[g], peer(k))

    def last_send(g, a):
        i = clip(g, a, c)
        k = mod(x - i + 4, 4) - 1
        n = 2 * g + a
        return with_row(cb.at[n], ct.at[n], gb.at[k], gt.at[k], s_out, s_rc, place(y, z, i, c))

    def project(l, h, sh, blocks, rows, first):
        out = dot(h, wq[l, sh])
        q = rounded(out[:, 0:128] + qb[sh, 0, l : l + 1]) * 0.125
        k = rounded(out[:, 128:256] + qb[sh, 1, l : l + 1])
        v = rounded(out[:, 256:384] + qb[sh, 2, l : l + 1])
        kr, vr, qr = swap(k), swap(v), swap(q)
        for a in range(2):
            o, r = 64 * a, 128 + a
            for hh in range(2):
                kk, vv = (k, vr) if hh == 0 else (kr, v)
                q0, q1 = (q, qr) if hh == 0 else (qr, q)
                m = blocks.at[a, first + hh]
                m[0:64] = jnp.where(low, kk[o : o + 64], vv[o : o + 64]).astype(BF16)
                m[64:96] = jnp.where(low32, q0[o : o + 32], q1[o + 32 : o + 64]).astype(BF16)
                rows[a, first + hh] = jnp.concatenate(
                    [jnp.where(low1, kk[r : r + 1], vv[r : r + 1]), jnp.where(low1, q0[r : r + 1], 0.0)], axis=1
                )

    def send_shard(l, g, sh):
        far = 1 - mod(z - 4 * c - 2 * sh + 11, 8) // 4
        for n in range(2):
            for a in range(2):
                start(msg_send(l, g, a, 2 * sh + mod(n + far, 2)))

    def attend(l):
        with scope("wait_msg"):

            @pl.loop(0, 4)
            def _(a):
                n = mod(y + a + a // 2 * (5 - 2 * a), 4)
                came(4 * 25, s_rm.at[l, n])
                start(forward(l, n))

        low512 = iota((512, 128), 1) < 64
        low1024 = iota((1024, 128), 1) < 64

        def values(kv, n):
            return jnp.where(low1024[0:n], jnp.ones((n, 128), BF16), kv)

        def queries():
            q = rk[l, :, 64:96, :].astype(F32).reshape(512, 128)
            qq = jnp.concatenate([jnp.where(low512, q, 0.0), jnp.where(low512, swap(q), 0.0)], axis=0).astype(BF16)
            hot = (mod(iota((1024, 128), 0), 512) // 32 == iota((1024, 128), 1)).astype(BF16)
            slots = rkl[l].reshape(16, 256).astype(BF16)
            ksl[0:16, 0:128] = slots[:, 0:128]
            slots_q = jnp.concatenate([slots[:, 128:256], (row16 == lane16).astype(BF16)], axis=1)
            qx[...] = jnp.concatenate([jnp.concatenate([qq, hot], axis=1), slots_q], axis=0)

        def scored(k, bias):
            return dot_t(qx[...], jnp.concatenate([k, bias[...].reshape(1024, 128)], axis=1))

        def top_of(s):
            return jnp.max(s, axis=1, keepdims=True)

        def weighted(s, top, kv, n):
            return dot(jnp.exp((s - top).astype(BF16)), values(kv, n))

        def own_keys():
            return rk[l, :, 0:64, :].reshape(1024, 128)

        def passed_keys():
            return fk[l].reshape(1024, 128)

        def slot_keys():
            ksl[16:32, 0:128] = fkl[l].reshape(16, 128).astype(BF16)
            ksl[:, 128:256] = bsl[...]
            return dot_t(qx[...], ksl[...])

        def finish(o):
            lo_, hi_, sl = o[0:512], o[512:1024], o[1024:1040]
            mixed = jnp.where(low512, swap(lo_), hi_) / jnp.where(low512, lo_, swap(hi_))
            ob[l] = mixed.astype(BF16).reshape(16, 32, 128)
            obl[l] = jnp.where(lane16 >= 64, rounded(sl / swap(sl)), 0.0).reshape(16, 1, 128)

        with scope("queries"):
            queries()

        @pl.when(half == zh)
        def _():
            k1 = own_keys()
            s1 = scored(k1, bd)
            top1 = top_of(s1)
            o1 = weighted(s1, top1, k1, 1024)
            came(264, s_rf.at[l])
            k2 = passed_keys()
            s2, s3 = scored(k2, bf), slot_keys()
            top = jnp.maximum(jnp.maximum(top_of(s2), top_of(s3)), top1)
            o = jnp.exp(top1 - top) * o1 + weighted(s2, top, k2, 1024)
            finish(o + weighted(s3, top, ksl[:, 0:128], 32))

        @pl.when(half != zh)
        def _():
            came(264, s_rf.at[l])
            k1, k2 = own_keys(), passed_keys()
            s1, s3 = scored(k1, bd), slot_keys()
            top1 = jnp.maximum(top_of(s1), top_of(s3))
            o1 = weighted(s1, top1, k1, 1024) + weighted(s3, top1, ksl[:, 0:128], 32)
            s2 = scored(k2, bf)
            top2 = top_of(s2)
            o2 = weighted(s2, top2, k2, 1024)
            top = jnp.maximum(top1, top2)
            finish(jnp.exp(top1 - top) * o1 + jnp.exp(top2 - top) * o2)

        @pl.loop(0, 16)
        def _(n):
            start(result_send(l, far_first(n)))

    def assemble(l, g):
        for a in range(2):
            q = 4 * (2 * g + a)
            with scope("wait_result"):
                came(34, s_rr.at[l, 2 * g + a])

            for m in range(2):
                u = ab[l, q + 2 * m].astype(F32)
                v = ab[l, q + 2 * m + 1].astype(F32)
                cols = slice(128 * m, 128 * m + 128)
                ag[l, g, x, a, 0:32, cols] = jnp.where(low32, u, swap(v)).astype(BF16)
                ag[l, g, x, a, 32:64, cols] = jnp.where(low32, swap(u), v).astype(BF16)
                agl[l, g, x, a, :, cols] = jnp.where(low1, swap(abl[l, q + 2 * m]), abl[l, q + 2 * m + 1])
        for k in (2, 1, 3):
            start(gather_send(l, g, k))

    def stacked(blocks, rows):
        n = rows[0].shape[1]
        which = iota((16, n), 0)
        tile = jnp.where(which == 0, jnp.broadcast_to(rows[0], (16, n)), 0.0)
        tile = jnp.where(which == 1, jnp.broadcast_to(rows[1], (16, n)), tile)
        return jnp.concatenate([*blocks, tile.astype(blocks[0].dtype)], axis=0)

    def stream(l, g):
        return stacked([xs[l, g, a].astype(F32) for a in range(2)], [xl[l, g, a] for a in range(2)])

    def mix(l, g):
        def arrive(odd):
            with scope("wait_gather"):
                came(66 * (1 + odd), s_rg.at[l, g, odd])

        def piece(k):
            xx = mod(x + k, 4)
            attended = stacked([ag[l, g, xx, a] for a in range(2)], [agl[l, g, xx, a] for a in range(2)])
            return dot(attended, wo[l, pl.ds(2 * xx, 2)].reshape(256, D))

        with scope("out_proj"):
            first = stream(l, g) + outb[l : l + 1] + piece(0)
        arrive(1)
        with scope("out_proj"):
            first = first + (piece(1) + piece(3))
        arrive(0)
        with scope("out_proj"):
            first = first + piece(2)
            fst[g] = first
            normed = layer_norm(first, ln2g[l : l + 1], ln2b[l : l + 1]).astype(BF16)
        with scope("mlp"):
            inner = [gelu(dot(normed, w1[l, sh]) + b1[sh, l : l + 1]).astype(BF16) for sh in range(2)]
            total = dot(jnp.concatenate(inner, axis=1), w2[l].reshape(D, D))
            pf[g] = total
            for a in range(2):
                mine = total[64 * a : 64 * a + 64].astype(BF16)
                row = rounded(total[128 + a : 129 + a])
                if l == 0:
                    for xx in range(4):
                        pb[g, xx, a] = mine[16 * xx : 16 * xx + 16]
                        ps[g, xx, a] = row[:, 256 * xx : 256 * xx + 256]
                else:
                    cb[2 * g + a] = mine
                    ct[2 * g + a] = row
        if l == 0:
            for k in (2, 1, 3):
                start(part_send(g, k))
        else:
            for a in range(2):

                @pl.when(x != clip(g, a, c))
                def _():
                    start(last_send(g, a))

    def next_rows(g):
        with scope("wait_part"):
            came(3 * 66, s_rp.at[g])
        for a in range(2):
            own = pl.ds(pl.multiple_of(64 * a + 16 * x, 16), 16)
            row = pl.ds(128 + a, 1)
            total = pf[g, own] + fst[g, own] + fc2b[0:1]
            slot_row = pf[g, row, cols_of(x)] + fst[g, row, cols_of(x)] + fc2b[0:1, cols_of(x)]
            for k in range(3):
                total = total + rb[g, k, a].astype(F32)
                slot_row = slot_row + rs[g, k, a]
            xs[1, g, a, rows_of(x)] = total.astype(BF16)
            xl[1, g, a, :, cols_of(x)] = rounded(slot_row)
        for k in (2, 1, 3):
            start(row_send(g, k))

    def first_rows(g, parity):
        r = iota((144, 520), 0)
        i = clip(g, jnp.where(r < 128, r // 64, r - 128), parity)
        want = jnp.where(r < 130, 65 * (2 * i + parity) + jnp.where(r < 128, mod(r, 64), 64), -1)
        rows = dot((want == iota((144, 520), 1)).astype(BF16), xin[...])
        return rows, layer_norm(rows, ln1g[0:1], ln1b[0:1]).astype(BF16)

    def for_sibling(g):
        project(0, first_rows(g, 1 - c)[1], c, om.at[g], oml.at[g], 0)

    def give(g):
        heads = pl.ds(pl.multiple_of(2 * c, 2), 2)
        return with_row(
            om.at[g], oml.at[g], msg.at[0, g, :, heads], msl.at[0, g, :, heads], s_out, s_take.at[g], sib
        )

    def own_rows(g):
        rows, h = first_rows(g, c)
        for a in range(2):
            xs[0, g, a] = rows[64 * a : 64 * a + 64].astype(BF16)
            xl[0, g, a] = rows[128 + a : 129 + a]
        project(0, h, c, msg.at[0, g], msl.at[0, g], 2 * c)

    with scope("first_rows"):
        lx().wait()
        pltpu.make_async_copy(ruler.at[pl.ds(0, 55)], ruler.at[pl.ds(0, 55)], s_p).wait()
        lq_wait(0)
        for_sibling(0)
        own_rows(0)

    with scope("barrier"):
        pl.semaphore_wait(barrier, 20)

    start(give(0))
    send_shard(0, 0, c)
    with scope("second_rows"):
        for_sibling(1)
    start(give(1))
    with scope("wait_take"):
        came(100, s_take.at[0])
    send_shard(0, 0, 1 - c)
    with scope("second_rows"):
        own_rows(1)
    send_shard(0, 1, c)
    with scope("wait_take"):
        came(100, s_take.at[1])
    send_shard(0, 1, 1 - c)
    wo_start(0)
    rb0().start()
    rb1().start()
    for l in range(LAYERS):
        r1(l).start()
        r2(l).start()
    for j in range(3):
        rq(1, j).start()
        lq(1, j).start()
    for l in range(LAYERS):
        lo(l).start()
        l1(l).start()
        l2(l).start()

    copy_t.wait()
    copy_c.wait()
    tq = jnp.zeros((16, 128), jnp.int32)
    td, tf, nd, nf = tq, tq, tq, tq
    for j in range(16):
        fd = 4 * (j // 4) + 2 * (1 - c) + (j % 4) // 2
        fp = 4 * (j // 4) + 2 * c + (j % 4) // 2
        tq = jnp.where(lane16 == j, time_ref[fd], tq)
        td = jnp.where(row16 == j, time_ref[fd], td)
        tf = jnp.where(row16 == j, time_ref[fp], tf)
        nd = jnp.where(row16 == j, cond_ref[fd], nd)
        nf = jnp.where(row16 == j, cond_ref[fp], nf)
    part = mod(row16, 2)
    bias_d = jnp.where(td <= tq, 0.0, NEG)
    bias_f = jnp.where(tf <= tq, 0.0, NEG)
    bsl[0:16] = jnp.where(part < nd, bias_d, NEG).astype(BF16)
    bsl[16:32] = jnp.where(part < nf, bias_f, NEG).astype(BF16)
    for j in range(16):
        bd[j] = jnp.broadcast_to(bias_d[j : j + 1], (64, 128)).astype(BF16)
        bf[j] = jnp.broadcast_to(bias_f[j : j + 1], (64, 128)).astype(BF16)


    for l in range(LAYERS):
        if l == 1:
            lq_wait(1)
            came(3 * 256 + 3, s_rq)
            for g in range(2):
                with scope("wait_row"):
                    came(3 * 66, s_rx.at[g])
                with scope("project1"):
                    h = layer_norm(stream(1, g), ln1g[1:2], ln1b[1:2]).astype(BF16)
                    for k in range(2):
                        sh = mod(k + 1 - mod(z - 4 * c + 10, 8) // 4, 2)
                        project(1, h, sh, msg.at[1, g], msl.at[1, g], 2 * sh)
                        send_shard(1, g, sh)
            wo_start(1)

        attend(l)

        with scope("assemble"):
            assemble(l, 0)
        with scope("wait_wo"):
            loaded = ruler.at[pl.ds(0, 256 + 2 * 1024)]
            pltpu.make_async_copy(loaded, loaded, s_lw.at[l]).wait()
            arrived(wo.at[l, pl.ds(0, 3)], s_ro.at[l])
            for k in range(1, 4):
                wo_forward(l, k).start()
        with scope("assemble"):
            assemble(l, 1)
        with scope("wait_w"):
            arrived(wo.at[l, pl.ds(0, 4)], s_rfo.at[l])
            came(2 * 1024 + (4 if l == 0 else 0), s_rw.at[l])
        for g in range(2):
            mix(l, g)
        if l == 0:
            for g in range(2):
                next_rows(g)

    gx, ax = mod(x + c, 2), x // 2
    own, own_row = pl.ds(pl.multiple_of(64 * ax, 64), 64), pl.ds(128 + ax, 1)
    last = pf[gx, own] + fst[gx, own] + fc2b[1:2]
    row = pf[gx, own_row] + fst[gx, own_row] + fc2b[1:2]
    with scope("wait_last"):
        came(3 * 132, s_rc)
    for k in range(3):
        last = last + gb[k].astype(F32)
        row = row + gt[k]
    out_ref[0, 0:64] = last
    out_ref[0, 64:65] = row
    with scope("leave"):
        layer = 7 * 256 + 16 * 25 + 264 + 136 + 6 * 66
        total = 2 * layer + 4 * 1024 + 3 * 256 + 3 + 4 + 200 + 12 * 66 + 3 * 132
        for n in range(0, total, 2304):
            left(min(2304, total - n), s_out)


def shards(
    frames_in, frame_time, cond_count, ln1_gain, ln1_bias, qkv_weight, qkv_bias, out_weight, out_bias,
    ln2_gain, ln2_bias, fc1_weight, fc1_bias, fc2_weight, fc2_bias,
):
    any_ = pl.BlockSpec(memory_space=pl.ANY)
    vm = pl.BlockSpec(memory_space=VMEM)
    L = LAYERS
    rows = pl.pallas_call(
        kernel,
        name="layers",
        out_shape=VMEM((1, 65, D), F32),
        in_specs=[any_] * 15,
        out_specs=vm,
        scratch_shapes=[
            pltpu.SMEM((16,), jnp.int32), pltpu.SMEM((16,), jnp.int32), *[VMEM((L, D), F32)] * 6,
            VMEM((520, D), BF16), VMEM((L, 2, 2, 64, D), BF16), VMEM((L, 2, 2, 1, D), F32),
            VMEM((2, 2, 2, 96, 128), BF16), VMEM((2, 2, 2, 1, 256), F32),
            VMEM((L, 2, D, 384), BF16), VMEM((2, 3, L, 128), F32), VMEM((L, 8, 128, D), BF16),
            VMEM((L, 2, D, 512), BF16), VMEM((2, L, 512), F32), VMEM((L, 2, 512, D), BF16),
            VMEM((L, 2, 2, 4, 96, 128), BF16), VMEM((L, 2, 2, 4, 1, 256), F32),
            VMEM((L, 16, 96, 128), BF16), VMEM((L, 16, 1, 256), F32),
            VMEM((L, 16, 64, 128), BF16), VMEM((L, 16, 1, 128), F32), VMEM((32, 256), BF16),
            VMEM((L, 16, 32, 128), BF16), VMEM((L, 16, 1, 128), F32),
            VMEM((L, 16, 32, 128), BF16), VMEM((L, 16, 1, 128), F32),
            VMEM((L, 2, 4, 2, 64, 256), BF16), VMEM((L, 2, 4, 2, 1, 256), F32),
            VMEM((2, 144, D), F32), VMEM((2, 144, D), F32),
            VMEM((2, 4, 2, 16, D), BF16), VMEM((2, 4, 2, 1, 256), F32),
            VMEM((2, 3, 2, 16, D), BF16), VMEM((2, 3, 2, 1, 256), F32),
            VMEM((4, 64, D), BF16), VMEM((4, 1, D), F32), VMEM((3, 64, D), BF16), VMEM((3, 1, D), F32),
            VMEM((16, 64, 128), BF16), VMEM((16, 64, 128), BF16), VMEM((32, 128), BF16),
            VMEM((1040, 256), BF16), VMEM((2304, 1, 256), F32),
            DMA((2,)), DMA, DMA, DMA((L,)), DMA((L,)), DMA, DMA, DMA((L,)), DMA((L,)), DMA((L,)),
            DMA((L, 4)), DMA((L,)), DMA((L, 4)), DMA((L, 2, 2)), DMA((2,)), DMA((2,)), DMA, DMA((2,)),
        ],
        compiler_params=pltpu.CompilerParams(
            collective_id=0, has_side_effects=True, vmem_limit_bytes=60 * 2**20
        ),
    )(
        frame_time, cond_count, ln1_gain, ln1_bias, ln2_gain, ln2_bias, out_bias, fc2_bias,
        jnp.transpose(qkv_bias, (1, 0, 2)), fc1_bias, frames_in, qkv_weight, out_weight, fc1_weight, fc2_weight,
    )
    return rows.astype(BF16)


def solution(mesh):
    in_specs = (
        P("tm", None, None), P(), P(), P(), P(),
        P(None, None, None, "tensor"), P(None, None, "tensor"), P(None, "tensor", None), P(), P(), P(),
        P(None, None, "tensor"), P(None, "tensor"), P(None, "tensor", None), P(),
    )
    return jax.shard_map(shards, mesh=mesh, in_specs=in_specs, out_specs=P("tm", "tensor", None), check_vma=False)
```

```python
import jax
import jax.numpy as jnp
from jax import lax
from jax.experimental import pallas as pl
from jax.experimental.pallas import tpu as pltpu
from jax.sharding import PartitionSpec as P

MESH = pl.DeviceIdType.MESH
LAYERS = 2
D = 1024
F32 = jnp.float32
BF16 = jnp.bfloat16
NEG = -1e30
VMEM = pltpu.VMEM
DMA = pltpu.SemaphoreType.DMA
scope = jax.named_scope


def mod(a, n):
    return lax.rem(a, n)


def place(y, z, x, c):
    return {"tm": y * 8 + z, "tensor": x * 2 + c}


def iota(shape, dim):
    return lax.broadcasted_iota(jnp.int32, shape, dim)


def layer_norm(rows, gain, bias):
    center = jnp.mean(rows, axis=-1, keepdims=True)
    moved = rows - center
    spread = jnp.mean(moved * moved, axis=-1, keepdims=True)
    return moved * lax.rsqrt(spread + 1e-06) * gain + bias


def gelu(v):
    return 0.5 * v * (1.0 + lax.erf(v * (0.5**0.5)))


def dot(a, b):
    return lax.dot_general(a, b, (((1,), (0,)), ((), ())), preferred_element_type=F32)


def dot_t(a, b):
    return lax.dot_general(a, b, (((1,), (1,)), ((), ())), preferred_element_type=F32)


def rounded(v):
    return v.astype(BF16).astype(F32)


def swap(v):
    return pltpu.roll(v, 64, 1)


def kernel(
    time_hbm, cond_hbm, ln1g_hbm, ln1b_hbm, ln2g_hbm, ln2b_hbm, outb_hbm, fc2b_hbm, qkvb_hbm, fc1b_hbm,
    x_hbm, wq_hbm, wo_hbm, w1_hbm, w2_hbm,
    out_ref,
    time_ref, cond_ref, ln1g, ln1b, ln2g, ln2b, outb, fc2b,
    xin, xs, xl, om, oml, wq, qb, wo, w1, b1, w2, msg, msl, rk, rkl, fk, fkl, ksl, ob, obl, ab, abl, ag, agl, fst, pf,
    pb, ps, rb, rs, cb, ct, gb, gt, bd, bf, bsl, qx, ruler,
    s_t, s_p, s_x, s_lq, s_lw, s_out, s_rq, s_rw, s_ro, s_rfo, s_rm, s_rf, s_rr, s_rg, s_rp, s_rx, s_rc, s_take,
):
    p = lax.axis_index("tm")
    t = lax.axis_index("tensor")
    y, z = p // 8, mod(p, 8)
    x, c = t // 2, mod(t, 2)
    sib = place(y, z, x, 1 - c)
    zh, zl = z // 4, mod(z, 4)
    att = mod(y - zl + 4, 4)
    half = 1 - c
    slot = y * 4 + zl

    def peer(k):
        return place(y, z, mod(x + k, 4), c)

    def clip(g, a, parity):
        return 2 * a + mod(g + parity, 2)

    def clip_home(i, h):
        return place(mod(i + h, 4), 4 * c + h, x, 1 - zh)

    def part_source(j):
        return place(j // 4, 4 * half + mod(j, 4), x, zh)

    def far_first(n):
        a, r = 3 - n // 4, mod(n, 4)
        down = 1 - mod(z - 4 * half + 10, 8) // 4
        return mod(y + a + a // 2 * (5 - 2 * a), 4) * 4 + r + down * (3 - 2 * r)

    def remote(src, dst, ssem, rsem, dev):
        return pltpu.make_async_remote_copy(
            src_ref=src, dst_ref=dst, send_sem=ssem, recv_sem=rsem, device_id=dev, device_id_type=MESH
        )

    def arrived(dst, rsem):
        remote(dst, dst, rsem, rsem, sib).wait_recv()

    def sent(src, ssem):
        remote(src, src, ssem, ssem, sib).wait_send()

    barrier = pltpu.get_barrier_semaphore()

    def greet(dev):
        pl.semaphore_signal(barrier, inc=1, device_id=dev, device_id_type=MESH)

    @pl.loop(0, 16)
    def _(j):
        greet(part_source(j))

    for k in range(1, 4):
        greet(peer(k))
    greet(sib)

    def lx():
        return pltpu.make_async_copy(x_hbm.at[0], xin, s_x)

    def lq(l, j):
        return pltpu.make_async_copy(wq_hbm.at[l, j], wq.at[l, c, :, pl.ds(128 * j, 128)], s_lq.at[l])

    def lq_wait(l):
        pltpu.make_async_copy(wq.at[l, c], wq.at[l, c], s_lq.at[l]).wait()

    def lo(l):
        return pltpu.make_async_copy(wo_hbm.at[l], wo.at[l, t], s_lw.at[l])

    def l1(l):
        return pltpu.make_async_copy(w1_hbm.at[l], w1.at[l, c], s_lw.at[l])

    def l2(l):
        return pltpu.make_async_copy(w2_hbm.at[l], w2.at[l, c], s_lw.at[l])

    lx().start()
    params = (
        (ln1g_hbm, ln1g), (ln1b_hbm, ln1b), (ln2g_hbm, ln2g), (ln2b_hbm, ln2b), (outb_hbm, outb), (fc2b_hbm, fc2b),
        (qkvb_hbm, qb.at[c]), (fc1b_hbm, b1.at[c]),
    )
    for src, dst in params:
        pltpu.make_async_copy(src, dst, s_p).start()
    copy_t = pltpu.make_async_copy(time_hbm, time_ref, s_t.at[0])
    copy_c = pltpu.make_async_copy(cond_hbm, cond_ref, s_t.at[1])
    copy_t.start()
    copy_c.start()
    for j in range(3):
        lq(0, j).start()

    low = iota((64, 128), 1) < 64
    low1 = iota((1, 128), 1) < 64
    low32 = iota((32, 128), 1) < 64
    row16 = iota((16, 128), 0)
    lane16 = iota((16, 128), 1)

    def rq(l, j):
        return remote(wq_hbm.at[l, j], wq.at[l, c, :, pl.ds(128 * j, 128)], s_out, s_rq, sib)

    def rb0():
        return remote(qkvb_hbm, qb.at[c], s_out, s_rq, sib)

    def rb1():
        return remote(fc1b_hbm, b1.at[c], s_out, s_rw.at[0], sib)

    def r1(l):
        return remote(w1_hbm.at[l], w1.at[l, c], s_out, s_rw.at[l], sib)

    def r2(l):
        return remote(w2_hbm.at[l], w2.at[l, c], s_out, s_rw.at[l], sib)

    def wo_send(l, k):
        return remote(wo_hbm.at[l], wo.at[l, t], s_out, s_ro.at[l], peer(k))

    def wo_forward(l, k):
        xx = mod(x + k, 4)
        src = wo_hbm.at[l] if k == 0 else wo.at[l, 2 * xx + c]
        return remote(src, wo.at[l, 2 * xx + c], s_out, s_rfo.at[l], sib)

    def wo_start(l):
        for k in (2, 1, 3):
            wo_send(l, k).start()
        wo_forward(l, 0).start()

    def with_row(rows, slot_row, rows_to, slot_to, ssem, rsem, dev):
        return remote(rows, rows_to, ssem, rsem, dev), remote(slot_row, slot_to, ssem, rsem, dev)

    def start(copies):
        for copy in copies:
            copy.start()

    def came(kib, rsem):
        arrived(ruler.at[pl.ds(0, kib)], rsem)

    def left(kib, ssem):
        sent(ruler.at[pl.ds(0, kib)], ssem)

    def msg_send(l, g, a, h):
        return with_row(
            msg.at[l, g, a, h], msl.at[l, g, a, h], rk.at[l, slot], rkl.at[l, slot], s_out, s_rm.at[l, y],
            clip_home(clip(g, a, c), h),
        )

    def four(n):
        return pl.ds(pl.multiple_of(4 * n, 4), 4)

    def forward(l, n):
        return with_row(
            rk.at[l, four(n), pl.ds(0, 64)], rkl.at[l, four(n), :, pl.ds(0, 128)], fk.at[l, four(n)],
            fkl.at[l, four(n)], s_out, s_rf.at[l], sib,
        )

    def result_send(l, j):
        me = 2 * mod(att + zh, 2) + att // 2
        return with_row(
            ob.at[l, j], obl.at[l, j], ab.at[l, 4 * me + zl], abl.at[l, 4 * me + zl], s_out, s_rr.at[l, me],
            part_source(j),
        )

    def gather_send(l, g, k):
        rows, row = ag.at[l, g, x], agl.at[l, g, x]
        return with_row(rows, row, rows, row, s_out, s_rg.at[l, g, k % 2], peer(k))

    def gather_far(l, g, a):
        rows, row = ag.at[l, g, x, a], agl.at[l, g, x, a]
        return with_row(rows, row, rows, row, s_out, s_rg.at[l, g, 0], peer(2))

    def row_far(g, a):
        rows, row = xs.at[1, g, a, rows_of(x)], xl.at[1, g, a, :, cols_of(x)]
        return with_row(rows, row, rows, row, s_out, s_rx.at[g], peer(2))

    def rows_of(xx):
        return pl.ds(pl.multiple_of(16 * xx, 16), 16)

    def cols_of(xx):
        return pl.ds(pl.multiple_of(256 * xx, 256), 256)

    def part_send(g, k):
        xx = mod(x + k, 4)
        return with_row(
            pb.at[g, xx], ps.at[g, xx], rb.at[g, 3 - k], rs.at[g, 3 - k], s_out, s_rp.at[g], peer(k)
        )

    def row_send(g, k):
        rows, row = xs.at[1, g, :, rows_of(x)], xl.at[1, g, :, :, cols_of(x)]
        return with_row(rows, row, rows, row, s_out, s_rx.at[g], peer(k))

    def last_send(g, a):
        i = clip(g, a, c)
        k = mod(x - i + 4, 4) - 1
        n = 2 * g + a
        return with_row(cb.at[n], ct.at[n], gb.at[k], gt.at[k], s_out, s_rc, place(y, z, i, c))

    def project(l, h, sh, blocks, rows, first):
        out = dot(h, wq[l, sh])
        q = rounded(out[:, 0:128] + qb[sh, 0, l : l + 1]) * 0.125
        k = rounded(out[:, 128:256] + qb[sh, 1, l : l + 1])
        v = rounded(out[:, 256:384] + qb[sh, 2, l : l + 1])
        kr, vr, qr = swap(k), swap(v), swap(q)
        for a in range(2):
            o, r = 64 * a, 128 + a
            for hh in range(2):
                kk, vv = (k, vr) if hh == 0 else (kr, v)
                q0, q1 = (q, qr) if hh == 0 else (qr, q)
                m = blocks.at[a, first + hh]
                m[0:64] = jnp.where(low, kk[o : o + 64], vv[o : o + 64]).astype(BF16)
                m[64:96] = jnp.where(low32, q0[o : o + 32], q1[o + 32 : o + 64]).astype(BF16)
                rows[a, first + hh] = jnp.concatenate(
                    [jnp.where(low1, kk[r : r + 1], vv[r : r + 1]), jnp.where(low1, q0[r : r + 1], 0.0)], axis=1
                )

    def send_shard(l, g, sh):
        far = 1 - mod(z - 4 * c - 2 * sh + 11, 8) // 4
        for n in range(2):
            for a in range(2):
                start(msg_send(l, g, a, 2 * sh + mod(n + far, 2)))

    def attend(l):
        with scope("wait_msg"):

            @pl.loop(0, 4)
            def _(a):
                n = mod(y + a + a // 2 * (5 - 2 * a), 4)
                came(4 * 25, s_rm.at[l, n])
                start(forward(l, n))

        low512 = iota((512, 128), 1) < 64
        low1024 = iota((1024, 128), 1) < 64

        def values(kv, n):
            return jnp.where(low1024[0:n], jnp.ones((n, 128), BF16), kv)

        def queries():
            q = rk[l, :, 64:96, :].astype(F32).reshape(512, 128)
            qq = jnp.concatenate([jnp.where(low512, q, 0.0), jnp.where(low512, swap(q), 0.0)], axis=0).astype(BF16)
            hot = (mod(iota((1024, 128), 0), 512) // 32 == iota((1024, 128), 1)).astype(BF16)
            slots = rkl[l].reshape(16, 256).astype(BF16)
            ksl[0:16, 0:128] = slots[:, 0:128]
            slots_q = jnp.concatenate([slots[:, 128:256], (row16 == lane16).astype(BF16)], axis=1)
            qx[...] = jnp.concatenate([jnp.concatenate([qq, hot], axis=1), slots_q], axis=0)

        def scored(k, bias):
            return dot_t(qx[...], jnp.concatenate([k, bias[...].reshape(1024, 128)], axis=1))

        def top_of(s):
            return jnp.max(s, axis=1, keepdims=True)

        def weighted(s, top, kv, n):
            return dot(jnp.exp((s - top).astype(BF16)), values(kv, n))

        def own_keys():
            return rk[l, :, 0:64, :].reshape(1024, 128)

        def passed_keys():
            return fk[l].reshape(1024, 128)

        def slot_keys():
            ksl[16:32, 0:128] = fkl[l].reshape(16, 128).astype(BF16)
            ksl[:, 128:256] = bsl[...]
            return dot_t(qx[...], ksl[...])

        def finish(o):
            lo_, hi_, sl = o[0:512], o[512:1024], o[1024:1040]
            mixed = jnp.where(low512, swap(lo_), hi_) / jnp.where(low512, lo_, swap(hi_))
            ob[l] = mixed.astype(BF16).reshape(16, 32, 128)
            obl[l] = jnp.where(lane16 >= 64, rounded(sl / swap(sl)), 0.0).reshape(16, 1, 128)

        with scope("queries"):
            queries()

        @pl.when(half == zh)
        def _():
            k1 = own_keys()
            s1 = scored(k1, bd)
            top1 = top_of(s1)
            o1 = weighted(s1, top1, k1, 1024)
            came(264, s_rf.at[l])
            k2 = passed_keys()
            s2, s3 = scored(k2, bf), slot_keys()
            top = jnp.maximum(jnp.maximum(top_of(s2), top_of(s3)), top1)
            o = jnp.exp(top1 - top) * o1 + weighted(s2, top, k2, 1024)
            finish(o + weighted(s3, top, ksl[:, 0:128], 32))

        @pl.when(half != zh)
        def _():
            came(264, s_rf.at[l])
            k1, k2 = own_keys(), passed_keys()
            s1, s3 = scored(k1, bd), slot_keys()
            top1 = jnp.maximum(top_of(s1), top_of(s3))
            o1 = weighted(s1, top1, k1, 1024) + weighted(s3, top1, ksl[:, 0:128], 32)
            s2 = scored(k2, bf)
            top2 = top_of(s2)
            o2 = weighted(s2, top2, k2, 1024)
            top = jnp.maximum(top1, top2)
            finish(jnp.exp(top1 - top) * o1 + jnp.exp(top2 - top) * o2)

        @pl.loop(0, 16)
        def _(n):
            start(result_send(l, far_first(n)))

    def assemble(l, g):
        for a in range(2):
            q = 4 * (2 * g + a)
            with scope("wait_result"):
                came(34, s_rr.at[l, 2 * g + a])

            for m in range(2):
                u = ab[l, q + 2 * m].astype(F32)
                v = ab[l, q + 2 * m + 1].astype(F32)
                cols = slice(128 * m, 128 * m + 128)
                ag[l, g, x, a, 0:32, cols] = jnp.where(low32, u, swap(v)).astype(BF16)
                ag[l, g, x, a, 32:64, cols] = jnp.where(low32, swap(u), v).astype(BF16)
                agl[l, g, x, a, :, cols] = jnp.where(low1, swap(abl[l, q + 2 * m]), abl[l, q + 2 * m + 1])
            start(gather_far(l, g, a))
        for k in (1, 3):
            start(gather_send(l, g, k))

    def stacked(blocks, rows):
        n = rows[0].shape[1]
        which = iota((16, n), 0)
        tile = jnp.where(which == 0, jnp.broadcast_to(rows[0], (16, n)), 0.0)
        tile = jnp.where(which == 1, jnp.broadcast_to(rows[1], (16, n)), tile)
        return jnp.concatenate([*blocks, tile.astype(blocks[0].dtype)], axis=0)

    def stream(l, g):
        return stacked([xs[l, g, a].astype(F32) for a in range(2)], [xl[l, g, a] for a in range(2)])

    def mix(l, g):
        def arrive(odd):
            with scope("wait_gather"):
                came(66 * (1 + odd), s_rg.at[l, g, odd])

        def piece(k):
            xx = mod(x + k, 4)
            attended = stacked([ag[l, g, xx, a] for a in range(2)], [agl[l, g, xx, a] for a in range(2)])
            return dot(attended, wo[l, pl.ds(2 * xx, 2)].reshape(256, D))

        with scope("out_proj"):
            first = stream(l, g) + outb[l : l + 1] + piece(0)
        arrive(1)
        with scope("out_proj"):
            first = first + (piece(1) + piece(3))
        arrive(0)
        with scope("out_proj"):
            first = first + piece(2)
            fst[g] = first
            normed = layer_norm(first, ln2g[l : l + 1], ln2b[l : l + 1]).astype(BF16)
        with scope("mlp"):
            inner = [gelu(dot(normed, w1[l, sh]) + b1[sh, l : l + 1]).astype(BF16) for sh in range(2)]
            total = dot(jnp.concatenate(inner, axis=1), w2[l].reshape(D, D))
            pf[g] = total
            for a in range(2):
                mine = total[64 * a : 64 * a + 64].astype(BF16)
                row = rounded(total[128 + a : 129 + a])
                if l == 0:
                    for xx in range(4):
                        pb[g, xx, a] = mine[16 * xx : 16 * xx + 16]
                        ps[g, xx, a] = row[:, 256 * xx : 256 * xx + 256]
                else:
                    cb[2 * g + a] = mine
                    ct[2 * g + a] = row
        if l == 0:
            for k in (2, 1, 3):
                start(part_send(g, k))
        else:
            for a in range(2):

                @pl.when(x != clip(g, a, c))
                def _():
                    start(last_send(g, a))

    def next_rows(g):
        with scope("wait_part"):
            came(3 * 66, s_rp.at[g])
        for a in range(2):
            own = pl.ds(pl.multiple_of(64 * a + 16 * x, 16), 16)
            row = pl.ds(128 + a, 1)
            total = pf[g, own] + fst[g, own] + fc2b[0:1]
            slot_row = pf[g, row, cols_of(x)] + fst[g, row, cols_of(x)] + fc2b[0:1, cols_of(x)]
            for k in range(3):
                total = total + rb[g, k, a].astype(F32)
                slot_row = slot_row + rs[g, k, a]
            xs[1, g, a, rows_of(x)] = total.astype(BF16)
            xl[1, g, a, :, cols_of(x)] = rounded(slot_row)
            start(row_far(g, a))
        for k in (1, 3):
            start(row_send(g, k))

    def first_rows(g, parity):
        r = iota((144, 520), 0)
        i = clip(g, jnp.where(r < 128, r // 64, r - 128), parity)
        want = jnp.where(r < 130, 65 * (2 * i + parity) + jnp.where(r < 128, mod(r, 64), 64), -1)
        rows = dot((want == iota((144, 520), 1)).astype(BF16), xin[...])
        return rows, layer_norm(rows, ln1g[0:1], ln1b[0:1]).astype(BF16)

    def for_sibling(g):
        project(0, first_rows(g, 1 - c)[1], c, om.at[g], oml.at[g], 0)

    def give(g):
        heads = pl.ds(pl.multiple_of(2 * c, 2), 2)
        return with_row(
            om.at[g], oml.at[g], msg.at[0, g, :, heads], msl.at[0, g, :, heads], s_out, s_take.at[g], sib
        )

    def own_rows(g):
        rows, h = first_rows(g, c)
        for a in range(2):
            xs[0, g, a] = rows[64 * a : 64 * a + 64].astype(BF16)
            xl[0, g, a] = rows[128 + a : 129 + a]
        project(0, h, c, msg.at[0, g], msl.at[0, g], 2 * c)

    with scope("first_rows"):
        lx().wait()
        pltpu.make_async_copy(ruler.at[pl.ds(0, 55)], ruler.at[pl.ds(0, 55)], s_p).wait()
        lq_wait(0)
        for_sibling(0)
        own_rows(0)

    with scope("barrier"):
        pl.semaphore_wait(barrier, 20)

    start(give(0))
    send_shard(0, 0, c)
    with scope("second_rows"):
        for_sibling(1)
    start(give(1))
    with scope("wait_take"):
        came(100, s_take.at[0])
    send_shard(0, 0, 1 - c)
    with scope("second_rows"):
        own_rows(1)
    send_shard(0, 1, c)
    with scope("wait_take"):
        came(100, s_take.at[1])
    send_shard(0, 1, 1 - c)
    wo_start(0)
    rb0().start()
    rb1().start()
    for l in range(LAYERS):
        r1(l).start()
        r2(l).start()
    for j in range(3):
        rq(1, j).start()
        lq(1, j).start()
    for l in range(LAYERS):
        lo(l).start()
        l1(l).start()
        l2(l).start()

    copy_t.wait()
    copy_c.wait()
    tq = jnp.zeros((16, 128), jnp.int32)
    td, tf, nd, nf = tq, tq, tq, tq
    for j in range(16):
        fd = 4 * (j // 4) + 2 * (1 - c) + (j % 4) // 2
        fp = 4 * (j // 4) + 2 * c + (j % 4) // 2
        tq = jnp.where(lane16 == j, time_ref[fd], tq)
        td = jnp.where(row16 == j, time_ref[fd], td)
        tf = jnp.where(row16 == j, time_ref[fp], tf)
        nd = jnp.where(row16 == j, cond_ref[fd], nd)
        nf = jnp.where(row16 == j, cond_ref[fp], nf)
    part = mod(row16, 2)
    bias_d = jnp.where(td <= tq, 0.0, NEG)
    bias_f = jnp.where(tf <= tq, 0.0, NEG)
    bsl[0:16] = jnp.where(part < nd, bias_d, NEG).astype(BF16)
    bsl[16:32] = jnp.where(part < nf, bias_f, NEG).astype(BF16)
    for j in range(16):
        bd[j] = jnp.broadcast_to(bias_d[j : j + 1], (64, 128)).astype(BF16)
        bf[j] = jnp.broadcast_to(bias_f[j : j + 1], (64, 128)).astype(BF16)


    for l in range(LAYERS):
        if l == 1:
            lq_wait(1)
            came(3 * 256 + 3, s_rq)
            for g in range(2):
                with scope("wait_row"):
                    came(3 * 66, s_rx.at[g])
                with scope("project1"):
                    h = layer_norm(stream(1, g), ln1g[1:2], ln1b[1:2]).astype(BF16)
                    for k in range(2):
                        sh = mod(k + 1 - mod(z - 4 * c + 10, 8) // 4, 2)
                        project(1, h, sh, msg.at[1, g], msl.at[1, g], 2 * sh)
                        send_shard(1, g, sh)
            wo_start(1)

        attend(l)

        with scope("assemble"):
            assemble(l, 0)
        with scope("wait_wo"):
            loaded = ruler.at[pl.ds(0, 256 + 2 * 1024)]
            pltpu.make_async_copy(loaded, loaded, s_lw.at[l]).wait()
            arrived(wo.at[l, pl.ds(0, 3)], s_ro.at[l])
            for k in range(1, 4):
                wo_forward(l, k).start()
        with scope("assemble"):
            assemble(l, 1)
        with scope("wait_w"):
            arrived(wo.at[l, pl.ds(0, 4)], s_rfo.at[l])
            came(2 * 1024 + (4 if l == 0 else 0), s_rw.at[l])
        for g in range(2):
            mix(l, g)
        if l == 0:
            for g in range(2):
                next_rows(g)

    gx, ax = mod(x + c, 2), x // 2
    own, own_row = pl.ds(pl.multiple_of(64 * ax, 64), 64), pl.ds(128 + ax, 1)
    last = pf[gx, own] + fst[gx, own] + fc2b[1:2]
    row = pf[gx, own_row] + fst[gx, own_row] + fc2b[1:2]
    with scope("wait_last"):
        came(3 * 132, s_rc)
    for k in range(3):
        last = last + gb[k].astype(F32)
        row = row + gt[k]
    out_ref[0, 0:64] = last
    out_ref[0, 64:65] = row
    with scope("leave"):
        layer = 7 * 256 + 16 * 25 + 264 + 136 + 6 * 66
        total = 2 * layer + 4 * 1024 + 3 * 256 + 3 + 4 + 200 + 12 * 66 + 3 * 132
        for n in range(0, total, 2304):
            left(min(2304, total - n), s_out)


def shards(
    frames_in, frame_time, cond_count, ln1_gain, ln1_bias, qkv_weight, qkv_bias, out_weight, out_bias,
    ln2_gain, ln2_bias, fc1_weight, fc1_bias, fc2_weight, fc2_bias,
):
    any_ = pl.BlockSpec(memory_space=pl.ANY)
    vm = pl.BlockSpec(memory_space=VMEM)
    L = LAYERS
    rows = pl.pallas_call(
        kernel,
        name="layers",
        out_shape=VMEM((1, 65, D), F32),
        in_specs=[any_] * 15,
        out_specs=vm,
        scratch_shapes=[
            pltpu.SMEM((16,), jnp.int32), pltpu.SMEM((16,), jnp.int32), *[VMEM((L, D), F32)] * 6,
            VMEM((520, D), BF16), VMEM((L, 2, 2, 64, D), BF16), VMEM((L, 2, 2, 1, D), F32),
            VMEM((2, 2, 2, 96, 128), BF16), VMEM((2, 2, 2, 1, 256), F32),
            VMEM((L, 2, D, 384), BF16), VMEM((2, 3, L, 128), F32), VMEM((L, 8, 128, D), BF16),
            VMEM((L, 2, D, 512), BF16), VMEM((2, L, 512), F32), VMEM((L, 2, 512, D), BF16),
            VMEM((L, 2, 2, 4, 96, 128), BF16), VMEM((L, 2, 2, 4, 1, 256), F32),
            VMEM((L, 16, 96, 128), BF16), VMEM((L, 16, 1, 256), F32),
            VMEM((L, 16, 64, 128), BF16), VMEM((L, 16, 1, 128), F32), VMEM((32, 256), BF16),
            VMEM((L, 16, 32, 128), BF16), VMEM((L, 16, 1, 128), F32),
            VMEM((L, 16, 32, 128), BF16), VMEM((L, 16, 1, 128), F32),
            VMEM((L, 2, 4, 2, 64, 256), BF16), VMEM((L, 2, 4, 2, 1, 256), F32),
            VMEM((2, 144, D), F32), VMEM((2, 144, D), F32),
            VMEM((2, 4, 2, 16, D), BF16), VMEM((2, 4, 2, 1, 256), F32),
            VMEM((2, 3, 2, 16, D), BF16), VMEM((2, 3, 2, 1, 256), F32),
            VMEM((4, 64, D), BF16), VMEM((4, 1, D), F32), VMEM((3, 64, D), BF16), VMEM((3, 1, D), F32),
            VMEM((16, 64, 128), BF16), VMEM((16, 64, 128), BF16), VMEM((32, 128), BF16),
            VMEM((1040, 256), BF16), VMEM((2304, 1, 256), F32),
            DMA((2,)), DMA, DMA, DMA((L,)), DMA((L,)), DMA, DMA, DMA((L,)), DMA((L,)), DMA((L,)),
            DMA((L, 4)), DMA((L,)), DMA((L, 4)), DMA((L, 2, 2)), DMA((2,)), DMA((2,)), DMA, DMA((2,)),
        ],
        compiler_params=pltpu.CompilerParams(
            collective_id=0, has_side_effects=True, vmem_limit_bytes=60 * 2**20
        ),
    )(
        frame_time, cond_count, ln1_gain, ln1_bias, ln2_gain, ln2_bias, out_bias, fc2_bias,
        jnp.transpose(qkv_bias, (1, 0, 2)), fc1_bias, frames_in, qkv_weight, out_weight, fc1_weight, fc2_weight,
    )
    return rows.astype(BF16)


def solution(mesh):
    in_specs = (
        P("tm", None, None), P(), P(), P(), P(),
        P(None, None, None, "tensor"), P(None, None, "tensor"), P(None, "tensor", None), P(), P(), P(),
        P(None, None, "tensor"), P(None, "tensor"), P(None, "tensor", None), P(),
    )
    return jax.shard_map(shards, mesh=mesh, in_specs=in_specs, out_specs=P("tm", "tensor", None), check_vma=False)
```
